8 devices in a mesh: data: 1 (over z), stage: 8 (over y, x, core).
Axes of the slice: x: 2, y: 2, z: 1, core: 2. Of those that a mesh axis runs over, the one named last changes fastest.
Arguments:
- acts_in: bfloat16 [8, 2048, 768], P(('data', 'stage'))
- grad_out: bfloat16 [8, 2048, 768], P(('data', 'stage'))
- w_up_a: bfloat16 [8, 768, 3072], P('stage')
- w_down_a: bfloat16 [8, 3072, 768], P('stage')
- w_up_b: bfloat16 [8, 768, 768], P('stage')
- w_down_b: bfloat16 [8, 768, 768], P('stage')
Outputs:
- output 1: bfloat16 [8, 2048, 768], P(('data', 'stage'))
- output 2: bfloat16 [8, 2048, 768], P(('data', 'stage'))
- output 3: float32 [8, 768, 3072], P(('data', 'stage'))
- output 4: float32 [8, 3072, 768], P(('data', 'stage'))
- output 5: float32 [8, 768, 768], P(('data', 'stage'))
- output 6: float32 [8, 768, 768], P(('data', 'stage'))
All inputs are finite; a program needn't handle non-finite values.
Results may differ from the reference program's by a relative error of at most 0.02.
Values are sent between devices in bfloat16 or wider.
A program may use at most 1 GiB of HBM per device.

```python
import jax
import jax.numpy as jnp
from jax import lax

D_MODEL = 768
D_FF = 3072
STAGES = 8
ROUNDS = 1
N_MICRO = 8
TOKENS = 2048

PAIRS = ROUNDS * STAGES
NARROW = D_FF // 4
LAYERS = 2 * PAIRS


def setup_inputs(seed: int = 0, part: int = 0) -> dict:
    data_root, weight_root = jax.random.split(jax.random.key(seed), 2)
    part_key = jax.random.fold_in(data_root, part)
    key_acts, key_grad = jax.random.split(part_key, 2)
    key_up_a, key_down_a, key_up_b, key_down_b = jax.random.split(weight_root, 4)
    depth_gain = (3.0 / LAYERS) ** 0.5
    acts_in = jax.random.normal(key_acts, (N_MICRO, TOKENS, D_MODEL), jnp.float32)
    grad_out = jax.random.normal(key_grad, (N_MICRO, TOKENS, D_MODEL), jnp.float32)
    w_up_a = jax.random.normal(key_up_a, (PAIRS, D_MODEL, D_FF), jnp.float32) * (D_MODEL ** -0.5)
    w_down_a = jax.random.normal(key_down_a, (PAIRS, D_FF, D_MODEL), jnp.float32) * (depth_gain * D_FF ** -0.5)
    w_up_b = jax.random.normal(key_up_b, (PAIRS, D_MODEL, NARROW), jnp.float32) * (D_MODEL ** -0.5)
    w_down_b = jax.random.normal(key_down_b, (PAIRS, NARROW, D_MODEL), jnp.float32) * (depth_gain * NARROW ** -0.5)
    return dict(acts_in=acts_in.astype(jnp.bfloat16), grad_out=grad_out.astype(jnp.bfloat16), w_up_a=w_up_a.astype(jnp.bfloat16), w_down_a=w_down_a.astype(jnp.bfloat16), w_up_b=w_up_b.astype(jnp.bfloat16), w_down_b=w_down_b.astype(jnp.bfloat16))


def layer_forward(hidden, w_up, w_down):
    pre_act = jnp.dot(hidden, w_up, preferred_element_type=jnp.float32)
    gelu_out = jax.nn.gelu(pre_act).astype(jnp.bfloat16)
    resid_delta = jnp.dot(gelu_out, w_down, preferred_element_type=jnp.float32)
    return (hidden.astype(jnp.float32) + resid_delta).astype(jnp.bfloat16)


def layer_backward(hidden, w_up, w_down, grad_next):
    pre_act = jnp.dot(hidden, w_up, preferred_element_type=jnp.float32)
    gelu_val, gelu_pull = jax.vjp(jax.nn.gelu, pre_act)
    gelu_out = gelu_val.astype(jnp.bfloat16)
    dw_down = jnp.dot(gelu_out.T, grad_next, preferred_element_type=jnp.float32)
    d_gelu = jnp.dot(grad_next, w_down.T, preferred_element_type=jnp.float32)
    d_pre = gelu_pull(d_gelu)[0].astype(jnp.bfloat16)
    dw_up = jnp.dot(hidden.T, d_pre, preferred_element_type=jnp.float32)
    back_prod = jnp.dot(d_pre, w_up.T, preferred_element_type=jnp.float32)
    grad_prev = (grad_next.astype(jnp.float32) + back_prod).astype(jnp.bfloat16)
    return grad_prev, dw_up, dw_down


def to_pair_order(weight):
    return weight.reshape((STAGES, ROUNDS) + weight.shape[1:]).swapaxes(0, 1).reshape(weight.shape)


def from_pair_order(grad_stack):
    return grad_stack.reshape((ROUNDS, STAGES) + grad_stack.shape[1:]).swapaxes(0, 1).reshape(grad_stack.shape)


def pair_forward(hidden, pair_weights):
    up_a, down_a, up_b, down_b = pair_weights
    mid_hidden = layer_forward(hidden, up_a, down_a)
    return layer_forward(mid_hidden, up_b, down_b), (hidden, mid_hidden)


def pair_backward(grad_next, step_in):
    (hidden, mid_hidden), (up_a, down_a, up_b, down_b) = step_in
    grad_mid, dw_up_b, dw_down_b = layer_backward(mid_hidden, up_b, down_b, grad_next)
    grad_prev, dw_up_a, dw_down_a = layer_backward(hidden, up_a, down_a, grad_mid)
    return grad_prev, (dw_up_a, dw_down_a, dw_up_b, dw_down_b)


def reference(acts_in, grad_out, w_up_a, w_down_a, w_up_b, w_down_b):
    ordered = tuple(to_pair_order(weight) for weight in (w_up_a, w_down_a, w_up_b, w_down_b))

    def micro_step(grad_sums, micro_in):
        micro_acts, micro_grad = micro_in
        last_hidden, saved_acts = lax.scan(pair_forward, micro_acts, ordered)
        first_grad, pair_grads = lax.scan(pair_backward, micro_grad, (saved_acts, ordered), reverse=True)
        new_sums = tuple(run_sum + micro_part for run_sum, micro_part in zip(grad_sums, pair_grads))
        return new_sums, (last_hidden, first_grad)

    zero_sums = tuple(jnp.zeros(weight.shape, jnp.float32) for weight in ordered)
    grad_sums, (acts_out, grad_in) = lax.scan(micro_step, zero_sums, (acts_in, grad_out))
    weight_grads = tuple(from_pair_order(grad_stack) for grad_stack in grad_sums)
    return (acts_out, grad_in, weight_grads[0], weight_grads[1], weight_grads[2], weight_grads[3])
```

```python
import functools

import jax
import jax.numpy as jnp
from jax import lax
from jax.experimental import pallas as pl
from jax.experimental.pallas import tpu as pltpu
from jax.sharding import PartitionSpec as P

MESH = pl.DeviceIdType.MESH
ANY = pl.BlockSpec(memory_space=pl.ANY)
VMEM_LIMIT = 67043328

GELU_C = 0.7978845608028654
GELU_K = 0.044715

ROWS = 256
HOP = 2
SLOTS = 4
WIDE_COLS = 512
F_ORDER = 'zzzczczczcccyo'
B_ORDER = 'dmxxpxpxpxpxpp'
FB_ORDER = 'zdzmzczcxzcxzcccpxpxpyxpxpop'

NT = (((1,), (1,)), ((), ()))
TN = (((0,), (0,)), ((), ()))


def mm(lhs, rhs, dims=(((1,), (0,)), ((), ()))):
    return lax.dot_general(lhs, rhs, dims, preferred_element_type=jnp.float32)


def gelu_and_slope(z):
    zz = z * z
    half = 0.5 + 0.5 * jnp.tanh(z * (GELU_C + (GELU_C * GELU_K) * zz))
    act = z * half
    return act, half + act * (1.0 - half) * (2.0 * GELU_C + (6.0 * GELU_C * GELU_K) * zz)


def blocks(size, width):
    return [slice(start, min(start + width, size)) for start in range(0, size, width)]


def forward_tasks(h, weights, saved, done):
    ua, wa, ub, wb = weights
    a_buf, gp_buf, mid_buf, ab_buf, gpb_buf = saved
    cols = blocks(ua.shape[1], WIDE_COLS)

    def wide_up():
        for part in cols:
            act, slope = gelu_and_slope(mm(h[...], ua[:, part]))
            a_buf[:, part] = act.astype(jnp.bfloat16)
            gp_buf[:, part] = slope
            yield

    def wide_down():
        total = 0.0
        for k, part in enumerate(cols):
            product = mm(a_buf[:, part], wa[part, :])
            total = product if k == 0 else total + product
            if k == len(cols) - 1:
                mid_buf[...] = (h[...].astype(jnp.float32) + total).astype(jnp.bfloat16)
            yield

    def narrow_up():
        act, slope = gelu_and_slope(mm(mid_buf[...], ub[...]))
        ab_buf[...] = act.astype(jnp.bfloat16)
        gpb_buf[...] = slope
        yield

    def narrow_down():
        done((mid_buf[...].astype(jnp.float32) + mm(ab_buf[...], wb[...])).astype(jnp.bfloat16))
        yield

    return dict(z=wide_up(), c=wide_down(), y=narrow_up(), o=narrow_down())


def backward_tasks(g, weights, slopes, kept, done):
    ua, wa, ub, wb = weights
    gp_buf, gpb_buf = slopes
    dzb_buf, gmid_buf, dz_buf = kept
    cols = blocks(wa.shape[0], WIDE_COLS)

    def narrow_down():
        dzb_buf[...] = (mm(g[...], wb[...], NT) * gpb_buf[...]).astype(jnp.bfloat16)
        yield

    def narrow_up():
        gmid_buf[...] = (g[...].astype(jnp.float32) + mm(dzb_buf[...], ub[...], NT)).astype(jnp.bfloat16)
        yield

    def wide_down():
        for part in cols:
            dz_buf[:, part] = (mm(gmid_buf[...], wa[part, :], NT) * gp_buf[:, part]).astype(jnp.bfloat16)
            yield

    def wide_up():
        total = 0.0
        for k, part in enumerate(cols):
            product = mm(dz_buf[:, part], ua[:, part], NT)
            total = product if k == 0 else total + product
            if k == len(cols) - 1:
                done((gmid_buf[...].astype(jnp.float32) + total).astype(jnp.bfloat16))
            yield

    return dict(d=narrow_down(), m=narrow_up(), x=wide_down(), p=wide_up())


def run_tasks(order, tasks):
    for name in order:
        next(tasks[name])


def add_product(total, lhs, rhs, width):
    for rows in blocks(total.shape[0], width):
        total[rows, :] += mm(lhs[:, rows].T, rhs[...])


def kernel(
    axis, acts, gout, ua_hbm, wa_hbm, ub_hbm, wb_hbm,
    acts_out, grad_in, dua_hbm, dwa_hbm, dub_hbm, dwb_hbm,
    h_all, g_all, mid_all, a_all, gp_all, ab_all, gpb_all,
    ua, wa, ub, wb, dua, dwa, dub, dwb,
    h_buf, a_buf, gp_buf, mid_buf, ab_buf, gpb_buf, f_send,
    g_buf, gp_in, gpb_in, dzb_buf, gmid_buf, dz_buf, b_send,
    a_in, h_in, mid_in, ab_in,
    got_h, got_g, got_out, got_gin, f_sem, b_sem, feed_h_sem, feed_g_sem,
    h_sem, g_sem, gp_sem, gpb_sem, w_sem, st_sem, param_sem,
):
    me = lax.axis_index(axis)
    stages = lax.axis_size(axis)
    last = stages - 1
    own = acts.shape[0]
    chunks = own * stages
    span = HOP * last

    weights = (ua, wa, ub, wb)

    def fwd_chunk(t):
        return t - HOP * me

    def bwd_chunk(t):
        return t - 2 * span - 1 + HOP * me

    def valid(c):
        return (c >= 0) & (c < chunks)

    def on(device):
        return dict(device_id={axis: device}, device_id_type=MESH)

    def load(src, dst, sem):
        return pltpu.make_async_copy(src, dst, sem)

    params = [load(src, dst, param_sem.at[k]) for k, (src, dst) in enumerate(
        [(ua_hbm, ua), (wa_hbm, wa), (ub_hbm, ub), (wb_hbm, wb)])]
    for copy in params:
        copy.start()

    def arrival(buf, c, sem):
        return pltpu.make_async_remote_copy(buf.at[c], buf.at[c], sem.at[c], sem.at[c], **on(me))

    def fetch_h(c):
        @pl.when(valid(c))
        def _():
            local = (me == 0) & (c < own)

            @pl.when(local)
            def _():
                load(acts.at[lax.rem(c, own)], h_buf, h_sem).start()

            @pl.when(jnp.logical_not(local))
            def _():
                arrival(h_all, c, got_h).wait_recv()
                load(h_all.at[c], h_buf, h_sem).start()

    def fetch_g(c):
        @pl.when(valid(c))
        def _():
            load(gp_all.at[c], gp_in, gp_sem).start()
            load(gpb_all.at[c], gpb_in, gpb_sem).start()
            local = (me == last) & (c >= chunks - own)
            buf = g_buf.at[lax.rem(c, 2)]

            @pl.when(local)
            def _():
                load(gout.at[lax.rem(c, own)], buf, g_sem).start()

            @pl.when(jnp.logical_not(local))
            def _():
                arrival(g_all, c, got_g).wait_recv()
                load(g_all.at[c], buf, g_sem).start()

    def fetch_weight_operands(c):
        local_h = (me == 0) & (c < own)

        @pl.when(local_h)
        def _():
            load(acts.at[lax.rem(c, own)], h_in, w_sem.at[0]).start()

        @pl.when(jnp.logical_not(local_h))
        def _():
            load(h_all.at[c], h_in, w_sem.at[0]).start()
        load(a_all.at[c], a_in, w_sem.at[1]).start()
        load(mid_all.at[c], mid_in, w_sem.at[2]).start()
        load(ab_all.at[c], ab_in, w_sem.at[3]).start()

    def send(slot_ref, sem, c, inner, next_device, next_all, next_sem, home_out, home_sem):
        home = c // own
        spot = lax.rem(c, own)

        @pl.when(inner)
        def _():
            pltpu.make_async_remote_copy(slot_ref, next_all.at[c], sem, next_sem.at[c], **on(next_device)).start()

        @pl.when(jnp.logical_not(inner) & (home != me))
        def _():
            pltpu.make_async_remote_copy(slot_ref, home_out.at[spot], sem, home_sem.at[spot], **on(home)).start()

        @pl.when(jnp.logical_not(inner) & (home == me))
        def _():
            load(slot_ref, home_out.at[spot], sem).start()

    def sent(slot_ref, sem):
        load(slot_ref, slot_ref, sem).wait()

    def store_copies(c):
        pairs = [(a_buf, a_all), (gp_buf, gp_all), (mid_buf, mid_all), (ab_buf, ab_all), (gpb_buf, gpb_all)]
        return [load(src, dst.at[c], st_sem.at[k]) for k, (src, dst) in enumerate(pairs)]

    fetch_h(fwd_chunk(0))
    for total in (dua, dwa, dub, dwb):
        total[...] = jnp.zeros_like(total)
    for copy in params:
        copy.wait()

    def step(t, _):
        cf, cb = fwd_chunk(t), bwd_chunk(t)
        has_f, has_b = valid(cf), valid(cb)
        fed = t + own - own * me

        @pl.when((me != 0) & (fed >= 0) & (fed < own))
        def _():
            pltpu.make_async_remote_copy(acts.at[fed], h_all.at[own * me + fed], feed_h_sem.at[fed], got_h.at[own * me + fed], **on(0)).start()

        fed_g = t - own * me

        @pl.when((me != last) & (fed_g >= 0) & (fed_g < own))
        def _():
            pltpu.make_async_remote_copy(gout.at[fed_g], g_all.at[own * me + fed_g], feed_g_sem.at[fed_g], got_g.at[own * me + fed_g], **on(last)).start()

        @pl.when(has_b)
        def _():
            fetch_weight_operands(cb)

        g_now = g_buf.at[lax.rem(jnp.maximum(cb, 0), 2)]
        f_slot, b_slot = lax.rem(cf, SLOTS), lax.rem(cb, SLOTS)

        def f_begin():
            load(h_buf, h_buf, h_sem).wait()

            @pl.when(cf >= SLOTS)
            def _():
                sent(f_send.at[f_slot], f_sem.at[f_slot])

        def f_tasks():
            def done(h):
                f_send[f_slot] = h
            return forward_tasks(h_buf, weights, (a_buf, gp_buf, mid_buf, ab_buf, gpb_buf), done)

        def f_end():
            send(f_send.at[f_slot], f_sem.at[f_slot], cf, me != last, me + 1, h_all, got_h, acts_out, got_out)
            for copy in store_copies(cf):
                copy.start()

        def b_begin():
            load(g_buf.at[0], g_buf.at[0], g_sem).wait()
            load(gp_in, gp_in, gp_sem).wait()
            load(gpb_in, gpb_in, gpb_sem).wait()

            @pl.when(cb >= SLOTS)
            def _():
                sent(b_send.at[b_slot], b_sem.at[b_slot])

        def b_tasks():
            def done(g):
                b_send[b_slot] = g
            return backward_tasks(g_now, weights, (gp_in, gpb_in), (dzb_buf, gmid_buf, dz_buf), done)

        def b_end():
            send(b_send.at[b_slot], b_sem.at[b_slot], cb, me != 0, me - 1, g_all, got_g, grad_in, got_gin)

        @pl.when(has_f & has_b)
        def _():
            f_begin()
            b_begin()
            run_tasks(FB_ORDER, f_tasks() | b_tasks())
            b_end()
            f_end()

        @pl.when(has_f & jnp.logical_not(has_b))
        def _():
            f_begin()
            run_tasks(F_ORDER, f_tasks())
            f_end()

        @pl.when(has_b & jnp.logical_not(has_f))
        def _():
            b_begin()
            run_tasks(B_ORDER, b_tasks())
            b_end()

        @pl.when(has_f)
        def _():
            for copy in store_copies(cf):
                copy.wait()

        fetch_g(cb + 1)
        fetch_h(cf + 1)

        @pl.when(has_b)
        def _():
            for k, buf in enumerate((h_in, a_in, mid_in, ab_in)):
                load(buf, buf, w_sem.at[k]).wait()
            add_product(dwb, ab_in, g_now, 256)
            add_product(dub, mid_in, dzb_buf, 256)
            add_product(dwa, a_in, gmid_buf, 256)
            add_product(dua, h_in, dz_buf, 256)
        return 0

    lax.fori_loop(0, chunks + 2 * span + 1, step, 0)

    finals = [load(src, dst, param_sem.at[k]) for k, (src, dst) in enumerate(
        [(dua, dua_hbm), (dwa, dwa_hbm), (dub, dub_hbm), (dwb, dwb_hbm)])]
    for copy in finals:
        copy.start()
    for slot in range(SLOTS):
        sent(f_send.at[slot], f_sem.at[slot])
        sent(b_send.at[slot], b_sem.at[slot])

    def settle(k, _):
        @pl.when(me != 0)
        def _():
            load(acts.at[k], acts.at[k], feed_h_sem.at[k]).wait()
            arrival(grad_in, k, got_gin).wait_recv()

        @pl.when(me != last)
        def _():
            load(gout.at[k], gout.at[k], feed_g_sem.at[k]).wait()
            arrival(acts_out, k, got_out).wait_recv()
        return 0

    lax.fori_loop(0, own, settle, 0)
    for copy in finals:
        copy.wait()


def run_stages(axis, stages, acts, gout, ua, wa, ub, wb):
    tokens, width = acts.shape
    own = tokens // ROWS
    chunks = own * stages
    wide, narrow = ua.shape[1], ub.shape[1]
    bf, f32 = jnp.bfloat16, jnp.float32
    shape = jax.ShapeDtypeStruct
    outs = [
        shape((own, ROWS, width), bf), shape((own, ROWS, width), bf),
        shape(ua.shape, f32), shape(wa.shape, f32), shape(ub.shape, f32), shape(wb.shape, f32),
        shape((chunks, ROWS, width), bf), shape((chunks, ROWS, width), bf), shape((chunks, ROWS, width), bf),
        shape((chunks, ROWS, wide), bf), shape((chunks, ROWS, wide), f32),
        shape((chunks, ROWS, narrow), bf), shape((chunks, ROWS, narrow), f32),
    ]
    vm, dma = pltpu.VMEM, pltpu.SemaphoreType.DMA
    tok, wid, nar = (ROWS, width), (ROWS, wide), (ROWS, narrow)
    scratch = [
        vm(ua.shape, bf), vm(wa.shape, bf), vm(ub.shape, bf), vm(wb.shape, bf),
        vm(ua.shape, f32), vm(wa.shape, f32), vm(ub.shape, f32), vm(wb.shape, f32),
        vm(tok, bf), vm(wid, bf), vm(wid, f32), vm(tok, bf), vm(nar, bf), vm(nar, f32), vm((SLOTS,) + tok, bf),
        vm((2,) + tok, bf), vm(wid, f32), vm(nar, f32), vm(nar, bf), vm(tok, bf), vm(wid, bf), vm((SLOTS,) + tok, bf),
        vm(wid, bf), vm(tok, bf), vm(tok, bf), vm(nar, bf),
        dma((chunks,)), dma((chunks,)), dma((own,)), dma((own,)), dma((SLOTS,)), dma((SLOTS,)), dma((own,)), dma((own,)),
        dma, dma, dma, dma, dma((4,)), dma((5,)), dma((4,)),
    ]
    results = pl.pallas_call(
        functools.partial(kernel, axis),
        out_shape=outs,
        in_specs=[ANY] * 6,
        out_specs=[ANY] * len(outs),
        scratch_shapes=scratch,
        compiler_params=pltpu.CompilerParams(vmem_limit_bytes=VMEM_LIMIT, has_side_effects=True),
    )(acts.reshape(own, ROWS, width), gout.reshape(own, ROWS, width), ua, wa, ub, wb)
    return results[:6]


def solution(mesh):
    tok_spec = P(('data', 'stage'))
    row_spec = P('stage')
    stages = mesh.shape['stage']

    def device_body(acts_in, grad_out, w_up_a, w_down_a, w_up_b, w_down_b):
        tokens, width = acts_in.shape[0] * acts_in.shape[1], acts_in.shape[2]
        out, gin, dua, dwa, dub, dwb = run_stages(
            'stage', stages, acts_in.reshape(tokens, width), grad_out.reshape(tokens, width),
            w_up_a[0], w_down_a[0], w_up_b[0], w_down_b[0])
        return (out.reshape(acts_in.shape), gin.reshape(acts_in.shape), dua[None], dwa[None], dub[None], dwb[None])

    return jax.shard_map(device_body, mesh=mesh, in_specs=(tok_spec, tok_spec, row_spec, row_spec, row_spec, row_spec), out_specs=(tok_spec,) * 6, check_vma=False)
```

```python
import functools

import jax
import jax.numpy as jnp
from jax import lax
from jax.experimental import pallas as pl
from jax.experimental.pallas import tpu as pltpu
from jax.sharding import PartitionSpec as P

MESH = pl.DeviceIdType.MESH
ANY = pl.BlockSpec(memory_space=pl.ANY)
VMEM_LIMIT = 67043328

GELU_C = 0.7978845608028654
GELU_K = 0.044715

ROWS = 256
HOP = 3
SLOTS = 4
WIDE_COLS = 512
F_ORDER = 'zzczczczczccyo'
B_ORDER = 'dmxxpxpxpxpxpp'
FB_ORDER = 'zdmzxzcxpzcxpzcxpzccpxcxpypo'

NT = (((1,), (1,)), ((), ()))
TN = (((0,), (0,)), ((), ()))


def mm(lhs, rhs, dims=(((1,), (0,)), ((), ()))):
    return lax.dot_general(lhs, rhs, dims, preferred_element_type=jnp.float32)


def gelu_and_slope(z):
    zz = z * z
    half = 0.5 + 0.5 * jnp.tanh(z * (GELU_C + (GELU_C * GELU_K) * zz))
    act = z * half
    return act, half + act * (1.0 - half) * (2.0 * GELU_C + (6.0 * GELU_C * GELU_K) * zz)


def blocks(size, width):
    return [slice(start, min(start + width, size)) for start in range(0, size, width)]


def forward_tasks(h, weights, saved, done):
    ua, wa, ub, wb = weights
    a_buf, gp_buf, mid_buf, ab_buf, gpb_buf = saved
    cols = blocks(ua.shape[1], WIDE_COLS)

    def wide_up():
        for part in cols:
            act, slope = gelu_and_slope(mm(h[...], ua[:, part]))
            a_buf[:, part] = act.astype(jnp.bfloat16)
            gp_buf[:, part] = slope
            yield

    def wide_down():
        total = 0.0
        for k, part in enumerate(cols):
            product = mm(a_buf[:, part], wa[part, :])
            total = product if k == 0 else total + product
            if k == len(cols) - 1:
                mid_buf[...] = (h[...].astype(jnp.float32) + total).astype(jnp.bfloat16)
            yield

    def narrow_up():
        act, slope = gelu_and_slope(mm(mid_buf[...], ub[...]))
        ab_buf[...] = act.astype(jnp.bfloat16)
        gpb_buf[...] = slope
        yield

    def narrow_down():
        done((mid_buf[...].astype(jnp.float32) + mm(ab_buf[...], wb[...])).astype(jnp.bfloat16))
        yield

    return dict(z=wide_up(), c=wide_down(), y=narrow_up(), o=narrow_down())


def backward_tasks(g, weights, slopes, kept, done):
    ua, wa, ub, wb = weights
    gp_buf, gpb_buf = slopes
    dzb_buf, gmid_buf, dz_buf = kept
    cols = blocks(wa.shape[0], WIDE_COLS)

    def narrow_down():
        dzb_buf[...] = (mm(g[...], wb[...], NT) * gpb_buf[...]).astype(jnp.bfloat16)
        yield

    def narrow_up():
        gmid_buf[...] = (g[...].astype(jnp.float32) + mm(dzb_buf[...], ub[...], NT)).astype(jnp.bfloat16)
        yield

    def wide_down():
        for part in cols:
            dz_buf[:, part] = (mm(gmid_buf[...], wa[part, :], NT) * gp_buf[:, part]).astype(jnp.bfloat16)
            yield

    def wide_up():
        total = 0.0
        for k, part in enumerate(cols):
            product = mm(dz_buf[:, part], ua[:, part], NT)
            total = product if k == 0 else total + product
            if k == len(cols) - 1:
                done((gmid_buf[...].astype(jnp.float32) + total).astype(jnp.bfloat16))
            yield

    return dict(d=narrow_down(), m=narrow_up(), x=wide_down(), p=wide_up())


def run_tasks(order, tasks):
    for name in order:
        next(tasks[name])


def add_product(total, lhs, rhs, width):
    for rows in blocks(total.shape[0], width):
        total[rows, :] += mm(lhs[:, rows].T, rhs[...])


def kernel(
    axis, acts, gout, ua_hbm, wa_hbm, ub_hbm, wb_hbm,
    acts_out, grad_in, dua_hbm, dwa_hbm, dub_hbm, dwb_hbm,
    h_all, g_all, mid_all, a_all, gp_all, ab_all, gpb_all,
    ua, wa, ub, wb, dua, dwa, dub, dwb,
    h_buf, a_buf, gp_buf, mid_buf, ab_buf, gpb_buf, f_send,
    g_buf, gp_in, gpb_in, dzb_buf, gmid_buf, dz_buf, b_send,
    a_in, h_in, mid_in, ab_in,
    got_h, got_g, got_out, got_gin, f_sem, b_sem, feed_h_sem, feed_g_sem,
    h_sem, g_sem, gp_sem, gpb_sem, w_sem, st_sem, param_sem,
):
    me = lax.axis_index(axis)
    stages = lax.axis_size(axis)
    last = stages - 1
    own = acts.shape[0]
    chunks = own * stages
    span = HOP * last

    weights = (ua, wa, ub, wb)

    def fwd_chunk(t):
        return t - HOP * me

    def bwd_chunk(t):
        return t - 2 * span - 1 + HOP * me

    def valid(c):
        return (c >= 0) & (c < chunks)

    def on(device):
        return dict(device_id={axis: device}, device_id_type=MESH)

    def load(src, dst, sem):
        return pltpu.make_async_copy(src, dst, sem)

    params = [load(src, dst, param_sem.at[k]) for k, (src, dst) in enumerate(
        [(ua_hbm, ua), (wa_hbm, wa), (ub_hbm, ub), (wb_hbm, wb)])]
    for copy in params:
        copy.start()

    def arrival(buf, c, sem):
        return pltpu.make_async_remote_copy(buf.at[c], buf.at[c], sem.at[c], sem.at[c], **on(me))

    def fetch_h(c):
        @pl.when(valid(c))
        def _():
            local = (me == 0) & (c < own)

            @pl.when(local)
            def _():
                load(acts.at[lax.rem(c, own)], h_buf, h_sem).start()

            @pl.when(jnp.logical_not(local))
            def _():
                arrival(h_all, c, got_h).wait_recv()
                load(h_all.at[c], h_buf, h_sem).start()

    def fetch_g(c):
        @pl.when(valid(c))
        def _():
            load(gp_all.at[c], gp_in, gp_sem).start()
            load(gpb_all.at[c], gpb_in, gpb_sem).start()
            local = (me == last) & (c >= chunks - own)
            buf = g_buf.at[lax.rem(c, 2)]

            @pl.when(local)
            def _():
                load(gout.at[lax.rem(c, own)], buf, g_sem).start()

            @pl.when(jnp.logical_not(local))
            def _():
                arrival(g_all, c, got_g).wait_recv()
                load(g_all.at[c], buf, g_sem).start()

    def fetch_weight_operands(c):
        local_h = (me == 0) & (c < own)

        @pl.when(local_h)
        def _():
            load(acts.at[lax.rem(c, own)], h_in, w_sem.at[0]).start()

        @pl.when(jnp.logical_not(local_h))
        def _():
            load(h_all.at[c], h_in, w_sem.at[0]).start()
        load(a_all.at[c], a_in, w_sem.at[1]).start()
        load(mid_all.at[c], mid_in, w_sem.at[2]).start()
        load(ab_all.at[c], ab_in, w_sem.at[3]).start()

    def send(slot_ref, sem, c, inner, next_device, next_all, next_sem, home_out, home_sem):
        home = c // own
        spot = lax.rem(c, own)

        @pl.when(inner)
        def _():
            pltpu.make_async_remote_copy(slot_ref, next_all.at[c], sem, next_sem.at[c], **on(next_device)).start()

        @pl.when(jnp.logical_not(inner) & (home != me))
        def _():
            pltpu.make_async_remote_copy(slot_ref, home_out.at[spot], sem, home_sem.at[spot], **on(home)).start()

        @pl.when(jnp.logical_not(inner) & (home == me))
        def _():
            load(slot_ref, home_out.at[spot], sem).start()

    def sent(slot_ref, sem):
        load(slot_ref, slot_ref, sem).wait()

    def store_copies(c):
        pairs = [(a_buf, a_all), (gp_buf, gp_all), (mid_buf, mid_all), (ab_buf, ab_all), (gpb_buf, gpb_all)]
        return [load(src, dst.at[c], st_sem.at[k]) for k, (src, dst) in enumerate(pairs)]

    fetch_h(fwd_chunk(0))
    for total in (dua, dwa, dub, dwb):
        total[...] = jnp.zeros_like(total)
    for copy in params:
        copy.wait()

    def step(t, _):
        cf, cb = fwd_chunk(t), bwd_chunk(t)
        has_f, has_b = valid(cf), valid(cb)
        fed = t + own - own * me

        @pl.when((me != 0) & (fed >= 0) & (fed < own))
        def _():
            pltpu.make_async_remote_copy(acts.at[fed], h_all.at[own * me + fed], feed_h_sem.at[fed], got_h.at[own * me + fed], **on(0)).start()

        fed_g = t - own * me

        @pl.when((me != last) & (fed_g >= 0) & (fed_g < own))
        def _():
            pltpu.make_async_remote_copy(gout.at[fed_g], g_all.at[own * me + fed_g], feed_g_sem.at[fed_g], got_g.at[own * me + fed_g], **on(last)).start()

        @pl.when(has_b)
        def _():
            fetch_weight_operands(cb)

        g_now = g_buf.at[lax.rem(jnp.maximum(cb, 0), 2)]
        f_slot, b_slot = lax.rem(cf, SLOTS), lax.rem(cb, SLOTS)

        def f_begin():
            load(h_buf, h_buf, h_sem).wait()

            @pl.when(cf >= SLOTS)
            def _():
                sent(f_send.at[f_slot], f_sem.at[f_slot])

        def f_tasks():
            def done(h):
                f_send[f_slot] = h
            return forward_tasks(h_buf, weights, (a_buf, gp_buf, mid_buf, ab_buf, gpb_buf), done)

        def f_end():
            send(f_send.at[f_slot], f_sem.at[f_slot], cf, me != last, me + 1, h_all, got_h, acts_out, got_out)
            for copy in store_copies(cf):
                copy.start()

        def b_begin():
            load(g_buf.at[0], g_buf.at[0], g_sem).wait()
            load(gp_in, gp_in, gp_sem).wait()
            load(gpb_in, gpb_in, gpb_sem).wait()

            @pl.when(cb >= SLOTS)
            def _():
                sent(b_send.at[b_slot], b_sem.at[b_slot])

        def b_tasks():
            def done(g):
                b_send[b_slot] = g
            return backward_tasks(g_now, weights, (gp_in, gpb_in), (dzb_buf, gmid_buf, dz_buf), done)

        def b_end():
            send(b_send.at[b_slot], b_sem.at[b_slot], cb, me != 0, me - 1, g_all, got_g, grad_in, got_gin)

        @pl.when(has_f & has_b)
        def _():
            f_begin()
            b_begin()
            run_tasks(FB_ORDER, f_tasks() | b_tasks())
            b_end()
            f_end()

        @pl.when(has_f & jnp.logical_not(has_b))
        def _():
            f_begin()
            run_tasks(F_ORDER, f_tasks())
            f_end()

        @pl.when(has_b & jnp.logical_not(has_f))
        def _():
            b_begin()
            run_tasks(B_ORDER, b_tasks())
            b_end()

        @pl.when(has_f)
        def _():
            for copy in store_copies(cf):
                copy.wait()

        steady = valid(cf + 1)

        @pl.when(steady)
        def _():
            fetch_g(cb + 1)
            fetch_h(cf + 1)

        @pl.when(has_b)
        def _():
            for k, buf in enumerate((h_in, a_in, mid_in, ab_in)):
                load(buf, buf, w_sem.at[k]).wait()
            add_product(dwb, ab_in, g_now, 256)
            add_product(dub, mid_in, dzb_buf, 256)
            add_product(dwa, a_in, gmid_buf, 256)
            add_product(dua, h_in, dz_buf, 256)

        @pl.when(jnp.logical_not(steady))
        def _():
            fetch_g(cb + 1)
        return 0

    lax.fori_loop(0, chunks + 2 * span + 1, step, 0)

    finals = [load(src, dst, param_sem.at[k]) for k, (src, dst) in enumerate(
        [(dua, dua_hbm), (dwa, dwa_hbm), (dub, dub_hbm), (dwb, dwb_hbm)])]
    for copy in finals:
        copy.start()
    for slot in range(SLOTS):
        sent(f_send.at[slot], f_sem.at[slot])
        sent(b_send.at[slot], b_sem.at[slot])

    def settle(k, _):
        @pl.when(me != 0)
        def _():
            load(acts.at[k], acts.at[k], feed_h_sem.at[k]).wait()
            arrival(grad_in, k, got_gin).wait_recv()

        @pl.when(me != last)
        def _():
            load(gout.at[k], gout.at[k], feed_g_sem.at[k]).wait()
            arrival(acts_out, k, got_out).wait_recv()
        return 0

    lax.fori_loop(0, own, settle, 0)
    for copy in finals:
        copy.wait()


def run_stages(axis, stages, acts, gout, ua, wa, ub, wb):
    tokens, width = acts.shape
    own = tokens // ROWS
    chunks = own * stages
    wide, narrow = ua.shape[1], ub.shape[1]
    bf, f32 = jnp.bfloat16, jnp.float32
    shape = jax.ShapeDtypeStruct
    outs = [
        shape((own, ROWS, width), bf), shape((own, ROWS, width), bf),
        shape(ua.shape, f32), shape(wa.shape, f32), shape(ub.shape, f32), shape(wb.shape, f32),
        shape((chunks, ROWS, width), bf), shape((chunks, ROWS, width), bf), shape((chunks, ROWS, width), bf),
        shape((chunks, ROWS, wide), bf), shape((chunks, ROWS, wide), f32),
        shape((chunks, ROWS, narrow), bf), shape((chunks, ROWS, narrow), f32),
    ]
    vm, dma = pltpu.VMEM, pltpu.SemaphoreType.DMA
    tok, wid, nar = (ROWS, width), (ROWS, wide), (ROWS, narrow)
    scratch = [
        vm(ua.shape, bf), vm(wa.shape, bf), vm(ub.shape, bf), vm(wb.shape, bf),
        vm(ua.shape, f32), vm(wa.shape, f32), vm(ub.shape, f32), vm(wb.shape, f32),
        vm(tok, bf), vm(wid, bf), vm(wid, f32), vm(tok, bf), vm(nar, bf), vm(nar, f32), vm((SLOTS,) + tok, bf),
        vm((2,) + tok, bf), vm(wid, f32), vm(nar, f32), vm(nar, bf), vm(tok, bf), vm(wid, bf), vm((SLOTS,) + tok, bf),
        vm(wid, bf), vm(tok, bf), vm(tok, bf), vm(nar, bf),
        dma((chunks,)), dma((chunks,)), dma((own,)), dma((own,)), dma((SLOTS,)), dma((SLOTS,)), dma((own,)), dma((own,)),
        dma, dma, dma, dma, dma((4,)), dma((5,)), dma((4,)),
    ]
    results = pl.pallas_call(
        functools.partial(kernel, axis),
        out_shape=outs,
        in_specs=[ANY] * 6,
        out_specs=[ANY] * len(outs),
        scratch_shapes=scratch,
        compiler_params=pltpu.CompilerParams(vmem_limit_bytes=VMEM_LIMIT, has_side_effects=True),
    )(acts.reshape(own, ROWS, width), gout.reshape(own, ROWS, width), ua, wa, ub, wb)
    return results[:6]


def solution(mesh):
    tok_spec = P(('data', 'stage'))
    row_spec = P('stage')
    stages = mesh.shape['stage']

    def device_body(acts_in, grad_out, w_up_a, w_down_a, w_up_b, w_down_b):
        tokens, width = acts_in.shape[0] * acts_in.shape[1], acts_in.shape[2]
        out, gin, dua, dwa, dub, dwb = run_stages(
            'stage', stages, acts_in.reshape(tokens, width), grad_out.reshape(tokens, width),
            w_up_a[0], w_down_a[0], w_up_b[0], w_down_b[0])
        return (out.reshape(acts_in.shape), gin.reshape(acts_in.shape), dua[None], dwa[None], dub[None], dwb[None])

    return jax.shard_map(device_body, mesh=mesh, in_specs=(tok_spec, tok_spec, row_spec, row_spec, row_spec, row_spec), out_specs=(tok_spec,) * 6, check_vma=False)
```

```python
import functools

import jax
import jax.numpy as jnp
from jax import lax
from jax.experimental import pallas as pl
from jax.experimental.pallas import tpu as pltpu
from jax.sharding import PartitionSpec as P

MESH = pl.DeviceIdType.MESH
ANY = pl.BlockSpec(memory_space=pl.ANY)
VMEM_LIMIT = 67043328

GELU_C = 0.7978845608028654
GELU_K = 0.044715

ROWS = 256
HOP = 2
LAG = 2
SLOTS = 4
WIDE_COLS = 512
F_ORDER = 'zzczczczczccyo'
B_ORDER = 'dmxxpxpxpxpxpp'
FB_ORDER = 'zdmzxzcxpzcxpzcxpzccpxcxpypo'

NT = (((1,), (1,)), ((), ()))
TN = (((0,), (0,)), ((), ()))


def mm(lhs, rhs, dims=(((1,), (0,)), ((), ()))):
    return lax.dot_general(lhs, rhs, dims, preferred_element_type=jnp.float32)


def gelu_and_slope(z):
    zz = z * z
    half = 0.5 + 0.5 * jnp.tanh(z * (GELU_C + (GELU_C * GELU_K) * zz))
    act = z * half
    return act, half + act * (1.0 - half) * (2.0 * GELU_C + (6.0 * GELU_C * GELU_K) * zz)


def blocks(size, width):
    return [slice(start, min(start + width, size)) for start in range(0, size, width)]


def forward_tasks(h, weights, saved, done):
    ua, wa, ub, wb = weights
    a_buf, gp_buf, mid_buf, ab_buf, gpb_buf = saved
    cols = blocks(ua.shape[1], WIDE_COLS)

    def wide_up():
        for part in cols:
            act, slope = gelu_and_slope(mm(h[...], ua[:, part]))
            a_buf[:, part] = act.astype(jnp.bfloat16)
            gp_buf[:, part] = slope
            yield

    def wide_down():
        total = 0.0
        for k, part in enumerate(cols):
            product = mm(a_buf[:, part], wa[part, :])
            total = product if k == 0 else total + product
            if k == len(cols) - 1:
                mid_buf[...] = (h[...].astype(jnp.float32) + total).astype(jnp.bfloat16)
            yield

    def narrow_up():
        act, slope = gelu_and_slope(mm(mid_buf[...], ub[...]))
        ab_buf[...] = act.astype(jnp.bfloat16)
        gpb_buf[...] = slope
        yield

    def narrow_down():
        done((mid_buf[...].astype(jnp.float32) + mm(ab_buf[...], wb[...])).astype(jnp.bfloat16))
        yield

    return dict(z=wide_up(), c=wide_down(), y=narrow_up(), o=narrow_down())


def backward_tasks(g, weights, slopes, kept, done):
    ua, wa, ub, wb = weights
    gp_buf, gpb_buf = slopes
    dzb_buf, gmid_buf, dz_buf = kept
    cols = blocks(wa.shape[0], WIDE_COLS)

    def narrow_down():
        dzb_buf[...] = (mm(g[...], wb[...], NT) * gpb_buf[...]).astype(jnp.bfloat16)
        yield

    def narrow_up():
        gmid_buf[...] = (g[...].astype(jnp.float32) + mm(dzb_buf[...], ub[...], NT)).astype(jnp.bfloat16)
        yield

    def wide_down():
        for part in cols:
            dz_buf[:, part] = (mm(gmid_buf[...], wa[part, :], NT) * gp_buf[:, part]).astype(jnp.bfloat16)
            yield

    def wide_up():
        total = 0.0
        for k, part in enumerate(cols):
            product = mm(dz_buf[:, part], ua[:, part], NT)
            total = product if k == 0 else total + product
            if k == len(cols) - 1:
                done((gmid_buf[...].astype(jnp.float32) + total).astype(jnp.bfloat16))
            yield

    return dict(d=narrow_down(), m=narrow_up(), x=wide_down(), p=wide_up())


def run_tasks(order, tasks):
    for name in order:
        next(tasks[name])


def add_product(total, lhs, rhs, width):
    for rows in blocks(total.shape[0], width):
        total[rows, :] += mm(lhs[:, rows].T, rhs[...])


def kernel(
    axis, acts, gout, ua_hbm, wa_hbm, ub_hbm, wb_hbm,
    acts_out, grad_in, dua_hbm, dwa_hbm, dub_hbm, dwb_hbm,
    h_all, g_all, mid_all, a_all, gp_all, ab_all, gpb_all,
    ua, wa, ub, wb, dua, dwa, dub, dwb,
    h_buf, a_buf, gp_buf, mid_buf, ab_buf, gpb_buf, f_send,
    g_buf, gp_in, gpb_in, dzb_buf, gmid_buf, dz_buf, b_send,
    a_in, h_in, mid_in, ab_in,
    got_h, got_g, got_out, got_gin, f_sem, b_sem, feed_h_sem, feed_g_sem,
    h_sem, g_sem, gp_sem, gpb_sem, w_sem, st_sem, param_sem,
):
    me = lax.axis_index(axis)
    stages = lax.axis_size(axis)
    last = stages - 1
    own = acts.shape[0]
    chunks = own * stages

    def offset(stage):
        return HOP * stage + stage // (stages // 2)

    span = offset(last)

    weights = (ua, wa, ub, wb)

    def fwd_chunk(t):
        return t - offset(me)

    def bwd_chunk(t):
        return t - 2 * span - LAG + offset(me)

    def valid(c):
        return (c >= 0) & (c < chunks)

    def on(device):
        return dict(device_id={axis: device}, device_id_type=MESH)

    def load(src, dst, sem):
        return pltpu.make_async_copy(src, dst, sem)

    params = [load(src, dst, param_sem.at[k]) for k, (src, dst) in enumerate(
        [(ua_hbm, ua), (wa_hbm, wa), (ub_hbm, ub), (wb_hbm, wb)])]
    for copy in params:
        copy.start()

    def arrival(buf, c, sem):
        return pltpu.make_async_remote_copy(buf.at[c], buf.at[c], sem.at[c], sem.at[c], **on(me))

    def fetch_h(c):
        @pl.when(valid(c))
        def _():
            local = (me == 0) & (c < own)

            @pl.when(local)
            def _():
                load(acts.at[lax.rem(c, own)], h_buf, h_sem).start()

            @pl.when(jnp.logical_not(local))
            def _():
                arrival(h_all, c, got_h).wait_recv()
                load(h_all.at[c], h_buf, h_sem).start()

    def fetch_slopes(c):
        @pl.when(valid(c))
        def _():
            side = lax.rem(c, 2)
            load(gp_all.at[c], gp_in.at[side], gp_sem.at[side]).start()
            load(gpb_all.at[c], gpb_in.at[side], gpb_sem.at[side]).start()

    def fetch_g(c):
        @pl.when(valid(c))
        def _():
            local = (me == last) & (c >= chunks - own)
            buf = g_buf.at[lax.rem(c, 2)]

            @pl.when(local)
            def _():
                load(gout.at[lax.rem(c, own)], buf, g_sem).start()

            @pl.when(jnp.logical_not(local))
            def _():
                arrival(g_all, c, got_g).wait_recv()
                load(g_all.at[c], buf, g_sem).start()

    def fetch_weight_operands(c):
        local_h = (me == 0) & (c < own)

        @pl.when(local_h)
        def _():
            load(acts.at[lax.rem(c, own)], h_in, w_sem.at[0]).start()

        @pl.when(jnp.logical_not(local_h))
        def _():
            load(h_all.at[c], h_in, w_sem.at[0]).start()
        load(a_all.at[c], a_in, w_sem.at[1]).start()
        load(mid_all.at[c], mid_in, w_sem.at[2]).start()
        load(ab_all.at[c], ab_in, w_sem.at[3]).start()

    def send(slot_ref, sem, c, inner, next_device, next_all, next_sem, home_out, home_sem):
        home = c // own
        spot = lax.rem(c, own)

        @pl.when(inner)
        def _():
            pltpu.make_async_remote_copy(slot_ref, next_all.at[c], sem, next_sem.at[c], **on(next_device)).start()

        @pl.when(jnp.logical_not(inner) & (home != me))
        def _():
            pltpu.make_async_remote_copy(slot_ref, home_out.at[spot], sem, home_sem.at[spot], **on(home)).start()

        @pl.when(jnp.logical_not(inner) & (home == me))
        def _():
            load(slot_ref, home_out.at[spot], sem).start()

    def sent(slot_ref, sem):
        load(slot_ref, slot_ref, sem).wait()

    def store_copies(c):
        pairs = [(a_buf, a_all), (gp_buf, gp_all), (mid_buf, mid_all), (ab_buf, ab_all), (gpb_buf, gpb_all)]
        return [load(src, dst.at[c], st_sem.at[k]) for k, (src, dst) in enumerate(pairs)]

    fetch_h(fwd_chunk(0))
    for total in (dua, dwa, dub, dwb):
        total[...] = jnp.zeros_like(total)
    for copy in params:
        copy.wait()

    def step(t, _):
        cf, cb = fwd_chunk(t), bwd_chunk(t)
        has_f, has_b = valid(cf), valid(cb)
        fed = t + own - own * me

        @pl.when((me != 0) & (fed >= 0) & (fed < own))
        def _():
            pltpu.make_async_remote_copy(acts.at[fed], h_all.at[own * me + fed], feed_h_sem.at[fed], got_h.at[own * me + fed], **on(0)).start()

        fed_g = t - own * me

        @pl.when((me != last) & (fed_g >= 0) & (fed_g < own))
        def _():
            pltpu.make_async_remote_copy(gout.at[fed_g], g_all.at[own * me + fed_g], feed_g_sem.at[fed_g], got_g.at[own * me + fed_g], **on(last)).start()

        @pl.when(valid(cf - 1))
        def _():
            for copy in store_copies(cf - 1):
                copy.wait()

        fetch_slopes(cb + 1)

        @pl.when(has_b)
        def _():
            fetch_weight_operands(cb)

        b_side = lax.rem(jnp.maximum(cb, 0), 2)
        g_now, gp_now, gpb_now = g_buf.at[b_side], gp_in.at[b_side], gpb_in.at[b_side]
        f_slot, b_slot = lax.rem(cf, SLOTS), lax.rem(cb, SLOTS)

        def f_begin():
            load(h_buf, h_buf, h_sem).wait()

            @pl.when(cf >= SLOTS)
            def _():
                sent(f_send.at[f_slot], f_sem.at[f_slot])

        def f_tasks():
            def done(h):
                f_send[f_slot] = h
            return forward_tasks(h_buf, weights, (a_buf, gp_buf, mid_buf, ab_buf, gpb_buf), done)

        def f_end():
            send(f_send.at[f_slot], f_sem.at[f_slot], cf, me != last, me + 1, h_all, got_h, acts_out, got_out)
            for copy in store_copies(cf):
                copy.start()

        def b_begin():
            load(g_buf.at[0], g_buf.at[0], g_sem).wait()
            load(gp_now, gp_now, gp_sem.at[b_side]).wait()
            load(gpb_now, gpb_now, gpb_sem.at[b_side]).wait()

            @pl.when(cb >= SLOTS)
            def _():
                sent(b_send.at[b_slot], b_sem.at[b_slot])

        def b_tasks():
            def done(g):
                b_send[b_slot] = g
            return backward_tasks(g_now, weights, (gp_now, gpb_now), (dzb_buf, gmid_buf, dz_buf), done)

        def b_end():
            send(b_send.at[b_slot], b_sem.at[b_slot], cb, me != 0, me - 1, g_all, got_g, grad_in, got_gin)

        @pl.when(has_f & has_b)
        def _():
            f_begin()
            b_begin()
            run_tasks(FB_ORDER, f_tasks() | b_tasks())
            b_end()
            f_end()

        @pl.when(has_f & jnp.logical_not(has_b))
        def _():
            f_begin()
            run_tasks(F_ORDER, f_tasks())
            f_end()

        @pl.when(has_b & jnp.logical_not(has_f))
        def _():
            b_begin()
            run_tasks(B_ORDER, b_tasks())
            b_end()

        steady = valid(cf + 1)

        @pl.when(steady)
        def _():
            fetch_g(cb + 1)
            fetch_h(cf + 1)

        @pl.when(has_b)
        def _():
            for k, buf in enumerate((h_in, a_in, mid_in, ab_in)):
                load(buf, buf, w_sem.at[k]).wait()
            add_product(dwb, ab_in, g_now, 256)
            add_product(dub, mid_in, dzb_buf, 256)
            add_product(dwa, a_in, gmid_buf, 256)
            add_product(dua, h_in, dz_buf, 256)

        @pl.when(jnp.logical_not(steady))
        def _():
            fetch_g(cb + 1)
        return 0

    lax.fori_loop(0, chunks + 2 * span + LAG, step, 0)

    finals = [load(src, dst, param_sem.at[k]) for k, (src, dst) in enumerate(
        [(dua, dua_hbm), (dwa, dwa_hbm), (dub, dub_hbm), (dwb, dwb_hbm)])]
    for copy in finals:
        copy.start()
    for slot in range(SLOTS):
        sent(f_send.at[slot], f_sem.at[slot])
        sent(b_send.at[slot], b_sem.at[slot])

    def settle(k, _):
        @pl.when(me != 0)
        def _():
            load(acts.at[k], acts.at[k], feed_h_sem.at[k]).wait()
            arrival(grad_in, k, got_gin).wait_recv()

        @pl.when(me != last)
        def _():
            load(gout.at[k], gout.at[k], feed_g_sem.at[k]).wait()
            arrival(acts_out, k, got_out).wait_recv()
        return 0

    lax.fori_loop(0, own, settle, 0)
    for copy in finals:
        copy.wait()


def run_stages(axis, stages, acts, gout, ua, wa, ub, wb):
    tokens, width = acts.shape
    own = tokens // ROWS
    chunks = own * stages
    wide, narrow = ua.shape[1], ub.shape[1]
    bf, f32 = jnp.bfloat16, jnp.float32
    shape = jax.ShapeDtypeStruct
    outs = [
        shape((own, ROWS, width), bf), shape((own, ROWS, width), bf),
        shape(ua.shape, f32), shape(wa.shape, f32), shape(ub.shape, f32), shape(wb.shape, f32),
        shape((chunks, ROWS, width), bf), shape((chunks, ROWS, width), bf), shape((chunks, ROWS, width), bf),
        shape((chunks, ROWS, wide), bf), shape((chunks, ROWS, wide), f32),
        shape((chunks, ROWS, narrow), bf), shape((chunks, ROWS, narrow), f32),
    ]
    vm, dma = pltpu.VMEM, pltpu.SemaphoreType.DMA
    tok, wid, nar = (ROWS, width), (ROWS, wide), (ROWS, narrow)
    scratch = [
        vm(ua.shape, bf), vm(wa.shape, bf), vm(ub.shape, bf), vm(wb.shape, bf),
        vm(ua.shape, f32), vm(wa.shape, f32), vm(ub.shape, f32), vm(wb.shape, f32),
        vm(tok, bf), vm(wid, bf), vm(wid, f32), vm(tok, bf), vm(nar, bf), vm(nar, f32), vm((SLOTS,) + tok, bf),
        vm((2,) + tok, bf), vm((2,) + wid, f32), vm((2,) + nar, f32), vm(nar, bf), vm(tok, bf), vm(wid, bf), vm((SLOTS,) + tok, bf),
        vm(wid, bf), vm(tok, bf), vm(tok, bf), vm(nar, bf),
        dma((chunks,)), dma((chunks,)), dma((own,)), dma((own,)), dma((SLOTS,)), dma((SLOTS,)), dma((own,)), dma((own,)),
        dma, dma, dma((2,)), dma((2,)), dma((4,)), dma((5,)), dma((4,)),
    ]
    results = pl.pallas_call(
        functools.partial(kernel, axis),
        out_shape=outs,
        in_specs=[ANY] * 6,
        out_specs=[ANY] * len(outs),
        scratch_shapes=scratch,
        compiler_params=pltpu.CompilerParams(vmem_limit_bytes=VMEM_LIMIT, has_side_effects=True),
    )(acts.reshape(own, ROWS, width), gout.reshape(own, ROWS, width), ua, wa, ub, wb)
    return results[:6]


def solution(mesh):
    tok_spec = P(('data', 'stage'))
    row_spec = P('stage')
    stages = mesh.shape['stage']

    def device_body(acts_in, grad_out, w_up_a, w_down_a, w_up_b, w_down_b):
        tokens, width = acts_in.shape[0] * acts_in.shape[1], acts_in.shape[2]
        out, gin, dua, dwa, dub, dwb = run_stages(
            'stage', stages, acts_in.reshape(tokens, width), grad_out.reshape(tokens, width),
            w_up_a[0], w_down_a[0], w_up_b[0], w_down_b[0])
        return (out.reshape(acts_in.shape), gin.reshape(acts_in.shape), dua[None], dwa[None], dub[None], dwb[None])

    return jax.shard_map(device_body, mesh=mesh, in_specs=(tok_spec, tok_spec, row_spec, row_spec, row_spec, row_spec), out_specs=(tok_spec,) * 6, check_vma=False)
```

```python
import functools

import jax
import jax.numpy as jnp
from jax import lax
from jax.experimental import pallas as pl
from jax.experimental.pallas import tpu as pltpu
from jax.sharding import PartitionSpec as P

MESH = pl.DeviceIdType.MESH
ANY = pl.BlockSpec(memory_space=pl.ANY)
VMEM_LIMIT = 67043328

GELU_C = 0.7978845608028654
GELU_K = 0.044715

ROWS = 256
HOP = 2
LAG = 2
SLOTS = 4
WIDE_COLS = 512
F_ORDER = 'zzczczczczccyo'
B_ORDER = 'dmxxpxpxpxpxpp'
FB_ORDER = 'zdmzxzcxpzcxpzcxpzccpxcxpypo'

NT = (((1,), (1,)), ((), ()))
TN = (((0,), (0,)), ((), ()))


def mm(lhs, rhs, dims=(((1,), (0,)), ((), ()))):
    return lax.dot_general(lhs, rhs, dims, preferred_element_type=jnp.float32)


def gelu_and_slope(z):
    zz = z * z
    half = 0.5 + 0.5 * jnp.tanh(z * (GELU_C + (GELU_C * GELU_K) * zz))
    act = z * half
    return act, half + act * (1.0 - half) * (2.0 * GELU_C + (6.0 * GELU_C * GELU_K) * zz)


def blocks(size, width):
    return [slice(start, min(start + width, size)) for start in range(0, size, width)]


def forward_tasks(h, weights, saved, done):
    ua, wa, ub, wb = weights
    a_buf, gp_buf, mid_buf, ab_buf, gpb_buf = saved
    cols = blocks(ua.shape[1], WIDE_COLS)

    def wide_up():
        for part in cols:
            act, slope = gelu_and_slope(mm(h[...], ua[:, part]))
            a_buf[:, part] = act.astype(jnp.bfloat16)
            gp_buf[:, part] = slope
            yield

    def wide_down():
        total = 0.0
        for k, part in enumerate(cols):
            product = mm(a_buf[:, part], wa[part, :])
            total = product if k == 0 else total + product
            if k == len(cols) - 1:
                mid_buf[...] = (h[...].astype(jnp.float32) + total).astype(jnp.bfloat16)
            yield

    def narrow_up():
        act, slope = gelu_and_slope(mm(mid_buf[...], ub[...]))
        ab_buf[...] = act.astype(jnp.bfloat16)
        gpb_buf[...] = slope
        yield

    def narrow_down():
        done((mid_buf[...].astype(jnp.float32) + mm(ab_buf[...], wb[...])).astype(jnp.bfloat16))
        yield

    return dict(z=wide_up(), c=wide_down(), y=narrow_up(), o=narrow_down())


def backward_tasks(g, weights, slopes, kept, done):
    ua, wa, ub, wb = weights
    gp_buf, gpb_buf = slopes
    dzb_buf, gmid_buf, dz_buf = kept
    cols = blocks(wa.shape[0], WIDE_COLS)

    def narrow_down():
        dzb_buf[...] = (mm(g[...], wb[...], NT) * gpb_buf[...]).astype(jnp.bfloat16)
        yield

    def narrow_up():
        gmid_buf[...] = (g[...].astype(jnp.float32) + mm(dzb_buf[...], ub[...], NT)).astype(jnp.bfloat16)
        yield

    def wide_down():
        for part in cols:
            dz_buf[:, part] = (mm(gmid_buf[...], wa[part, :], NT) * gp_buf[:, part]).astype(jnp.bfloat16)
            yield

    def wide_up():
        total = 0.0
        for k, part in enumerate(cols):
            product = mm(dz_buf[:, part], ua[:, part], NT)
            total = product if k == 0 else total + product
            if k == len(cols) - 1:
                done((gmid_buf[...].astype(jnp.float32) + total).astype(jnp.bfloat16))
            yield

    return dict(d=narrow_down(), m=narrow_up(), x=wide_down(), p=wide_up())


def run_tasks(order, tasks):
    for name in order:
        next(tasks[name])


def add_product(total, lhs, rhs, width):
    for rows in blocks(total.shape[0], width):
        total[rows, :] += mm(lhs[:, rows].T, rhs[...])


def kernel(
    axis, acts, gout, ua_hbm, wa_hbm, ub_hbm, wb_hbm,
    acts_out, grad_in, dua_hbm, dwa_hbm, dub_hbm, dwb_hbm,
    h_all, g_all, mid_all, a_all, gp_all, ab_all, gpb_all,
    ua, wa, ub, wb, dua, dwa, dub, dwb,
    h_buf, a_buf, gp_buf, mid_buf, ab_buf, gpb_buf, f_send,
    g_buf, gp_in, gpb_in, dzb_buf, gmid_buf, dz_buf, b_send,
    a_in, h_in, mid_in, ab_in,
    got_h, got_g, got_out, got_gin, f_sem, b_sem, feed_h_sem, feed_g_sem,
    h_sem, g_sem, gp_sem, gpb_sem, w_sem, st_sem, param_sem,
):
    me = lax.axis_index(axis)
    stages = lax.axis_size(axis)
    last = stages - 1
    own = acts.shape[0]
    chunks = own * stages

    def offset(stage):
        return HOP * stage + stage // 2

    span = offset(last)

    weights = (ua, wa, ub, wb)

    def fwd_chunk(t):
        return t - offset(me)

    def bwd_chunk(t):
        return t - 2 * span - LAG + offset(me)

    def valid(c):
        return (c >= 0) & (c < chunks)

    def on(device):
        return dict(device_id={axis: device}, device_id_type=MESH)

    def load(src, dst, sem):
        return pltpu.make_async_copy(src, dst, sem)

    params = [load(src, dst, param_sem.at[k]) for k, (src, dst) in enumerate(
        [(ua_hbm, ua), (wa_hbm, wa), (ub_hbm, ub), (wb_hbm, wb)])]
    for copy in params:
        copy.start()

    def arrival(buf, c, sem):
        return pltpu.make_async_remote_copy(buf.at[c], buf.at[c], sem.at[c], sem.at[c], **on(me))

    def fetch_h(c):
        @pl.when(valid(c))
        def _():
            local = (me == 0) & (c < own)

            @pl.when(local)
            def _():
                load(acts.at[lax.rem(c, own)], h_buf, h_sem).start()

            @pl.when(jnp.logical_not(local))
            def _():
                arrival(h_all, c, got_h).wait_recv()
                load(h_all.at[c], h_buf, h_sem).start()

    def fetch_slopes(c):
        @pl.when(valid(c))
        def _():
            side = lax.rem(c, 2)
            load(gp_all.at[c], gp_in.at[side], gp_sem.at[side]).start()
            load(gpb_all.at[c], gpb_in.at[side], gpb_sem.at[side]).start()

    def fetch_g(c):
        @pl.when(valid(c))
        def _():
            local = (me == last) & (c >= chunks - own)
            buf = g_buf.at[lax.rem(c, 2)]

            @pl.when(local)
            def _():
                load(gout.at[lax.rem(c, own)], buf, g_sem).start()

            @pl.when(jnp.logical_not(local))
            def _():
                arrival(g_all, c, got_g).wait_recv()
                load(g_all.at[c], buf, g_sem).start()

    def fetch_weight_operands(c):
        local_h = (me == 0) & (c < own)

        @pl.when(local_h)
        def _():
            load(acts.at[lax.rem(c, own)], h_in, w_sem.at[0]).start()

        @pl.when(jnp.logical_not(local_h))
        def _():
            load(h_all.at[c], h_in, w_sem.at[0]).start()
        load(a_all.at[c], a_in, w_sem.at[1]).start()
        load(mid_all.at[c], mid_in, w_sem.at[2]).start()
        load(ab_all.at[c], ab_in, w_sem.at[3]).start()

    def send(slot_ref, sem, c, inner, next_device, next_all, next_sem, home_out, home_sem):
        home = c // own
        spot = lax.rem(c, own)

        @pl.when(inner)
        def _():
            pltpu.make_async_remote_copy(slot_ref, next_all.at[c], sem, next_sem.at[c], **on(next_device)).start()

        @pl.when(jnp.logical_not(inner) & (home != me))
        def _():
            pltpu.make_async_remote_copy(slot_ref, home_out.at[spot], sem, home_sem.at[spot], **on(home)).start()

        @pl.when(jnp.logical_not(inner) & (home == me))
        def _():
            load(slot_ref, home_out.at[spot], sem).start()

    def sent(slot_ref, sem):
        load(slot_ref, slot_ref, sem).wait()

    def store_copies(c):
        pairs = [(a_buf, a_all), (gp_buf, gp_all), (mid_buf, mid_all), (ab_buf, ab_all), (gpb_buf, gpb_all)]
        return [load(src, dst.at[c], st_sem.at[k]) for k, (src, dst) in enumerate(pairs)]

    fetch_h(fwd_chunk(0))
    for total in (dua, dwa, dub, dwb):
        total[...] = jnp.zeros_like(total)
    for copy in params:
        copy.wait()

    def step(t, _):
        cf, cb = fwd_chunk(t), bwd_chunk(t)
        has_f, has_b = valid(cf), valid(cb)
        fed = t + own - own * me

        @pl.when((me != 0) & (fed >= 0) & (fed < own))
        def _():
            pltpu.make_async_remote_copy(acts.at[fed], h_all.at[own * me + fed], feed_h_sem.at[fed], got_h.at[own * me + fed], **on(0)).start()

        fed_g = t - own * me

        @pl.when((me != last) & (fed_g >= 0) & (fed_g < own))
        def _():
            pltpu.make_async_remote_copy(gout.at[fed_g], g_all.at[own * me + fed_g], feed_g_sem.at[fed_g], got_g.at[own * me + fed_g], **on(last)).start()

        @pl.when(valid(cf - 1))
        def _():
            for copy in store_copies(cf - 1):
                copy.wait()

        fetch_slopes(cb + 1)

        @pl.when(has_b)
        def _():
            fetch_weight_operands(cb)

        b_side = lax.rem(jnp.maximum(cb, 0), 2)
        g_now, gp_now, gpb_now = g_buf.at[b_side], gp_in.at[b_side], gpb_in.at[b_side]
        f_slot, b_slot = lax.rem(cf, SLOTS), lax.rem(cb, SLOTS)

        def f_begin():
            load(h_buf, h_buf, h_sem).wait()

            @pl.when(cf >= SLOTS)
            def _():
                sent(f_send.at[f_slot], f_sem.at[f_slot])

        def f_tasks():
            def done(h):
                f_send[f_slot] = h
            return forward_tasks(h_buf, weights, (a_buf, gp_buf, mid_buf, ab_buf, gpb_buf), done)

        def f_end():
            send(f_send.at[f_slot], f_sem.at[f_slot], cf, me != last, me + 1, h_all, got_h, acts_out, got_out)
            for copy in store_copies(cf):
                copy.start()

        def b_begin():
            load(g_buf.at[0], g_buf.at[0], g_sem).wait()
            load(gp_now, gp_now, gp_sem.at[b_side]).wait()
            load(gpb_now, gpb_now, gpb_sem.at[b_side]).wait()

            @pl.when(cb >= SLOTS)
            def _():
                sent(b_send.at[b_slot], b_sem.at[b_slot])

        def b_tasks():
            def done(g):
                b_send[b_slot] = g
            return backward_tasks(g_now, weights, (gp_now, gpb_now), (dzb_buf, gmid_buf, dz_buf), done)

        def b_end():
            send(b_send.at[b_slot], b_sem.at[b_slot], cb, me != 0, me - 1, g_all, got_g, grad_in, got_gin)

        @pl.when(has_f & has_b)
        def _():
            f_begin()
            b_begin()
            run_tasks(FB_ORDER, f_tasks() | b_tasks())
            b_end()
            f_end()

        @pl.when(has_f & jnp.logical_not(has_b))
        def _():
            f_begin()
            run_tasks(F_ORDER, f_tasks())
            f_end()

        @pl.when(has_b & jnp.logical_not(has_f))
        def _():
            b_begin()
            run_tasks(B_ORDER, b_tasks())
            b_end()

        steady = valid(cf + 1)

        @pl.when(steady)
        def _():
            fetch_g(cb + 1)
            fetch_h(cf + 1)

        @pl.when(has_b)
        def _():
            for k, buf in enumerate((h_in, a_in, mid_in, ab_in)):
                load(buf, buf, w_sem.at[k]).wait()
            add_product(dwb, ab_in, g_now, 256)
            add_product(dub, mid_in, dzb_buf, 256)
            add_product(dwa, a_in, gmid_buf, 256)
            add_product(dua, h_in, dz_buf, 256)

        @pl.when(jnp.logical_not(steady))
        def _():
            fetch_g(cb + 1)
        return 0

    lax.fori_loop(0, chunks + 2 * span + LAG, step, 0)

    finals = [load(src, dst, param_sem.at[k]) for k, (src, dst) in enumerate(
        [(dua, dua_hbm), (dwa, dwa_hbm), (dub, dub_hbm), (dwb, dwb_hbm)])]
    for copy in finals:
        copy.start()
    for slot in range(SLOTS):
        sent(f_send.at[slot], f_sem.at[slot])
        sent(b_send.at[slot], b_sem.at[slot])

    def settle(k, _):
        @pl.when(me != 0)
        def _():
            load(acts.at[k], acts.at[k], feed_h_sem.at[k]).wait()
            arrival(grad_in, k, got_gin).wait_recv()

        @pl.when(me != last)
        def _():
            load(gout.at[k], gout.at[k], feed_g_sem.at[k]).wait()
            arrival(acts_out, k, got_out).wait_recv()
        return 0

    lax.fori_loop(0, own, settle, 0)
    for copy in finals:
        copy.wait()


def run_stages(axis, stages, acts, gout, ua, wa, ub, wb):
    tokens, width = acts.shape
    own = tokens // ROWS
    chunks = own * stages
    wide, narrow = ua.shape[1], ub.shape[1]
    bf, f32 = jnp.bfloat16, jnp.float32
    shape = jax.ShapeDtypeStruct
    outs = [
        shape((own, ROWS, width), bf), shape((own, ROWS, width), bf),
        shape(ua.shape, f32), shape(wa.shape, f32), shape(ub.shape, f32), shape(wb.shape, f32),
        shape((chunks, ROWS, width), bf), shape((chunks, ROWS, width), bf), shape((chunks, ROWS, width), bf),
        shape((chunks, ROWS, wide), bf), shape((chunks, ROWS, wide), f32),
        shape((chunks, ROWS, narrow), bf), shape((chunks, ROWS, narrow), f32),
    ]
    vm, dma = pltpu.VMEM, pltpu.SemaphoreType.DMA
    tok, wid, nar = (ROWS, width), (ROWS, wide), (ROWS, narrow)
    scratch = [
        vm(ua.shape, bf), vm(wa.shape, bf), vm(ub.shape, bf), vm(wb.shape, bf),
        vm(ua.shape, f32), vm(wa.shape, f32), vm(ub.shape, f32), vm(wb.shape, f32),
        vm(tok, bf), vm(wid, bf), vm(wid, f32), vm(tok, bf), vm(nar, bf), vm(nar, f32), vm((SLOTS,) + tok, bf),
        vm((2,) + tok, bf), vm((2,) + wid, f32), vm((2,) + nar, f32), vm(nar, bf), vm(tok, bf), vm(wid, bf), vm((SLOTS,) + tok, bf),
        vm(wid, bf), vm(tok, bf), vm(tok, bf), vm(nar, bf),
        dma((chunks,)), dma((chunks,)), dma((own,)), dma((own,)), dma((SLOTS,)), dma((SLOTS,)), dma((own,)), dma((own,)),
        dma, dma, dma((2,)), dma((2,)), dma((4,)), dma((5,)), dma((4,)),
    ]
    results = pl.pallas_call(
        functools.partial(kernel, axis),
        out_shape=outs,
        in_specs=[ANY] * 6,
        out_specs=[ANY] * len(outs),
        scratch_shapes=scratch,
        compiler_params=pltpu.CompilerParams(vmem_limit_bytes=VMEM_LIMIT, has_side_effects=True),
    )(acts.reshape(own, ROWS, width), gout.reshape(own, ROWS, width), ua, wa, ub, wb)
    return results[:6]


def solution(mesh):
    tok_spec = P(('data', 'stage'))
    row_spec = P('stage')
    stages = mesh.shape['stage']

    def device_body(acts_in, grad_out, w_up_a, w_down_a, w_up_b, w_down_b):
        tokens, width = acts_in.shape[0] * acts_in.shape[1], acts_in.shape[2]
        out, gin, dua, dwa, dub, dwb = run_stages(
            'stage', stages, acts_in.reshape(tokens, width), grad_out.reshape(tokens, width),
            w_up_a[0], w_down_a[0], w_up_b[0], w_down_b[0])
        return (out.reshape(acts_in.shape), gin.reshape(acts_in.shape), dua[None], dwa[None], dub[None], dwb[None])

    return jax.shard_map(device_body, mesh=mesh, in_specs=(tok_spec, tok_spec, row_spec, row_spec, row_spec, row_spec), out_specs=(tok_spec,) * 6, check_vma=False)
```

```python
import functools

import jax
import jax.numpy as jnp
from jax import lax
from jax.experimental import pallas as pl
from jax.experimental.pallas import tpu as pltpu
from jax.sharding import PartitionSpec as P

MESH = pl.DeviceIdType.MESH
ANY = pl.BlockSpec(memory_space=pl.ANY)
VMEM_LIMIT = 67043328

GELU_C = 0.7978845608028654
GELU_K = 0.044715

ROWS = 256
HOP = 2
LAG = 2
SLOTS = 4
WIDE_COLS = 512
F_ORDER = 'zzczczczczccyo'
B_ORDER = 'dmxxpxpxpxpxpp'
FB_ORDER = 'zdmzxzcxpzcxpzcxpzccpxcxpypo'

NT = (((1,), (1,)), ((), ()))
TN = (((0,), (0,)), ((), ()))


def mm(lhs, rhs, dims=(((1,), (0,)), ((), ()))):
    return lax.dot_general(lhs, rhs, dims, preferred_element_type=jnp.float32)


def gelu_and_slope(z):
    zz = z * z
    half = 0.5 + 0.5 * jnp.tanh(z * (GELU_C + (GELU_C * GELU_K) * zz))
    act = z * half
    return act, half + act * (1.0 - half) * (2.0 * GELU_C + (6.0 * GELU_C * GELU_K) * zz)


def blocks(size, width):
    return [slice(start, min(start + width, size)) for start in range(0, size, width)]


def forward_tasks(h, weights, saved, done):
    ua, wa, ub, wb = weights
    a_buf, gp_buf, mid_buf, ab_buf, gpb_buf = saved
    cols = blocks(ua.shape[1], WIDE_COLS)

    def wide_up():
        for part in cols:
            act, slope = gelu_and_slope(mm(h[...], ua[:, part]))
            a_buf[:, part] = act.astype(jnp.bfloat16)
            gp_buf[:, part] = slope
            yield

    def wide_down():
        total = 0.0
        for k, part in enumerate(cols):
            product = mm(a_buf[:, part], wa[part, :])
            total = product if k == 0 else total + product
            if k == len(cols) - 1:
                mid_buf[...] = (h[...].astype(jnp.float32) + total).astype(jnp.bfloat16)
            yield

    def narrow_up():
        act, slope = gelu_and_slope(mm(mid_buf[...], ub[...]))
        ab_buf[...] = act.astype(jnp.bfloat16)
        gpb_buf[...] = slope
        yield

    def narrow_down():
        done((mid_buf[...].astype(jnp.float32) + mm(ab_buf[...], wb[...])).astype(jnp.bfloat16))
        yield

    return dict(z=wide_up(), c=wide_down(), y=narrow_up(), o=narrow_down())


def backward_tasks(g, weights, slopes, kept, done):
    ua, wa, ub, wb = weights
    gp_buf, gpb_buf = slopes
    dzb_buf, gmid_buf, dz_buf = kept
    cols = blocks(wa.shape[0], WIDE_COLS)

    def narrow_down():
        dzb_buf[...] = (mm(g[...], wb[...], NT) * gpb_buf[...]).astype(jnp.bfloat16)
        yield

    def narrow_up():
        gmid_buf[...] = (g[...].astype(jnp.float32) + mm(dzb_buf[...], ub[...], NT)).astype(jnp.bfloat16)
        yield

    def wide_down():
        for part in cols:
            dz_buf[:, part] = (mm(gmid_buf[...], wa[part, :], NT) * gp_buf[:, part]).astype(jnp.bfloat16)
            yield

    def wide_up():
        total = 0.0
        for k, part in enumerate(cols):
            product = mm(dz_buf[:, part], ua[:, part], NT)
            total = product if k == 0 else total + product
            if k == len(cols) - 1:
                done((gmid_buf[...].astype(jnp.float32) + total).astype(jnp.bfloat16))
            yield

    return dict(d=narrow_down(), m=narrow_up(), x=wide_down(), p=wide_up())


def run_tasks(order, tasks):
    for name in order:
        next(tasks[name])


def add_product(total, lhs, rhs, width):
    for rows in blocks(total.shape[0], width):
        total[rows, :] += mm(lhs[:, rows].T, rhs[...])


def kernel(
    axis, acts, gout, ua_hbm, wa_hbm, ub_hbm, wb_hbm,
    acts_out, grad_in, dua_hbm, dwa_hbm, dub_hbm, dwb_hbm,
    h_all, g_all, relay, mid_all, a_all, gp_all, ab_all, gpb_all,
    ua, wa, ub, wb, dua, dwa, dub, dwb,
    h_buf, a_buf, gp_buf, mid_buf, ab_buf, gpb_buf, f_send,
    g_buf, gp_in, gpb_in, dzb_buf, gmid_buf, dz_buf, b_send,
    a_in, h_in, mid_in, ab_in,
    got_h, got_g, got_out, got_gin, f_sem, b_sem, feed_h_sem, feed_g_sem, got_relay, relay_sem,
    h_sem, g_sem, gp_sem, gpb_sem, w_sem, st_sem, param_sem,
):
    me = lax.axis_index(axis)
    stages = lax.axis_size(axis)
    last = stages - 1
    own = acts.shape[0]
    chunks = own * stages

    def offset(stage):
        return HOP * stage + stage // 2

    span = offset(last)

    weights = (ua, wa, ub, wb)

    def fwd_chunk(t):
        return t - offset(me)

    def bwd_chunk(t):
        return t - 2 * span - LAG + offset(me)

    def valid(c):
        return (c >= 0) & (c < chunks)

    def on(device):
        return dict(device_id={axis: device}, device_id_type=MESH)

    def load(src, dst, sem):
        return pltpu.make_async_copy(src, dst, sem)

    params = [load(src, dst, param_sem.at[k]) for k, (src, dst) in enumerate(
        [(ua_hbm, ua), (wa_hbm, wa), (ub_hbm, ub), (wb_hbm, wb)])]
    for copy in params:
        copy.start()

    def arrival(buf, c, sem):
        return pltpu.make_async_remote_copy(buf.at[c], buf.at[c], sem.at[c], sem.at[c], **on(me))

    def fetch_h(c):
        @pl.when(valid(c))
        def _():
            local = (me == 0) & (c < own)

            @pl.when(local)
            def _():
                load(acts.at[lax.rem(c, own)], h_buf, h_sem).start()

            @pl.when(jnp.logical_not(local))
            def _():
                arrival(h_all, c, got_h).wait_recv()
                load(h_all.at[c], h_buf, h_sem).start()

    def fetch_slopes(c):
        @pl.when(valid(c))
        def _():
            side = lax.rem(c, 2)
            load(gp_all.at[c], gp_in.at[side], gp_sem.at[side]).start()
            load(gpb_all.at[c], gpb_in.at[side], gpb_sem.at[side]).start()

    def fetch_g(c):
        @pl.when(valid(c))
        def _():
            local = (me == last) & (c >= chunks - own)
            buf = g_buf.at[lax.rem(c, 2)]

            @pl.when(local)
            def _():
                load(gout.at[lax.rem(c, own)], buf, g_sem).start()

            @pl.when(jnp.logical_not(local))
            def _():
                arrival(g_all, c, got_g).wait_recv()
                load(g_all.at[c], buf, g_sem).start()

    def fetch_weight_operands(c):
        local_h = (me == 0) & (c < own)

        @pl.when(local_h)
        def _():
            load(acts.at[lax.rem(c, own)], h_in, w_sem.at[0]).start()

        @pl.when(jnp.logical_not(local_h))
        def _():
            load(h_all.at[c], h_in, w_sem.at[0]).start()
        load(a_all.at[c], a_in, w_sem.at[1]).start()
        load(mid_all.at[c], mid_in, w_sem.at[2]).start()
        load(ab_all.at[c], ab_in, w_sem.at[3]).start()

    def send(slot_ref, sem, c, inner, next_device, next_all, next_sem, home_out, home_sem):
        home = c // own
        spot = lax.rem(c, own)

        @pl.when(inner)
        def _():
            pltpu.make_async_remote_copy(slot_ref, next_all.at[c], sem, next_sem.at[c], **on(next_device)).start()

        @pl.when(jnp.logical_not(inner) & (home != me))
        def _():
            pltpu.make_async_remote_copy(slot_ref, home_out.at[spot], sem, home_sem.at[spot], **on(home)).start()

        @pl.when(jnp.logical_not(inner) & (home == me))
        def _():
            load(slot_ref, home_out.at[spot], sem).start()

    def sent(slot_ref, sem):
        load(slot_ref, slot_ref, sem).wait()

    half = stages // 2
    first_half, edge = me < half, half // 2

    def feed_acts(t):
        by_way = (me >= edge) & first_half
        lead = jnp.where(me == 1, own, jnp.where(by_way, 2 * own, own + own // 2))
        spot = t + lead - own * me
        due = (me != 0) & (spot >= 0) & (spot < own)

        @pl.when(due & jnp.logical_not(by_way))
        def _():
            pltpu.make_async_remote_copy(acts.at[spot], h_all.at[own * me + spot], feed_h_sem.at[spot], got_h.at[own * me + spot], **on(0)).start()

        @pl.when(due & by_way)
        def _():
            pltpu.make_async_remote_copy(acts.at[spot], relay.at[spot], feed_h_sem.at[spot], got_relay.at[spot], **on(me + half)).start()

        spot = t + own + own // 4 - own * (me - half)

        @pl.when((me >= half + edge) & (spot >= 0) & (spot < own))
        def _():
            arrival(relay, spot, got_relay).wait_recv()
            c = own * (me - half) + spot
            pltpu.make_async_remote_copy(relay.at[spot], h_all.at[c], relay_sem.at[spot], got_h.at[c], **on(0)).start()

    def feed_grads(t):
        by_way = jnp.logical_not(first_half) & (me < half + edge)
        spot = t - own // 2 - own * me
        due = (me != last) & (spot >= 0) & (spot < own)

        @pl.when(due & jnp.logical_not(by_way))
        def _():
            pltpu.make_async_remote_copy(gout.at[spot], g_all.at[own * me + spot], feed_g_sem.at[spot], got_g.at[own * me + spot], **on(last)).start()

        @pl.when(due & by_way)
        def _():
            pltpu.make_async_remote_copy(gout.at[spot], relay.at[spot], feed_g_sem.at[spot], got_relay.at[spot], **on(me - half)).start()

        spot = t - 2 * own - own * (me + half)

        @pl.when((me < edge) & (spot >= 0) & (spot < own))
        def _():
            arrival(relay, spot, got_relay).wait_recv()
            c = own * (me + half) + spot
            pltpu.make_async_remote_copy(relay.at[spot], g_all.at[c], relay_sem.at[spot], got_g.at[c], **on(last)).start()

    def store_copies(c):
        pairs = [(a_buf, a_all), (gp_buf, gp_all), (mid_buf, mid_all), (ab_buf, ab_all), (gpb_buf, gpb_all)]
        return [load(src, dst.at[c], st_sem.at[k]) for k, (src, dst) in enumerate(pairs)]

    fetch_h(fwd_chunk(0))
    for total in (dua, dwa, dub, dwb):
        total[...] = jnp.zeros_like(total)
    for copy in params:
        copy.wait()

    def step(t, _):
        cf, cb = fwd_chunk(t), bwd_chunk(t)
        has_f, has_b = valid(cf), valid(cb)
        feed_acts(t)
        feed_grads(t)

        @pl.when(valid(cf - 1))
        def _():
            for copy in store_copies(cf - 1):
                copy.wait()

        fetch_slopes(cb + 1)

        @pl.when(has_b)
        def _():
            fetch_weight_operands(cb)

        b_side = lax.rem(jnp.maximum(cb, 0), 2)
        g_now, gp_now, gpb_now = g_buf.at[b_side], gp_in.at[b_side], gpb_in.at[b_side]
        f_slot, b_slot = lax.rem(cf, SLOTS), lax.rem(cb, SLOTS)

        def f_begin():
            load(h_buf, h_buf, h_sem).wait()

            @pl.when(cf >= SLOTS)
            def _():
                sent(f_send.at[f_slot], f_sem.at[f_slot])

        def f_tasks():
            def done(h):
                f_send[f_slot] = h
            return forward_tasks(h_buf, weights, (a_buf, gp_buf, mid_buf, ab_buf, gpb_buf), done)

        def f_end():
            send(f_send.at[f_slot], f_sem.at[f_slot], cf, me != last, me + 1, h_all, got_h, acts_out, got_out)
            for copy in store_copies(cf):
                copy.start()

        def b_begin():
            load(g_buf.at[0], g_buf.at[0], g_sem).wait()
            load(gp_now, gp_now, gp_sem.at[b_side]).wait()
            load(gpb_now, gpb_now, gpb_sem.at[b_side]).wait()

            @pl.when(cb >= SLOTS)
            def _():
                sent(b_send.at[b_slot], b_sem.at[b_slot])

        def b_tasks():
            def done(g):
                b_send[b_slot] = g
            return backward_tasks(g_now, weights, (gp_now, gpb_now), (dzb_buf, gmid_buf, dz_buf), done)

        def b_end():
            send(b_send.at[b_slot], b_sem.at[b_slot], cb, me != 0, me - 1, g_all, got_g, grad_in, got_gin)

        @pl.when(has_f & has_b)
        def _():
            f_begin()
            b_begin()
            run_tasks(FB_ORDER, f_tasks() | b_tasks())
            b_end()
            f_end()

        @pl.when(has_f & jnp.logical_not(has_b))
        def _():
            f_begin()
            run_tasks(F_ORDER, f_tasks())
            f_end()

        @pl.when(has_b & jnp.logical_not(has_f))
        def _():
            b_begin()
            run_tasks(B_ORDER, b_tasks())
            b_end()

        steady = valid(cf + 1)

        @pl.when(steady)
        def _():
            fetch_g(cb + 1)
            fetch_h(cf + 1)

        @pl.when(has_b)
        def _():
            for k, buf in enumerate((h_in, a_in, mid_in, ab_in)):
                load(buf, buf, w_sem.at[k]).wait()
            add_product(dwb, ab_in, g_now, 256)
            add_product(dub, mid_in, dzb_buf, 256)
            add_product(dwa, a_in, gmid_buf, 256)
            add_product(dua, h_in, dz_buf, 256)

        @pl.when(jnp.logical_not(steady))
        def _():
            fetch_g(cb + 1)
        return 0

    lax.fori_loop(0, chunks + 2 * span + LAG, step, 0)

    finals = [load(src, dst, param_sem.at[k]) for k, (src, dst) in enumerate(
        [(dua, dua_hbm), (dwa, dwa_hbm), (dub, dub_hbm), (dwb, dwb_hbm)])]
    for copy in finals:
        copy.start()
    for slot in range(SLOTS):
        sent(f_send.at[slot], f_sem.at[slot])
        sent(b_send.at[slot], b_sem.at[slot])

    def settle(k, _):
        @pl.when(me != 0)
        def _():
            load(acts.at[k], acts.at[k], feed_h_sem.at[k]).wait()
            arrival(grad_in, k, got_gin).wait_recv()

        @pl.when(me != last)
        def _():
            load(gout.at[k], gout.at[k], feed_g_sem.at[k]).wait()
            arrival(acts_out, k, got_out).wait_recv()

        @pl.when((me < edge) | (me >= half + edge))
        def _():
            load(relay.at[k], relay.at[k], relay_sem.at[k]).wait()
        return 0

    lax.fori_loop(0, own, settle, 0)
    for copy in finals:
        copy.wait()


def run_stages(axis, stages, acts, gout, ua, wa, ub, wb):
    tokens, width = acts.shape
    own = tokens // ROWS
    chunks = own * stages
    wide, narrow = ua.shape[1], ub.shape[1]
    bf, f32 = jnp.bfloat16, jnp.float32
    shape = jax.ShapeDtypeStruct
    outs = [
        shape((own, ROWS, width), bf), shape((own, ROWS, width), bf),
        shape(ua.shape, f32), shape(wa.shape, f32), shape(ub.shape, f32), shape(wb.shape, f32),
        shape((chunks, ROWS, width), bf), shape((chunks, ROWS, width), bf), shape((own, ROWS, width), bf), shape((chunks, ROWS, width), bf),
        shape((chunks, ROWS, wide), bf), shape((chunks, ROWS, wide), f32),
        shape((chunks, ROWS, narrow), bf), shape((chunks, ROWS, narrow), f32),
    ]
    vm, dma = pltpu.VMEM, pltpu.SemaphoreType.DMA
    tok, wid, nar = (ROWS, width), (ROWS, wide), (ROWS, narrow)
    scratch = [
        vm(ua.shape, bf), vm(wa.shape, bf), vm(ub.shape, bf), vm(wb.shape, bf),
        vm(ua.shape, f32), vm(wa.shape, f32), vm(ub.shape, f32), vm(wb.shape, f32),
        vm(tok, bf), vm(wid, bf), vm(wid, f32), vm(tok, bf), vm(nar, bf), vm(nar, f32), vm((SLOTS,) + tok, bf),
        vm((2,) + tok, bf), vm((2,) + wid, f32), vm((2,) + nar, f32), vm(nar, bf), vm(tok, bf), vm(wid, bf), vm((SLOTS,) + tok, bf),
        vm(wid, bf), vm(tok, bf), vm(tok, bf), vm(nar, bf),
        dma((chunks,)), dma((chunks,)), dma((own,)), dma((own,)), dma((SLOTS,)), dma((SLOTS,)), dma((own,)), dma((own,)), dma((own,)), dma((own,)),
        dma, dma, dma((2,)), dma((2,)), dma((4,)), dma((5,)), dma((4,)),
    ]
    results = pl.pallas_call(
        functools.partial(kernel, axis),
        out_shape=outs,
        in_specs=[ANY] * 6,
        out_specs=[ANY] * len(outs),
        scratch_shapes=scratch,
        compiler_params=pltpu.CompilerParams(vmem_limit_bytes=VMEM_LIMIT, has_side_effects=True),
    )(acts.reshape(own, ROWS, width), gout.reshape(own, ROWS, width), ua, wa, ub, wb)
    return results[:6]


def solution(mesh):
    tok_spec = P(('data', 'stage'))
    row_spec = P('stage')
    stages = mesh.shape['stage']

    def device_body(acts_in, grad_out, w_up_a, w_down_a, w_up_b, w_down_b):
        tokens, width = acts_in.shape[0] * acts_in.shape[1], acts_in.shape[2]
        out, gin, dua, dwa, dub, dwb = run_stages(
            'stage', stages, acts_in.reshape(tokens, width), grad_out.reshape(tokens, width),
            w_up_a[0], w_down_a[0], w_up_b[0], w_down_b[0])
        return (out.reshape(acts_in.shape), gin.reshape(acts_in.shape), dua[None], dwa[None], dub[None], dwb[None])

    return jax.shard_map(device_body, mesh=mesh, in_specs=(tok_spec, tok_spec, row_spec, row_spec, row_spec, row_spec), out_specs=(tok_spec,) * 6, check_vma=False)
```

```python
import functools

import jax
import jax.numpy as jnp
from jax import lax
from jax.experimental import pallas as pl
from jax.experimental.pallas import tpu as pltpu
from jax.sharding import PartitionSpec as P

MESH = pl.DeviceIdType.MESH
ANY = pl.BlockSpec(memory_space=pl.ANY)
VMEM_LIMIT = 67043328

GELU_C = 0.7978845608028654
GELU_K = 0.044715

ROWS = 256
LAG = 2
SLOTS = 4
WIDE_COLS = 512
F_ORDER = 'zzczczczczccyo'
B_ORDER = 'dmxxpxpxpxpxpp'
FB_ORDER = 'zdmzxzcxpzcxpzcxpzccpxcxpypo'

NT = (((1,), (1,)), ((), ()))
TN = (((0,), (0,)), ((), ()))


def mm(lhs, rhs, dims=(((1,), (0,)), ((), ()))):
    return lax.dot_general(lhs, rhs, dims, preferred_element_type=jnp.float32)


def gelu_and_slope(z):
    zz = z * z
    half = 0.5 + 0.5 * jnp.tanh(z * (GELU_C + (GELU_C * GELU_K) * zz))
    act = z * half
    return act, half + act * (1.0 - half) * (2.0 * GELU_C + (6.0 * GELU_C * GELU_K) * zz)


def blocks(size, width):
    return [slice(start, min(start + width, size)) for start in range(0, size, width)]


def forward_tasks(h, weights, saved, done):
    ua, wa, ub, wb = weights
    a_buf, gp_buf, mid_buf, ab_buf, gpb_buf = saved
    cols = blocks(ua.shape[1], WIDE_COLS)

    def wide_up():
        for part in cols:
            act, slope = gelu_and_slope(mm(h[...], ua[:, part]))
            a_buf[:, part] = act.astype(jnp.bfloat16)
            gp_buf[:, part] = slope
            yield

    def wide_down():
        total = 0.0
        for k, part in enumerate(cols):
            product = mm(a_buf[:, part], wa[part, :])
            total = product if k == 0 else total + product
            if k == len(cols) - 1:
                mid_buf[...] = (h[...].astype(jnp.float32) + total).astype(jnp.bfloat16)
            yield

    def narrow_up():
        act, slope = gelu_and_slope(mm(mid_buf[...], ub[...]))
        ab_buf[...] = act.astype(jnp.bfloat16)
        gpb_buf[...] = slope
        yield

    def narrow_down():
        done((mid_buf[...].astype(jnp.float32) + mm(ab_buf[...], wb[...])).astype(jnp.bfloat16))
        yield

    return dict(z=wide_up(), c=wide_down(), y=narrow_up(), o=narrow_down())


def backward_tasks(g, weights, slopes, kept, done):
    ua, wa, ub, wb = weights
    gp_buf, gpb_buf = slopes
    dzb_buf, gmid_buf, dz_buf = kept
    cols = blocks(wa.shape[0], WIDE_COLS)

    def narrow_down():
        dzb_buf[...] = (mm(g[...], wb[...], NT) * gpb_buf[...]).astype(jnp.bfloat16)
        yield

    def narrow_up():
        gmid_buf[...] = (g[...].astype(jnp.float32) + mm(dzb_buf[...], ub[...], NT)).astype(jnp.bfloat16)
        yield

    def wide_down():
        for part in cols:
            dz_buf[:, part] = (mm(gmid_buf[...], wa[part, :], NT) * gp_buf[:, part]).astype(jnp.bfloat16)
            yield

    def wide_up():
        total = 0.0
        for k, part in enumerate(cols):
            product = mm(dz_buf[:, part], ua[:, part], NT)
            total = product if k == 0 else total + product
            if k == len(cols) - 1:
                done((gmid_buf[...].astype(jnp.float32) + total).astype(jnp.bfloat16))
            yield

    return dict(d=narrow_down(), m=narrow_up(), x=wide_down(), p=wide_up())


def run_tasks(order, tasks):
    for name in order:
        next(tasks[name])


def add_product(total, lhs, rhs, width):
    for rows in blocks(total.shape[0], width):
        total[rows, :] += mm(lhs[:, rows].T, rhs[...])


def kernel(
    axis, acts, gout, ua_hbm, wa_hbm, ub_hbm, wb_hbm,
    acts_out, grad_in, dua_hbm, dwa_hbm, dub_hbm, dwb_hbm,
    h_all, g_all, relay, mid_all, a_all, gp_all, ab_all, gpb_all,
    ua, wa, ub, wb, dua, dwa, dub, dwb,
    h_buf, a_buf, gp_buf, mid_buf, ab_buf, gpb_buf, f_send,
    g_buf, gp_in, gpb_in, dzb_buf, gmid_buf, dz_buf, b_send,
    a_in, h_in, mid_in, ab_in,
    got_h, got_g, got_out, got_gin, f_sem, b_sem, feed_h_sem, feed_g_sem, got_relay, relay_sem,
    h_sem, g_sem, gp_sem, gpb_sem, w_sem, st_sem, param_sem,
):
    me = lax.axis_index(axis)
    stages = lax.axis_size(axis)
    last = stages - 1
    own = acts.shape[0]
    chunks = own * stages

    def ahead(stage):
        return stage + stage // 2

    def behind(stage):
        return 2 * stage + stage // 2

    span = ahead(last) + LAG + behind(last)

    weights = (ua, wa, ub, wb)

    def fwd_chunk(t):
        return t - ahead(me)

    def bwd_chunk(t):
        return t - span + behind(me)

    def valid(c):
        return (c >= 0) & (c < chunks)

    def on(device):
        return dict(device_id={axis: device}, device_id_type=MESH)

    def load(src, dst, sem):
        return pltpu.make_async_copy(src, dst, sem)

    params = [load(src, dst, param_sem.at[k]) for k, (src, dst) in enumerate(
        [(ua_hbm, ua), (wa_hbm, wa), (ub_hbm, ub), (wb_hbm, wb)])]
    for copy in params:
        copy.start()

    def arrival(buf, c, sem):
        return pltpu.make_async_remote_copy(buf.at[c], buf.at[c], sem.at[c], sem.at[c], **on(me))

    def fetch_h(c):
        @pl.when(valid(c))
        def _():
            local = (me == 0) & (c < own)

            side = lax.rem(c, 2)

            @pl.when(local)
            def _():
                load(acts.at[lax.rem(c, own)], h_buf.at[side], h_sem.at[side]).start()

            @pl.when(jnp.logical_not(local))
            def _():
                arrival(h_all, c, got_h).wait_recv()
                load(h_all.at[c], h_buf.at[side], h_sem.at[side]).start()

    def fetch_slopes(c):
        @pl.when(valid(c))
        def _():
            side = lax.rem(c, 2)
            load(gp_all.at[c], gp_in.at[side], gp_sem.at[side]).start()
            load(gpb_all.at[c], gpb_in.at[side], gpb_sem.at[side]).start()

    def fetch_g(c):
        @pl.when(valid(c))
        def _():
            local = (me == last) & (c >= chunks - own)
            buf = g_buf.at[lax.rem(c, 2)]

            @pl.when(local)
            def _():
                load(gout.at[lax.rem(c, own)], buf, g_sem).start()

            @pl.when(jnp.logical_not(local))
            def _():
                arrival(g_all, c, got_g).wait_recv()
                load(g_all.at[c], buf, g_sem).start()

    def fetch_weight_operands(c):
        local_h = (me == 0) & (c < own)

        @pl.when(local_h)
        def _():
            load(acts.at[lax.rem(c, own)], h_in, w_sem.at[0]).start()

        @pl.when(jnp.logical_not(local_h))
        def _():
            load(h_all.at[c], h_in, w_sem.at[0]).start()
        load(a_all.at[c], a_in, w_sem.at[1]).start()
        load(mid_all.at[c], mid_in, w_sem.at[2]).start()
        load(ab_all.at[c], ab_in, w_sem.at[3]).start()

    def send(slot_ref, sem, c, inner, next_device, next_all, next_sem, home_out, home_sem):
        home = c // own
        spot = lax.rem(c, own)

        @pl.when(inner)
        def _():
            pltpu.make_async_remote_copy(slot_ref, next_all.at[c], sem, next_sem.at[c], **on(next_device)).start()

        @pl.when(jnp.logical_not(inner) & (home != me))
        def _():
            pltpu.make_async_remote_copy(slot_ref, home_out.at[spot], sem, home_sem.at[spot], **on(home)).start()

        @pl.when(jnp.logical_not(inner) & (home == me))
        def _():
            load(slot_ref, home_out.at[spot], sem).start()

    def sent(slot_ref, sem):
        load(slot_ref, slot_ref, sem).wait()

    half = stages // 2
    first_half, edge = me < half, half // 2

    def feed_acts(t):
        by_way = (me >= edge) & first_half
        lead = jnp.where(first_half, own * me, own + own // 2)
        spot = t + lead - own * me
        due = (me != 0) & (spot >= 0) & (spot < own)

        @pl.when(due & jnp.logical_not(by_way))
        def _():
            pltpu.make_async_remote_copy(acts.at[spot], h_all.at[own * me + spot], feed_h_sem.at[spot], got_h.at[own * me + spot], **on(0)).start()

        @pl.when(due & by_way)
        def _():
            pltpu.make_async_remote_copy(acts.at[spot], relay.at[spot], feed_h_sem.at[spot], got_relay.at[spot], **on(me + half)).start()

        spot = t - me - 1

        @pl.when((me >= half + edge) & (spot >= 0) & (spot < own))
        def _():
            arrival(relay, spot, got_relay).wait_recv()
            c = own * (me - half) + spot
            pltpu.make_async_remote_copy(relay.at[spot], h_all.at[c], relay_sem.at[spot], got_h.at[c], **on(0)).start()

    def feed_grads(t):
        by_way = jnp.logical_not(first_half) & (me < half + edge)
        spot = t - jnp.where(by_way, 0, own // 2) - own * me
        due = (me != last) & (spot >= 0) & (spot < own)

        @pl.when(due & jnp.logical_not(by_way))
        def _():
            pltpu.make_async_remote_copy(gout.at[spot], g_all.at[own * me + spot], feed_g_sem.at[spot], got_g.at[own * me + spot], **on(last)).start()

        @pl.when(due & by_way)
        def _():
            pltpu.make_async_remote_copy(gout.at[spot], relay.at[spot], feed_g_sem.at[spot], got_relay.at[spot], **on(me - half)).start()

        spot = t - own - own // 2 - own * (me + half)

        @pl.when((me < edge) & (spot >= 0) & (spot < own))
        def _():
            arrival(relay, spot, got_relay).wait_recv()
            c = own * (me + half) + spot
            pltpu.make_async_remote_copy(relay.at[spot], g_all.at[c], relay_sem.at[spot], got_g.at[c], **on(last)).start()

    def wide_saves(c):
        pairs = [(a_buf, a_all), (gp_buf, gp_all), (mid_buf, mid_all)]
        return [load(src, dst.at[c], st_sem.at[k]) for k, (src, dst) in enumerate(pairs)]

    def narrow_saves(c):
        pairs = [(ab_buf, ab_all), (gpb_buf, gpb_all)]
        return [load(src, dst.at[c], st_sem.at[k + 3]) for k, (src, dst) in enumerate(pairs)]

    def start(copies):
        for copy in copies:
            copy.start()

    def saved(c, copies):
        @pl.when(valid(c))
        def _():
            for copy in copies(c):
                copy.wait()

    fetch_h(fwd_chunk(0))
    for total in (dua, dwa, dub, dwb):
        total[...] = jnp.zeros_like(total)
    for copy in params:
        copy.wait()

    def step(t, _):
        cf, cb = fwd_chunk(t), bwd_chunk(t)
        has_f, has_b = valid(cf), valid(cb)
        feed_acts(t)
        feed_grads(t)

        f_alone = has_f & jnp.logical_not(has_b)
        late = f_alone & (cb + 1 < 0)
        saved(cf - 1, wide_saves)

        @pl.when(jnp.logical_not(late))
        def _():
            saved(cf - 1, narrow_saves)

        fetch_slopes(cb + 1)

        @pl.when(me == 0)
        def _():
            fetch_h(cf + 1)

        @pl.when(has_b)
        def _():
            fetch_weight_operands(cb)

        b_side = lax.rem(jnp.maximum(cb, 0), 2)
        f_side = lax.rem(jnp.maximum(cf, 0), 2)
        h_now = h_buf.at[f_side]
        g_now, gp_now, gpb_now = g_buf.at[b_side], gp_in.at[b_side], gpb_in.at[b_side]
        f_slot, b_slot = lax.rem(cf, SLOTS), lax.rem(cb, SLOTS)

        def f_begin():
            load(h_now, h_now, h_sem.at[f_side]).wait()

            @pl.when(cf >= SLOTS)
            def _():
                sent(f_send.at[f_slot], f_sem.at[f_slot])

        def f_tasks():
            def done(h):
                f_send[f_slot] = h
            return forward_tasks(h_now, weights, (a_buf, gp_buf, mid_buf, ab_buf, gpb_buf), done)

        def f_end():
            send(f_send.at[f_slot], f_sem.at[f_slot], cf, me != last, me + 1, h_all, got_h, acts_out, got_out)

        def b_begin():
            load(g_buf.at[0], g_buf.at[0], g_sem).wait()
            load(gp_now, gp_now, gp_sem.at[b_side]).wait()
            load(gpb_now, gpb_now, gpb_sem.at[b_side]).wait()

            @pl.when(cb >= SLOTS)
            def _():
                sent(b_send.at[b_slot], b_sem.at[b_slot])

        def b_tasks():
            def done(g):
                b_send[b_slot] = g
            return backward_tasks(g_now, weights, (gp_now, gpb_now), (dzb_buf, gmid_buf, dz_buf), done)

        def b_end():
            send(b_send.at[b_slot], b_sem.at[b_slot], cb, me != 0, me - 1, g_all, got_g, grad_in, got_gin)

        @pl.when(has_f & has_b)
        def _():
            f_begin()
            b_begin()
            run_tasks(FB_ORDER, f_tasks() | b_tasks())
            b_end()
            f_end()
            start(wide_saves(cf) + narrow_saves(cf))

        @pl.when(f_alone)
        def _():
            tasks = f_tasks()
            f_begin()
            run_tasks(F_ORDER[:-2], tasks)
            start(wide_saves(cf))

            @pl.when(late)
            def _():
                saved(cf - 1, narrow_saves)
            run_tasks(F_ORDER[-2:], tasks)
            f_end()
            start(narrow_saves(cf))

        @pl.when(has_b & jnp.logical_not(has_f))
        def _():
            b_begin()
            run_tasks(B_ORDER, b_tasks())
            b_end()

        steady = valid(cf + 1)

        @pl.when(steady)
        def _():
            fetch_g(cb + 1)

            @pl.when(me != 0)
            def _():
                fetch_h(cf + 1)

        @pl.when(has_b)
        def _():
            for k, buf in enumerate((h_in, a_in, mid_in, ab_in)):
                load(buf, buf, w_sem.at[k]).wait()
            add_product(dwb, ab_in, g_now, 256)
            add_product(dub, mid_in, dzb_buf, 256)
            add_product(dwa, a_in, gmid_buf, 256)
            add_product(dua, h_in, dz_buf, 256)

        @pl.when(jnp.logical_not(steady))
        def _():
            fetch_g(cb + 1)
        return 0

    lax.fori_loop(0, chunks + span, step, 0)

    finals = [load(src, dst, param_sem.at[k]) for k, (src, dst) in enumerate(
        [(dua, dua_hbm), (dwa, dwa_hbm), (dub, dub_hbm), (dwb, dwb_hbm)])]
    for copy in finals:
        copy.start()
    for slot in range(SLOTS):
        sent(f_send.at[slot], f_sem.at[slot])
        sent(b_send.at[slot], b_sem.at[slot])

    def settle(k, _):
        @pl.when(me != 0)
        def _():
            load(acts.at[k], acts.at[k], feed_h_sem.at[k]).wait()
            arrival(grad_in, k, got_gin).wait_recv()

        @pl.when(me != last)
        def _():
            load(gout.at[k], gout.at[k], feed_g_sem.at[k]).wait()
            arrival(acts_out, k, got_out).wait_recv()

        @pl.when((me < edge) | (me >= half + edge))
        def _():
            load(relay.at[k], relay.at[k], relay_sem.at[k]).wait()
        return 0

    lax.fori_loop(0, own, settle, 0)
    for copy in finals:
        copy.wait()


def run_stages(axis, stages, acts, gout, ua, wa, ub, wb):
    tokens, width = acts.shape
    own = tokens // ROWS
    chunks = own * stages
    wide, narrow = ua.shape[1], ub.shape[1]
    bf, f32 = jnp.bfloat16, jnp.float32
    shape = jax.ShapeDtypeStruct
    outs = [
        shape((own, ROWS, width), bf), shape((own, ROWS, width), bf),
        shape(ua.shape, f32), shape(wa.shape, f32), shape(ub.shape, f32), shape(wb.shape, f32),
        shape((chunks, ROWS, width), bf), shape((chunks, ROWS, width), bf), shape((own, ROWS, width), bf), shape((chunks, ROWS, width), bf),
        shape((chunks, ROWS, wide), bf), shape((chunks, ROWS, wide), f32),
        shape((chunks, ROWS, narrow), bf), shape((chunks, ROWS, narrow), f32),
    ]
    vm, dma = pltpu.VMEM, pltpu.SemaphoreType.DMA
    tok, wid, nar = (ROWS, width), (ROWS, wide), (ROWS, narrow)
    scratch = [
        vm(ua.shape, bf), vm(wa.shape, bf), vm(ub.shape, bf), vm(wb.shape, bf),
        vm(ua.shape, f32), vm(wa.shape, f32), vm(ub.shape, f32), vm(wb.shape, f32),
        vm((2,) + tok, bf), vm(wid, bf), vm(wid, f32), vm(tok, bf), vm(nar, bf), vm(nar, f32), vm((SLOTS,) + tok, bf),
        vm((2,) + tok, bf), vm((2,) + wid, f32), vm((2,) + nar, f32), vm(nar, bf), vm(tok, bf), vm(wid, bf), vm((SLOTS,) + tok, bf),
        vm(wid, bf), vm(tok, bf), vm(tok, bf), vm(nar, bf),
        dma((chunks,)), dma((chunks,)), dma((own,)), dma((own,)), dma((SLOTS,)), dma((SLOTS,)), dma((own,)), dma((own,)), dma((own,)), dma((own,)),
        dma((2,)), dma, dma((2,)), dma((2,)), dma((4,)), dma((5,)), dma((4,)),
    ]
    results = pl.pallas_call(
        functools.partial(kernel, axis),
        out_shape=outs,
        in_specs=[ANY] * 6,
        out_specs=[ANY] * len(outs),
        scratch_shapes=scratch,
        compiler_params=pltpu.CompilerParams(vmem_limit_bytes=VMEM_LIMIT, has_side_effects=True),
    )(acts.reshape(own, ROWS, width), gout.reshape(own, ROWS, width), ua, wa, ub, wb)
    return results[:6]


def solution(mesh):
    tok_spec = P(('data', 'stage'))
    row_spec = P('stage')
    stages = mesh.shape['stage']

    def device_body(acts_in, grad_out, w_up_a, w_down_a, w_up_b, w_down_b):
        tokens, width = acts_in.shape[0] * acts_in.shape[1], acts_in.shape[2]
        out, gin, dua, dwa, dub, dwb = run_stages(
            'stage', stages, acts_in.reshape(tokens, width), grad_out.reshape(tokens, width),
            w_up_a[0], w_down_a[0], w_up_b[0], w_down_b[0])
        return (out.reshape(acts_in.shape), gin.reshape(acts_in.shape), dua[None], dwa[None], dub[None], dwb[None])

    return jax.shard_map(device_body, mesh=mesh, in_specs=(tok_spec, tok_spec, row_spec, row_spec, row_spec, row_spec), out_specs=(tok_spec,) * 6, check_vma=False)
```

```python
import functools

import jax
import jax.numpy as jnp
from jax import lax
from jax.experimental import pallas as pl
from jax.experimental.pallas import tpu as pltpu
from jax.sharding import PartitionSpec as P

MESH = pl.DeviceIdType.MESH
ANY = pl.BlockSpec(memory_space=pl.ANY)
VMEM_LIMIT = 67043328

GELU_C = 0.7978845608028654
GELU_K = 0.044715

ROWS = 256
LAG = 2
SLOTS = 4
WIDE_COLS = 512
F_ORDER = 'zzczczczczccyo'
B_ORDER = 'dmxxpxpxpxpxpp'
FB_ORDER = 'zdmzxzcxpzcxpzcxpzccpxcxpypo'

NT = (((1,), (1,)), ((), ()))
TN = (((0,), (0,)), ((), ()))


def mm(lhs, rhs, dims=(((1,), (0,)), ((), ()))):
    return lax.dot_general(lhs, rhs, dims, preferred_element_type=jnp.float32)


def gelu_and_slope(z):
    zz = z * z
    half = 0.5 + 0.5 * jnp.tanh(z * (GELU_C + (GELU_C * GELU_K) * zz))
    act = z * half
    return act, half + act * (1.0 - half) * (2.0 * GELU_C + (6.0 * GELU_C * GELU_K) * zz)


def blocks(size, width):
    return [slice(start, min(start + width, size)) for start in range(0, size, width)]


def forward_tasks(h, weights, saved, done):
    ua, wa, ub, wb = weights
    a_buf, gp_buf, mid_buf, ab_buf, gpb_buf = saved
    cols = blocks(ua.shape[1], WIDE_COLS)

    def wide_up():
        for part in cols:
            act, slope = gelu_and_slope(mm(h[...], ua[:, part]))
            a_buf[:, part] = act.astype(jnp.bfloat16)
            gp_buf[:, part] = slope
            yield

    def wide_down():
        total = 0.0
        for k, part in enumerate(cols):
            product = mm(a_buf[:, part], wa[part, :])
            total = product if k == 0 else total + product
            if k == len(cols) - 1:
                mid_buf[...] = (h[...].astype(jnp.float32) + total).astype(jnp.bfloat16)
            yield

    def narrow_up():
        act, slope = gelu_and_slope(mm(mid_buf[...], ub[...]))
        ab_buf[...] = act.astype(jnp.bfloat16)
        gpb_buf[...] = slope
        yield

    def narrow_down():
        done((mid_buf[...].astype(jnp.float32) + mm(ab_buf[...], wb[...])).astype(jnp.bfloat16))
        yield

    return dict(z=wide_up(), c=wide_down(), y=narrow_up(), o=narrow_down())


def backward_tasks(g, weights, slopes, kept, done):
    ua, wa, ub, wb = weights
    gp_buf, gpb_buf = slopes
    dzb_buf, gmid_buf, dz_buf = kept
    cols = blocks(wa.shape[0], WIDE_COLS)

    def narrow_down():
        dzb_buf[...] = (mm(g[...], wb[...], NT) * gpb_buf[...]).astype(jnp.bfloat16)
        yield

    def narrow_up():
        gmid_buf[...] = (g[...].astype(jnp.float32) + mm(dzb_buf[...], ub[...], NT)).astype(jnp.bfloat16)
        yield

    def wide_down():
        for part in cols:
            dz_buf[:, part] = (mm(gmid_buf[...], wa[part, :], NT) * gp_buf[:, part]).astype(jnp.bfloat16)
            yield

    def wide_up():
        total = 0.0
        for k, part in enumerate(cols):
            product = mm(dz_buf[:, part], ua[:, part], NT)
            total = product if k == 0 else total + product
            if k == len(cols) - 1:
                done((gmid_buf[...].astype(jnp.float32) + total).astype(jnp.bfloat16))
            yield

    return dict(d=narrow_down(), m=narrow_up(), x=wide_down(), p=wide_up())


def run_tasks(order, tasks):
    for name in order:
        next(tasks[name])


def add_product(total, lhs, rhs, width):
    for rows in blocks(total.shape[0], width):
        total[rows, :] += mm(lhs[:, rows].T, rhs[...])


def kernel(
    axis, acts, gout, ua_hbm, wa_hbm, ub_hbm, wb_hbm,
    acts_out, grad_in, dua_hbm, dwa_hbm, dub_hbm, dwb_hbm,
    h_all, g_all, relay, mid_all, a_all, gp_all, ab_all, gpb_all,
    ua, wa, ub, wb, dua, dwa, dub, dwb,
    h_buf, a_buf, gp_buf, mid_buf, ab_buf, gpb_buf, f_send,
    g_buf, gp_in, gpb_in, dzb_buf, gmid_buf, dz_buf, b_send,
    a_in, h_in, mid_in, ab_in,
    got_h, got_g, got_out, got_gin, f_sem, b_sem, feed_h_sem, feed_g_sem, got_relay, relay_sem,
    h_sem, g_sem, gp_sem, gpb_sem, w_sem, st_sem, param_sem,
):
    me = lax.axis_index(axis)
    stages = lax.axis_size(axis)
    last = stages - 1
    own = acts.shape[0]
    chunks = own * stages

    def ahead(stage):
        return stage + stage // 2

    def behind(stage):
        return 2 * stage + stage // 2

    span = ahead(last) + LAG + behind(last)

    weights = (ua, wa, ub, wb)

    def fwd_chunk(t):
        return t - ahead(me)

    def bwd_chunk(t):
        return t - span + behind(me)

    def valid(c):
        return (c >= 0) & (c < chunks)

    def on(device):
        return dict(device_id={axis: device}, device_id_type=MESH)

    def load(src, dst, sem):
        return pltpu.make_async_copy(src, dst, sem)

    params = [load(src, dst, param_sem.at[k]) for k, (src, dst) in enumerate(
        [(ua_hbm, ua), (wa_hbm, wa), (ub_hbm, ub), (wb_hbm, wb)])]
    for copy in params:
        copy.start()
    barrier = pltpu.get_barrier_semaphore()
    for device in range(stages):
        pl.semaphore_signal(barrier, inc=1, **on(device))

    def arrival(buf, c, sem):
        return pltpu.make_async_remote_copy(buf.at[c], buf.at[c], sem.at[c], sem.at[c], **on(me))

    def fetch_h(c):
        @pl.when(valid(c))
        def _():
            local = (me == 0) & (c < own)

            side = lax.rem(c, 2)

            @pl.when(local)
            def _():
                load(acts.at[lax.rem(c, own)], h_buf.at[side], h_sem.at[side]).start()

            @pl.when(jnp.logical_not(local))
            def _():
                arrival(h_all, c, got_h).wait_recv()
                load(h_all.at[c], h_buf.at[side], h_sem.at[side]).start()

    def fetch_slopes(c):
        @pl.when(valid(c))
        def _():
            side = lax.rem(c, 2)
            load(gp_all.at[c], gp_in.at[side], gp_sem.at[side]).start()
            load(gpb_all.at[c], gpb_in.at[side], gpb_sem.at[side]).start()

    def fetch_g(c):
        @pl.when(valid(c))
        def _():
            local = (me == last) & (c >= chunks - own)
            buf = g_buf.at[lax.rem(c, 2)]

            @pl.when(local)
            def _():
                load(gout.at[lax.rem(c, own)], buf, g_sem).start()

            @pl.when(jnp.logical_not(local))
            def _():
                arrival(g_all, c, got_g).wait_recv()
                load(g_all.at[c], buf, g_sem).start()

    def fetch_weight_operands(c):
        local_h = (me == 0) & (c < own)

        @pl.when(local_h)
        def _():
            load(acts.at[lax.rem(c, own)], h_in, w_sem.at[0]).start()

        @pl.when(jnp.logical_not(local_h))
        def _():
            load(h_all.at[c], h_in, w_sem.at[0]).start()
        load(a_all.at[c], a_in, w_sem.at[1]).start()
        load(mid_all.at[c], mid_in, w_sem.at[2]).start()
        load(ab_all.at[c], ab_in, w_sem.at[3]).start()

    def send(slot_ref, sem, c, inner, next_device, next_all, next_sem, home_out, home_sem):
        home = c // own
        spot = lax.rem(c, own)

        @pl.when(inner)
        def _():
            pltpu.make_async_remote_copy(slot_ref, next_all.at[c], sem, next_sem.at[c], **on(next_device)).start()

        @pl.when(jnp.logical_not(inner) & (home != me))
        def _():
            pltpu.make_async_remote_copy(slot_ref, home_out.at[spot], sem, home_sem.at[spot], **on(home)).start()

        @pl.when(jnp.logical_not(inner) & (home == me))
        def _():
            load(slot_ref, home_out.at[spot], sem).start()

    def sent(slot_ref, sem):
        load(slot_ref, slot_ref, sem).wait()

    half = stages // 2
    first_half, edge = me < half, half // 2

    def feed_acts(t):
        by_way = (me >= edge) & first_half
        lead = jnp.where(first_half, own * me, own + own // 2)
        spot = t + lead - own * me
        due = (me != 0) & (spot >= 0) & (spot < own)

        @pl.when(due & jnp.logical_not(by_way))
        def _():
            pltpu.make_async_remote_copy(acts.at[spot], h_all.at[own * me + spot], feed_h_sem.at[spot], got_h.at[own * me + spot], **on(0)).start()

        @pl.when(due & by_way)
        def _():
            pltpu.make_async_remote_copy(acts.at[spot], relay.at[spot], feed_h_sem.at[spot], got_relay.at[spot], **on(me + half)).start()

        spot = t - me - 1

        @pl.when((me >= half + edge) & (spot >= 0) & (spot < own))
        def _():
            arrival(relay, spot, got_relay).wait_recv()
            c = own * (me - half) + spot
            pltpu.make_async_remote_copy(relay.at[spot], h_all.at[c], relay_sem.at[spot], got_h.at[c], **on(0)).start()

    def feed_grads(t):
        by_way = (me == 0) | (jnp.logical_not(first_half) & (me < half + edge))
        spot = t - jnp.where(by_way, 0, own // 2) - own * me
        due = (me != last) & (spot >= 0) & (spot < own)

        @pl.when(due & jnp.logical_not(by_way))
        def _():
            pltpu.make_async_remote_copy(gout.at[spot], g_all.at[own * me + spot], feed_g_sem.at[spot], got_g.at[own * me + spot], **on(last)).start()

        @pl.when(due & by_way)
        def _():
            pltpu.make_async_remote_copy(gout.at[spot], relay.at[spot], feed_g_sem.at[spot], got_relay.at[spot], **on(lax.rem(me + half, stages))).start()

        source = jnp.where(me == half, 0, me + half)
        spot = t - jnp.where(me == half, ahead(half), own + own // 2 + own * source)

        @pl.when(((me < edge) | (me == half)) & (spot >= 0) & (spot < own))
        def _():
            arrival(relay, spot, got_relay).wait_recv()
            c = own * source + spot
            pltpu.make_async_remote_copy(relay.at[spot], g_all.at[c], relay_sem.at[spot], got_g.at[c], **on(last)).start()

    def wide_saves(c):
        pairs = [(a_buf, a_all), (gp_buf, gp_all), (mid_buf, mid_all)]
        return [load(src, dst.at[c], st_sem.at[k]) for k, (src, dst) in enumerate(pairs)]

    def narrow_saves(c):
        pairs = [(ab_buf, ab_all), (gpb_buf, gpb_all)]
        return [load(src, dst.at[c], st_sem.at[k + 3]) for k, (src, dst) in enumerate(pairs)]

    def start(copies):
        for copy in copies:
            copy.start()

    def saved(c, copies):
        @pl.when(valid(c))
        def _():
            for copy in copies(c):
                copy.wait()

    @pl.when(me == 0)
    def _():
        load(acts.at[0], h_buf.at[0], h_sem.at[0]).start()
    for total in (dua, dwa, dub, dwb):
        total[...] = jnp.zeros_like(total)
    pl.semaphore_wait(barrier, stages)
    for copy in params:
        copy.wait()

    def step(t, _):
        cf, cb = fwd_chunk(t), bwd_chunk(t)
        has_f, has_b = valid(cf), valid(cb)
        feed_acts(t)
        feed_grads(t)

        f_alone = has_f & jnp.logical_not(has_b)
        late = f_alone & (cb + 1 < 0)
        saved(cf - 1, wide_saves)

        @pl.when(jnp.logical_not(late))
        def _():
            saved(cf - 1, narrow_saves)

        fetch_slopes(cb + 1)

        @pl.when(me == 0)
        def _():
            fetch_h(cf + 1)

        @pl.when(has_b)
        def _():
            fetch_weight_operands(cb)

        b_side = lax.rem(jnp.maximum(cb, 0), 2)
        f_side = lax.rem(jnp.maximum(cf, 0), 2)
        h_now = h_buf.at[f_side]
        g_now, gp_now, gpb_now = g_buf.at[b_side], gp_in.at[b_side], gpb_in.at[b_side]
        f_slot, b_slot = lax.rem(cf, SLOTS), lax.rem(cb, SLOTS)

        def f_begin():
            load(h_now, h_now, h_sem.at[f_side]).wait()

            @pl.when(cf >= SLOTS)
            def _():
                sent(f_send.at[f_slot], f_sem.at[f_slot])

        def f_tasks():
            def done(h):
                f_send[f_slot] = h
            return forward_tasks(h_now, weights, (a_buf, gp_buf, mid_buf, ab_buf, gpb_buf), done)

        def f_end():
            send(f_send.at[f_slot], f_sem.at[f_slot], cf, me != last, me + 1, h_all, got_h, acts_out, got_out)

        def b_begin():
            load(g_buf.at[0], g_buf.at[0], g_sem).wait()
            load(gp_now, gp_now, gp_sem.at[b_side]).wait()
            load(gpb_now, gpb_now, gpb_sem.at[b_side]).wait()

            @pl.when(cb >= SLOTS)
            def _():
                sent(b_send.at[b_slot], b_sem.at[b_slot])

        def b_tasks():
            def done(g):
                b_send[b_slot] = g
            return backward_tasks(g_now, weights, (gp_now, gpb_now), (dzb_buf, gmid_buf, dz_buf), done)

        def b_end():
            send(b_send.at[b_slot], b_sem.at[b_slot], cb, me != 0, me - 1, g_all, got_g, grad_in, got_gin)

        @pl.when(has_f & has_b)
        def _():
            f_begin()
            b_begin()
            run_tasks(FB_ORDER, f_tasks() | b_tasks())
            b_end()
            f_end()
            start(wide_saves(cf) + narrow_saves(cf))

        @pl.when(f_alone)
        def _():
            tasks = f_tasks()
            f_begin()
            run_tasks(F_ORDER[:-2], tasks)
            start(wide_saves(cf))

            @pl.when(late)
            def _():
                saved(cf - 1, narrow_saves)
            run_tasks(F_ORDER[-2:], tasks)
            f_end()
            start(narrow_saves(cf))

        @pl.when(has_b & jnp.logical_not(has_f))
        def _():
            b_begin()
            run_tasks(B_ORDER, b_tasks())
            b_end()

        steady = valid(cf + 1)

        @pl.when(steady)
        def _():
            fetch_g(cb + 1)

            @pl.when(me != 0)
            def _():
                fetch_h(cf + 1)

        @pl.when(has_b)
        def _():
            for k, buf in enumerate((h_in, a_in, mid_in, ab_in)):
                load(buf, buf, w_sem.at[k]).wait()
            add_product(dwb, ab_in, g_now, 256)
            add_product(dub, mid_in, dzb_buf, 256)
            add_product(dwa, a_in, gmid_buf, 256)
            add_product(dua, h_in, dz_buf, 256)

        @pl.when(jnp.logical_not(steady))
        def _():
            fetch_g(cb + 1)
        return 0

    lax.fori_loop(0, chunks + span, step, 0)

    finals = [load(src, dst, param_sem.at[k]) for k, (src, dst) in enumerate(
        [(dua, dua_hbm), (dwa, dwa_hbm), (dub, dub_hbm), (dwb, dwb_hbm)])]
    for copy in finals:
        copy.start()
    for slot in range(SLOTS):
        sent(f_send.at[slot], f_sem.at[slot])
        sent(b_send.at[slot], b_sem.at[slot])

    def settle(k, _):
        @pl.when(me != 0)
        def _():
            load(acts.at[k], acts.at[k], feed_h_sem.at[k]).wait()
            arrival(grad_in, k, got_gin).wait_recv()

        @pl.when(me != last)
        def _():
            load(gout.at[k], gout.at[k], feed_g_sem.at[k]).wait()
            arrival(acts_out, k, got_out).wait_recv()

        @pl.when((me < edge) | (me == half) | (me >= half + edge))
        def _():
            load(relay.at[k], relay.at[k], relay_sem.at[k]).wait()
        return 0

    lax.fori_loop(0, own, settle, 0)
    for copy in finals:
        copy.wait()


def run_stages(axis, stages, acts, gout, ua, wa, ub, wb):
    tokens, width = acts.shape
    own = tokens // ROWS
    chunks = own * stages
    wide, narrow = ua.shape[1], ub.shape[1]
    bf, f32 = jnp.bfloat16, jnp.float32
    shape = jax.ShapeDtypeStruct
    outs = [
        shape((own, ROWS, width), bf), shape((own, ROWS, width), bf),
        shape(ua.shape, f32), shape(wa.shape, f32), shape(ub.shape, f32), shape(wb.shape, f32),
        shape((chunks, ROWS, width), bf), shape((chunks, ROWS, width), bf), shape((own, ROWS, width), bf), shape((chunks, ROWS, width), bf),
        shape((chunks, ROWS, wide), bf), shape((chunks, ROWS, wide), f32),
        shape((chunks, ROWS, narrow), bf), shape((chunks, ROWS, narrow), f32),
    ]
    vm, dma = pltpu.VMEM, pltpu.SemaphoreType.DMA
    tok, wid, nar = (ROWS, width), (ROWS, wide), (ROWS, narrow)
    scratch = [
        vm(ua.shape, bf), vm(wa.shape, bf), vm(ub.shape, bf), vm(wb.shape, bf),
        vm(ua.shape, f32), vm(wa.shape, f32), vm(ub.shape, f32), vm(wb.shape, f32),
        vm((2,) + tok, bf), vm(wid, bf), vm(wid, f32), vm(tok, bf), vm(nar, bf), vm(nar, f32), vm((SLOTS,) + tok, bf),
        vm((2,) + tok, bf), vm((2,) + wid, f32), vm((2,) + nar, f32), vm(nar, bf), vm(tok, bf), vm(wid, bf), vm((SLOTS,) + tok, bf),
        vm(wid, bf), vm(tok, bf), vm(tok, bf), vm(nar, bf),
        dma((chunks,)), dma((chunks,)), dma((own,)), dma((own,)), dma((SLOTS,)), dma((SLOTS,)), dma((own,)), dma((own,)), dma((own,)), dma((own,)),
        dma((2,)), dma, dma((2,)), dma((2,)), dma((4,)), dma((5,)), dma((4,)),
    ]
    results = pl.pallas_call(
        functools.partial(kernel, axis),
        out_shape=outs,
        in_specs=[ANY] * 6,
        out_specs=[ANY] * len(outs),
        scratch_shapes=scratch,
        compiler_params=pltpu.CompilerParams(vmem_limit_bytes=VMEM_LIMIT, has_side_effects=True, collective_id=0),
    )(acts.reshape(own, ROWS, width), gout.reshape(own, ROWS, width), ua, wa, ub, wb)
    return results[:6]


def solution(mesh):
    tok_spec = P(('data', 'stage'))
    row_spec = P('stage')
    stages = mesh.shape['stage']

    def device_body(acts_in, grad_out, w_up_a, w_down_a, w_up_b, w_down_b):
        tokens, width = acts_in.shape[0] * acts_in.shape[1], acts_in.shape[2]
        out, gin, dua, dwa, dub, dwb = run_stages(
            'stage', stages, acts_in.reshape(tokens, width), grad_out.reshape(tokens, width),
            w_up_a[0], w_down_a[0], w_up_b[0], w_down_b[0])
        return (out.reshape(acts_in.shape), gin.reshape(acts_in.shape), dua[None], dwa[None], dub[None], dwb[None])

    return jax.shard_map(device_body, mesh=mesh, in_specs=(tok_spec, tok_spec, row_spec, row_spec, row_spec, row_spec), out_specs=(tok_spec,) * 6, check_vma=False)
```

```python
import functools

import jax
import jax.numpy as jnp
from jax import lax
from jax.experimental import pallas as pl
from jax.experimental.pallas import tpu as pltpu
from jax.sharding import PartitionSpec as P

MESH = pl.DeviceIdType.MESH
ANY = pl.BlockSpec(memory_space=pl.ANY)
VMEM_LIMIT = 67043328

GELU_C = 0.7978845608028654
GELU_K = 0.044715

ROWS = 256
LAG = 2
SLOTS = 4
WIDE_COLS = 512
F_ORDER = 'zzczczczczccyo'
HALF_ORDER = 'zzczczczczccyo'
B_ORDER = 'dmxxpxpxpxpxpp'

FB_ORDER = 'zdmzxzcxpzcxpzcxpzccpxcxpypo'

NT = (((1,), (1,)), ((), ()))
TN = (((0,), (0,)), ((), ()))


def mm(lhs, rhs, dims=(((1,), (0,)), ((), ()))):
    return lax.dot_general(lhs, rhs, dims, preferred_element_type=jnp.float32)


def gelu_and_slope(z):
    zz = z * z
    half = 0.5 + 0.5 * jnp.tanh(z * (GELU_C + (GELU_C * GELU_K) * zz))
    act = z * half
    return act, half + act * (1.0 - half) * (2.0 * GELU_C + (6.0 * GELU_C * GELU_K) * zz)


def blocks(size, width):
    return [slice(start, min(start + width, size)) for start in range(0, size, width)]


def forward_tasks(h, weights, saved, done):
    ua, wa, ub, wb = weights
    a_buf, gp_buf, mid_buf, ab_buf, gpb_buf = saved
    cols = blocks(ua.shape[1], WIDE_COLS)

    def wide_up():
        for part in cols:
            act, slope = gelu_and_slope(mm(h[...], ua[:, part]))
            a_buf[:, part] = act.astype(jnp.bfloat16)
            gp_buf[:, part] = slope
            yield

    def wide_down():
        total = 0.0
        for k, part in enumerate(cols):
            product = mm(a_buf[:, part], wa[part, :])
            total = product if k == 0 else total + product
            if k == len(cols) - 1:
                mid_buf[...] = (h[...].astype(jnp.float32) + total).astype(jnp.bfloat16)
            yield

    def narrow_up():
        act, slope = gelu_and_slope(mm(mid_buf[...], ub[...]))
        ab_buf[...] = act.astype(jnp.bfloat16)
        gpb_buf[...] = slope
        yield

    def narrow_down():
        done((mid_buf[...].astype(jnp.float32) + mm(ab_buf[...], wb[...])).astype(jnp.bfloat16))
        yield

    return dict(z=wide_up(), c=wide_down(), y=narrow_up(), o=narrow_down())


def backward_tasks(g, weights, slopes, kept, done):
    ua, wa, ub, wb = weights
    gp_buf, gpb_buf = slopes
    dzb_buf, gmid_buf, dz_buf = kept
    cols = blocks(wa.shape[0], WIDE_COLS)

    def narrow_down():
        dzb_buf[...] = (mm(g[...], wb[...], NT) * gpb_buf[...]).astype(jnp.bfloat16)
        yield

    def narrow_up():
        gmid_buf[...] = (g[...].astype(jnp.float32) + mm(dzb_buf[...], ub[...], NT)).astype(jnp.bfloat16)
        yield

    def wide_down():
        for part in cols:
            dz_buf[:, part] = (mm(gmid_buf[...], wa[part, :], NT) * gp_buf[:, part]).astype(jnp.bfloat16)
            yield

    def wide_up():
        total = 0.0
        for k, part in enumerate(cols):
            product = mm(dz_buf[:, part], ua[:, part], NT)
            total = product if k == 0 else total + product
            if k == len(cols) - 1:
                done((gmid_buf[...].astype(jnp.float32) + total).astype(jnp.bfloat16))
            yield

    return dict(d=narrow_down(), m=narrow_up(), x=wide_down(), p=wide_up())


def run_tasks(order, tasks):
    for name in order:
        next(tasks[name])


def add_product(total, lhs, rhs, width):
    for rows in blocks(total.shape[0], width):
        total[rows, :] += mm(lhs[:, rows].T, rhs[...])


def kernel(
    axis, acts, gout, ua_hbm, wa_hbm, ub_hbm, wb_hbm,
    acts_out, grad_in, dua_hbm, dwa_hbm, dub_hbm, dwb_hbm,
    h_all, g_all, relay, mid_all, a_all, gp_all, ab_all, gpb_all,
    ua, wa, ub, wb, dua, dwa, dub, dwb,
    h_buf, a_buf, gp_buf, mid_buf, ab_buf, gpb_buf, f_send,
    g_buf, gp_in, gpb_in, dzb_buf, gmid_buf, dz_buf, b_send,
    a_in, h_in, mid_in, ab_in,
    got_h, got_g, got_out, got_gin, f_sem, b_sem, feed_h_sem, feed_g_sem, got_relay, relay_sem, half_sem, keep_sem,
    h_sem, g_sem, gp_sem, gpb_sem, w_sem, st_sem, param_sem,
):
    me = lax.axis_index(axis)
    stages = lax.axis_size(axis)
    last = stages - 1
    own = acts.shape[0]
    chunks = own * stages

    def ahead(stage):
        return stage + stage // 2

    def behind(stage):
        return 2 * stage + stage // 2

    span = ahead(last) + LAG + behind(last)

    weights = (ua, wa, ub, wb)

    def fwd_chunk(t):
        return t - ahead(me)

    def bwd_chunk(t):
        return t - span + behind(me)

    def valid(c):
        return (c >= 0) & (c < chunks)

    def on(device):
        return dict(device_id={axis: device}, device_id_type=MESH)

    def load(src, dst, sem):
        return pltpu.make_async_copy(src, dst, sem)

    params = [load(src, dst, param_sem.at[k]) for k, (src, dst) in enumerate(
        [(ua_hbm, ua), (wa_hbm, wa), (ub_hbm, ub), (wb_hbm, wb)])]
    for copy in params:
        copy.start()
    barrier = pltpu.get_barrier_semaphore()
    for device in range(stages):
        pl.semaphore_signal(barrier, inc=1, **on(device))

    def arrival(buf, c, sem):
        return pltpu.make_async_remote_copy(buf.at[c], buf.at[c], sem.at[c], sem.at[c], **on(me))

    def fetch_h(c):
        @pl.when(valid(c) & ((c > 0) | (me == 0)))
        def _():
            local = (me == 0) & (c < own)

            side = lax.rem(c, 2)

            @pl.when(local)
            def _():
                load(acts.at[lax.rem(c, own)], h_buf.at[side], h_sem.at[side]).start()

            @pl.when(jnp.logical_not(local))
            def _():
                arrival(h_all, c, got_h).wait_recv()
                load(h_all.at[c], h_buf.at[side], h_sem.at[side]).start()

    def fetch_slopes(c):
        @pl.when(valid(c))
        def _():
            side = lax.rem(c, 2)
            load(gp_all.at[c], gp_in.at[side], gp_sem.at[side]).start()
            load(gpb_all.at[c], gpb_in.at[side], gpb_sem.at[side]).start()

    def g_slot(c):
        return jnp.where(c == chunks - 1, 2, lax.rem(jnp.maximum(c, 0), 2))

    def comes_direct(c):
        return (c == chunks - 1) & (me != last)

    def fetch_g(c):
        @pl.when(valid(c) & jnp.logical_not(comes_direct(c)))
        def _():
            local = (me == last) & (c >= chunks - own)
            buf = g_buf.at[g_slot(c)]

            @pl.when(local)
            def _():
                load(gout.at[lax.rem(c, own)], buf, g_sem).start()

            @pl.when(jnp.logical_not(local))
            def _():
                arrival(g_all, c, got_g).wait_recv()
                load(g_all.at[c], buf, g_sem).start()

    def fetch_weight_operands(c):
        local_h = (me == 0) & (c < own)

        @pl.when(local_h)
        def _():
            load(acts.at[lax.rem(c, own)], h_in, w_sem.at[0]).start()

        @pl.when(jnp.logical_not(local_h))
        def _():
            load(h_all.at[c], h_in, w_sem.at[0]).start()
        load(a_all.at[c], a_in, w_sem.at[1]).start()
        load(mid_all.at[c], mid_in, w_sem.at[2]).start()
        load(ab_all.at[c], ab_in, w_sem.at[3]).start()

    def send(slot_ref, sem, c, inner, next_device, next_all, next_sem, home_out, home_sem):
        home = c // own
        spot = lax.rem(c, own)

        @pl.when(inner)
        def _():
            pltpu.make_async_remote_copy(slot_ref, next_all.at[c], sem, next_sem.at[c], **on(next_device)).start()

        @pl.when(jnp.logical_not(inner) & (home != me))
        def _():
            pltpu.make_async_remote_copy(slot_ref, home_out.at[spot], sem, home_sem.at[spot], **on(home)).start()

        @pl.when(jnp.logical_not(inner) & (home == me))
        def _():
            load(slot_ref, home_out.at[spot], sem).start()

    def sent(slot_ref, sem):
        load(slot_ref, slot_ref, sem).wait()

    half = stages // 2
    first_half, edge = me < half, half // 2

    def feed_acts(t):
        by_way = (me >= edge) & first_half
        lead = jnp.where(first_half, own * me, own + own // 2)
        spot = t + lead - own * me
        due = (me != 0) & (spot >= 0) & (spot < own)

        @pl.when(due & jnp.logical_not(by_way))
        def _():
            pltpu.make_async_remote_copy(acts.at[spot], h_all.at[own * me + spot], feed_h_sem.at[spot], got_h.at[own * me + spot], **on(0)).start()

        @pl.when(due & by_way)
        def _():
            pltpu.make_async_remote_copy(acts.at[spot], relay.at[spot], feed_h_sem.at[spot], got_relay.at[spot], **on(me + half)).start()

        spot = t - me - 1

        @pl.when((me >= half + edge) & (spot >= 0) & (spot < own))
        def _():
            arrival(relay, spot, got_relay).wait_recv()
            c = own * (me - half) + spot
            pltpu.make_async_remote_copy(relay.at[spot], h_all.at[c], relay_sem.at[spot], got_h.at[c], **on(0)).start()

    def feed_grads(t):
        by_way = (me == 0) | (jnp.logical_not(first_half) & (me < half + edge))
        spot = t - jnp.where(by_way, 0, own // 2) - own * me
        due = (me != last) & (spot >= 0) & (spot < own)

        @pl.when(due & jnp.logical_not(by_way))
        def _():
            pltpu.make_async_remote_copy(gout.at[spot], g_all.at[own * me + spot], feed_g_sem.at[spot], got_g.at[own * me + spot], **on(last)).start()

        @pl.when(due & by_way)
        def _():
            pltpu.make_async_remote_copy(gout.at[spot], relay.at[spot], feed_g_sem.at[spot], got_relay.at[spot], **on(lax.rem(me + half, stages))).start()

        source = jnp.where(me == half, 0, me + half)
        spot = t - jnp.where(me == half, ahead(half), own + own // 2 + own * source)

        @pl.when(((me < edge) | (me == half)) & (spot >= 0) & (spot < own))
        def _():
            arrival(relay, spot, got_relay).wait_recv()
            c = own * source + spot
            pltpu.make_async_remote_copy(relay.at[spot], g_all.at[c], relay_sem.at[spot], got_g.at[c], **on(last)).start()

    def wide_saves(c):
        pairs = [(a_buf, a_all), (gp_buf, gp_all), (mid_buf, mid_all)]
        return [load(src, dst.at[c], st_sem.at[k]) for k, (src, dst) in enumerate(pairs)]

    def narrow_saves(c):
        pairs = [(ab_buf, ab_all), (gpb_buf, gpb_all)]
        return [load(src, dst.at[c], st_sem.at[k + 3]) for k, (src, dst) in enumerate(pairs)]

    def start(copies):
        for copy in copies:
            copy.start()

    def saved(c, copies):
        @pl.when(valid(c))
        def _():
            for copy in copies(c):
                copy.wait()

    @pl.when(me == 0)
    def _():
        load(acts.at[0], h_buf.at[0], h_sem.at[0]).start()
    for total in (dua, dwa, dub, dwb):
        total[...] = jnp.zeros_like(total)
    pl.semaphore_wait(barrier, stages)
    for copy in params:
        copy.wait()

    def step(t, _):
        cf, cb = fwd_chunk(t), bwd_chunk(t)
        has_f, has_b = valid(cf), valid(cb)
        with jax.named_scope('feed'):
            feed_acts(t)
            feed_grads(t)

        f_alone = has_f & jnp.logical_not(has_b)
        late = f_alone & (cb + 1 < 0)
        with jax.named_scope('wst'):
            saved(cf - 1, wide_saves)

        @pl.when(jnp.logical_not(late))
        def _():
            saved(cf - 1, narrow_saves)

        fetch_slopes(cb + 1)

        @pl.when(me == 0)
        def _():
            fetch_h(cf + 1)

        @pl.when(has_b)
        def _():
            fetch_weight_operands(cb)

        b_side = lax.rem(jnp.maximum(cb, 0), 2)
        f_side = lax.rem(jnp.maximum(cf, 0), 2)
        h_now = h_buf.at[f_side]
        g_now, gp_now, gpb_now = g_buf.at[g_slot(cb)], gp_in.at[b_side], gpb_in.at[b_side]
        f_slot, b_slot = lax.rem(cf, SLOTS), lax.rem(cb, SLOTS)

        def f_begin():
            load(h_now, h_now, h_sem.at[f_side]).wait()

            @pl.when(cf >= SLOTS)
            def _():
                sent(f_send.at[f_slot], f_sem.at[f_slot])

        def f_tasks():
            def done(h):
                f_send[f_slot] = h
            return forward_tasks(h_now, weights, (a_buf, gp_buf, mid_buf, ab_buf, gpb_buf), done)

        def f_end():
            send(f_send.at[f_slot], f_sem.at[f_slot], cf, me != last, me + 1, h_all, got_h, acts_out, got_out)

        def b_begin():
            @pl.when(comes_direct(cb))
            def _():
                pltpu.make_async_remote_copy(g_now, g_now, got_g.at[chunks - 1], got_g.at[chunks - 1], **on(me)).wait_recv()

            @pl.when(jnp.logical_not(comes_direct(cb)))
            def _():
                load(g_now, g_now, g_sem).wait()
            load(gp_now, gp_now, gp_sem.at[b_side]).wait()
            load(gpb_now, gpb_now, gpb_sem.at[b_side]).wait()

            @pl.when(cb >= SLOTS)
            def _():
                sent(b_send.at[b_slot], b_sem.at[b_slot])

        def b_tasks():
            def done(g):
                b_send[b_slot] = g
            return backward_tasks(g_now, weights, (gp_now, gpb_now), (dzb_buf, gmid_buf, dz_buf), done)

        def b_end():
            @pl.when((cb == chunks - 1) & (me != 0))
            def _():
                pltpu.make_async_remote_copy(b_send.at[b_slot], g_buf.at[2], b_sem.at[b_slot], got_g.at[chunks - 1], **on(me - 1)).start()

            @pl.when((cb != chunks - 1) | (me == 0))
            def _():
                send_back()

        def send_back():
            send(b_send.at[b_slot], b_sem.at[b_slot], cb, me != 0, me - 1, g_all, got_g, grad_in, got_gin)

        @pl.when(has_f & has_b)
        def _():
            with jax.named_scope('wfb'):
                f_begin()
                b_begin()
            with jax.named_scope('fb'):
                run_tasks(FB_ORDER, f_tasks() | b_tasks())
            b_end()
            f_end()
            start(wide_saves(cf) + narrow_saves(cf))

        @pl.when(cf == 0)
        def _():
            @pl.when(me == 0)
            def _():
                load(h_now, h_now, h_sem.at[0]).wait()

            keep = load(h_buf.at[0], h_all.at[0], keep_sem)

            def half_chunk(r, _):
                rows = pl.ds(pl.multiple_of(r * (ROWS // 2), ROWS // 2), ROWS // 2)
                h_half, out_half = h_buf.at[0, rows], f_send.at[0, rows]

                @pl.when(me != 0)
                def _():
                    pltpu.make_async_remote_copy(h_half, h_half, half_sem.at[r], half_sem.at[r], **on(me)).wait_recv()

                    @pl.when(r == 1)
                    def _():
                        keep.start()

                def done(h):
                    out_half[...] = h
                with jax.named_scope('half'):
                  run_tasks(HALF_ORDER, forward_tasks(h_half, weights, [buf.at[rows] for buf in (a_buf, gp_buf, mid_buf, ab_buf, gpb_buf)], done))

                @pl.when(me != last)
                def _():
                    pltpu.make_async_remote_copy(out_half, h_half, f_sem.at[0], half_sem.at[r], **on(me + 1)).start()

                @pl.when(me == last)
                def _():
                    pltpu.make_async_remote_copy(out_half, acts_out.at[0, rows], f_sem.at[0], got_out.at[0], **on(0)).start()
                return 0

            lax.fori_loop(0, 2, half_chunk, 0)
            start(wide_saves(cf) + narrow_saves(cf))

            @pl.when(me != 0)
            def _():
                keep.wait()

        @pl.when(f_alone & (cf > 0))
        def _():
            tasks = f_tasks()
            with jax.named_scope('wf'):
                f_begin()
            with jax.named_scope('f'):
                run_tasks(F_ORDER[:-2], tasks)
            start(wide_saves(cf))

            @pl.when(late)
            def _():
                saved(cf - 1, narrow_saves)
            run_tasks(F_ORDER[-2:], tasks)
            f_end()
            start(narrow_saves(cf))

        @pl.when(has_b & jnp.logical_not(has_f))
        def _():
            with jax.named_scope('wb'):
                b_begin()
            with jax.named_scope('b'):
                run_tasks(B_ORDER, b_tasks())
            b_end()

        steady = valid(cf + 1)

        @pl.when(steady)
        def _():
            with jax.named_scope('ftg'):
                fetch_g(cb + 1)

            with jax.named_scope('fth'):
                @pl.when(me != 0)
                def _():
                    fetch_h(cf + 1)

        @pl.when(has_b)
        def _():
            for k, buf in enumerate((h_in, a_in, mid_in, ab_in)):
                load(buf, buf, w_sem.at[k]).wait()
            with jax.named_scope('w'):
                add_product(dwb, ab_in, g_now, 256)
                add_product(dub, mid_in, dzb_buf, 256)
                add_product(dwa, a_in, gmid_buf, 256)
                add_product(dua, h_in, dz_buf, 256)

        @pl.when(jnp.logical_not(steady))
        def _():
            fetch_g(cb + 1)
        return 0

    lax.fori_loop(0, chunks + span, step, 0)

    finals = [load(src, dst, param_sem.at[k]) for k, (src, dst) in enumerate(
        [(dua, dua_hbm), (dwa, dwa_hbm), (dub, dub_hbm), (dwb, dwb_hbm)])]
    for copy in finals:
        copy.start()
    for slot in range(SLOTS):
        sent(f_send.at[slot], f_sem.at[slot])
        sent(b_send.at[slot], b_sem.at[slot])

    def settle(k, _):
        @pl.when(me != 0)
        def _():
            load(acts.at[k], acts.at[k], feed_h_sem.at[k]).wait()
            arrival(grad_in, k, got_gin).wait_recv()

        @pl.when(me != last)
        def _():
            load(gout.at[k], gout.at[k], feed_g_sem.at[k]).wait()
            arrival(acts_out, k, got_out).wait_recv()

        @pl.when((me < edge) | (me == half) | (me >= half + edge))
        def _():
            load(relay.at[k], relay.at[k], relay_sem.at[k]).wait()
        return 0

    lax.fori_loop(0, own, settle, 0)
    for copy in finals:
        copy.wait()


def run_stages(axis, stages, acts, gout, ua, wa, ub, wb):
    tokens, width = acts.shape
    own = tokens // ROWS
    chunks = own * stages
    wide, narrow = ua.shape[1], ub.shape[1]
    bf, f32 = jnp.bfloat16, jnp.float32
    shape = jax.ShapeDtypeStruct
    outs = [
        shape((own, ROWS, width), bf), shape((own, ROWS, width), bf),
        shape(ua.shape, f32), shape(wa.shape, f32), shape(ub.shape, f32), shape(wb.shape, f32),
        shape((chunks, ROWS, width), bf), shape((chunks, ROWS, width), bf), shape((own, ROWS, width), bf), shape((chunks, ROWS, width), bf),
        shape((chunks, ROWS, wide), bf), shape((chunks, ROWS, wide), f32),
        shape((chunks, ROWS, narrow), bf), shape((chunks, ROWS, narrow), f32),
    ]
    vm, dma = pltpu.VMEM, pltpu.SemaphoreType.DMA
    tok, wid, nar = (ROWS, width), (ROWS, wide), (ROWS, narrow)
    scratch = [
        vm(ua.shape, bf), vm(wa.shape, bf), vm(ub.shape, bf), vm(wb.shape, bf),
        vm(ua.shape, f32), vm(wa.shape, f32), vm(ub.shape, f32), vm(wb.shape, f32),
        vm((2,) + tok, bf), vm(wid, bf), vm(wid, f32), vm(tok, bf), vm(nar, bf), vm(nar, f32), vm((SLOTS,) + tok, bf),
        vm((3,) + tok, bf), vm((2,) + wid, f32), vm((2,) + nar, f32), vm(nar, bf), vm(tok, bf), vm(wid, bf), vm((SLOTS,) + tok, bf),
        vm(wid, bf), vm(tok, bf), vm(tok, bf), vm(nar, bf),
        dma((chunks,)), dma((chunks,)), dma((own,)), dma((own,)), dma((SLOTS,)), dma((SLOTS,)), dma((own,)), dma((own,)), dma((own,)), dma((own,)), dma((2,)), dma,
        dma((2,)), dma, dma((2,)), dma((2,)), dma((4,)), dma((5,)), dma((4,)),
    ]
    results = pl.pallas_call(
        functools.partial(kernel, axis),
        out_shape=outs,
        in_specs=[ANY] * 6,
        out_specs=[ANY] * len(outs),
        scratch_shapes=scratch,
        compiler_params=pltpu.CompilerParams(vmem_limit_bytes=VMEM_LIMIT, has_side_effects=True, collective_id=0),
    )(acts.reshape(own, ROWS, width), gout.reshape(own, ROWS, width), ua, wa, ub, wb)
    return results[:6]


def solution(mesh):
    tok_spec = P(('data', 'stage'))
    row_spec = P('stage')
    stages = mesh.shape['stage']

    def device_body(acts_in, grad_out, w_up_a, w_down_a, w_up_b, w_down_b):
        tokens, width = acts_in.shape[0] * acts_in.shape[1], acts_in.shape[2]
        out, gin, dua, dwa, dub, dwb = run_stages(
            'stage', stages, acts_in.reshape(tokens, width), grad_out.reshape(tokens, width),
            w_up_a[0], w_down_a[0], w_up_b[0], w_down_b[0])
        return (out.reshape(acts_in.shape), gin.reshape(acts_in.shape), dua[None], dwa[None], dub[None], dwb[None])

    return jax.shard_map(device_body, mesh=mesh, in_specs=(tok_spec, tok_spec, row_spec, row_spec, row_spec, row_spec), out_specs=(tok_spec,) * 6, check_vma=False)
```

```python
import functools

import jax
import jax.numpy as jnp
from jax import lax
from jax.experimental import pallas as pl
from jax.experimental.pallas import tpu as pltpu
from jax.sharding import PartitionSpec as P

MESH = pl.DeviceIdType.MESH
ANY = pl.BlockSpec(memory_space=pl.ANY)
VMEM_LIMIT = 67043328

GELU_C = 0.7978845608028654
GELU_K = 0.044715

ROWS = 256
LAG = 2
FIRST = 5
SLOTS = 4
WIDE_COLS = 512
F_ORDER = 'zzczczczczccyo'
HALF_ORDER = 'zzczczczczccyo'
B_ORDER = 'dmxxpxpxpxpxpp'

FB_ORDER = 'zdmzxzcxpzcxpzcxpzccpxcxpypo'

NT = (((1,), (1,)), ((), ()))
TN = (((0,), (0,)), ((), ()))


def mm(lhs, rhs, dims=(((1,), (0,)), ((), ()))):
    return lax.dot_general(lhs, rhs, dims, preferred_element_type=jnp.float32)


def gelu_and_slope(z):
    zz = z * z
    half = 0.5 + 0.5 * jnp.tanh(z * (GELU_C + (GELU_C * GELU_K) * zz))
    act = z * half
    return act, half + act * (1.0 - half) * (2.0 * GELU_C + (6.0 * GELU_C * GELU_K) * zz)


def blocks(size, width):
    return [slice(start, min(start + width, size)) for start in range(0, size, width)]


def forward_tasks(h, weights, saved, done):
    ua, wa, ub, wb = weights
    a_buf, gp_buf, mid_buf, ab_buf, gpb_buf = saved
    cols = blocks(ua.shape[1], WIDE_COLS)

    def wide_up():
        for part in cols:
            act, slope = gelu_and_slope(mm(h[...], ua[:, part]))
            a_buf[:, part] = act.astype(jnp.bfloat16)
            gp_buf[:, part] = slope
            yield

    def wide_down():
        total = 0.0
        for k, part in enumerate(cols):
            product = mm(a_buf[:, part], wa[part, :])
            total = product if k == 0 else total + product
            if k == len(cols) - 1:
                mid_buf[...] = (h[...].astype(jnp.float32) + total).astype(jnp.bfloat16)
            yield

    def narrow_up():
        act, slope = gelu_and_slope(mm(mid_buf[...], ub[...]))
        ab_buf[...] = act.astype(jnp.bfloat16)
        gpb_buf[...] = slope
        yield

    def narrow_down():
        done((mid_buf[...].astype(jnp.float32) + mm(ab_buf[...], wb[...])).astype(jnp.bfloat16))
        yield

    return dict(z=wide_up(), c=wide_down(), y=narrow_up(), o=narrow_down())


def backward_tasks(g, weights, slopes, kept, done):
    ua, wa, ub, wb = weights
    gp_buf, gpb_buf = slopes
    dzb_buf, gmid_buf, dz_buf = kept
    cols = blocks(wa.shape[0], WIDE_COLS)

    def narrow_down():
        dzb_buf[...] = (mm(g[...], wb[...], NT) * gpb_buf[...]).astype(jnp.bfloat16)
        yield

    def narrow_up():
        gmid_buf[...] = (g[...].astype(jnp.float32) + mm(dzb_buf[...], ub[...], NT)).astype(jnp.bfloat16)
        yield

    def wide_down():
        for part in cols:
            dz_buf[:, part] = (mm(gmid_buf[...], wa[part, :], NT) * gp_buf[:, part]).astype(jnp.bfloat16)
            yield

    def wide_up():
        total = 0.0
        for k, part in enumerate(cols):
            product = mm(dz_buf[:, part], ua[:, part], NT)
            total = product if k == 0 else total + product
            if k == len(cols) - 1:
                done((gmid_buf[...].astype(jnp.float32) + total).astype(jnp.bfloat16))
            yield

    return dict(d=narrow_down(), m=narrow_up(), x=wide_down(), p=wide_up())


def run_tasks(order, tasks):
    for name in order:
        next(tasks[name])


def add_product(total, lhs, rhs, width):
    for rows in blocks(total.shape[0], width):
        total[rows, :] += mm(lhs[:, rows].T, rhs[...])


def kernel(
    axis, acts, gout, ua_hbm, wa_hbm, ub_hbm, wb_hbm,
    acts_out, grad_in, dua_hbm, dwa_hbm, dub_hbm, dwb_hbm,
    h_all, g_all, relay, mid_all, a_all, gp_all, ab_all, gpb_all,
    ua, wa, ub, wb, dua, dwa, dub, dwb,
    h_buf, a_buf, gp_buf, mid_buf, ab_buf, gpb_buf, f_send,
    g_buf, gp_in, gpb_in, dzb_buf, gmid_buf, dz_buf, b_send,
    a_in, h_in, mid_in, ab_in,
    got_h, got_g, got_out, got_gin, f_sem, b_sem, feed_h_sem, feed_g_sem, got_relay, relay_sem, half_sem, keep_sem, half_st_sem,
    h_sem, g_sem, gp_sem, gpb_sem, w_sem, st_sem, param_sem,
):
    me = lax.axis_index(axis)
    stages = lax.axis_size(axis)
    last = stages - 1
    own = acts.shape[0]
    chunks = own * stages

    def ahead(stage):
        return stage + stage // 2

    def behind(stage):
        return 2 * stage + stage // 2

    span = ahead(last) + LAG + behind(last)

    weights = (ua, wa, ub, wb)

    def fwd_chunk(t):
        return t - ahead(me)

    def bwd_chunk(t):
        return t - span + behind(me)

    def valid(c):
        return (c >= 0) & (c < chunks)

    def on(device):
        return dict(device_id={axis: device}, device_id_type=MESH)

    def load(src, dst, sem):
        return pltpu.make_async_copy(src, dst, sem)

    params = [load(src, dst, param_sem.at[k]) for k, (src, dst) in enumerate(
        [(ua_hbm, ua), (wa_hbm, wa), (ub_hbm, ub), (wb_hbm, wb)])]
    for copy in params:
        copy.start()
    barrier = pltpu.get_barrier_semaphore()
    for device in range(stages):
        pl.semaphore_signal(barrier, inc=1, **on(device))

    def arrival(buf, c, sem):
        return pltpu.make_async_remote_copy(buf.at[c], buf.at[c], sem.at[c], sem.at[c], **on(me))

    halved = jnp.where(me == last, LAG, FIRST)

    def h_slot(c):
        return jnp.where(c < FIRST, 2 + jnp.maximum(c, 0), lax.rem(jnp.maximum(c, 0), 2))

    def half_rows(r):
        return pl.ds(pl.multiple_of(r * (ROWS // 2), ROWS // 2), ROWS // 2)

    def half_arrival(c, r):
        buf = h_buf.at[h_slot(c), half_rows(r)]
        return pltpu.make_async_remote_copy(buf, buf, half_sem.at[c, r], half_sem.at[c, r], **on(me))

    def keep_copy(c):
        return load(h_buf.at[h_slot(c)], h_all.at[c], keep_sem.at[c])

    def half_saves(c, r):
        pairs = [(a_buf, a_all), (gp_buf, gp_all), (mid_buf, mid_all), (ab_buf, ab_all), (gpb_buf, gpb_all)]
        return [load(src.at[half_rows(r)], dst.at[c, half_rows(r)], half_st_sem.at[r, k]) for k, (src, dst) in enumerate(pairs)]

    def fetch_h(c):
        @pl.when(valid(c) & ((c >= FIRST) | (me == 0)))
        def _():
            local = (me == 0) & (c < own)

            side = lax.rem(c, 2)
            buf = h_buf.at[h_slot(c)]

            @pl.when(local)
            def _():
                load(acts.at[lax.rem(c, own)], buf, h_sem.at[side]).start()

            @pl.when(jnp.logical_not(local))
            def _():
                arrival(h_all, c, got_h).wait_recv()
                load(h_all.at[c], buf, h_sem.at[side]).start()

    def fetch_slopes(c):
        @pl.when(valid(c))
        def _():
            side = lax.rem(c, 2)
            load(gp_all.at[c], gp_in.at[side], gp_sem.at[side]).start()
            load(gpb_all.at[c], gpb_in.at[side], gpb_sem.at[side]).start()

    def g_slot(c):
        return jnp.where(c == chunks - 1, 2, lax.rem(jnp.maximum(c, 0), 2))

    def comes_direct(c):
        return (c == chunks - 1) & (me != last)

    def fetch_g(c):
        @pl.when(valid(c) & jnp.logical_not(comes_direct(c)))
        def _():
            local = (me == last) & (c >= chunks - own)
            buf = g_buf.at[g_slot(c)]

            @pl.when(local)
            def _():
                load(gout.at[lax.rem(c, own)], buf, g_sem).start()

            @pl.when(jnp.logical_not(local))
            def _():
                arrival(g_all, c, got_g).wait_recv()
                load(g_all.at[c], buf, g_sem).start()

    def fetch_weight_operands(c):
        local_h = (me == 0) & (c < own)

        @pl.when(local_h)
        def _():
            load(acts.at[lax.rem(c, own)], h_in, w_sem.at[0]).start()

        @pl.when(jnp.logical_not(local_h))
        def _():
            load(h_all.at[c], h_in, w_sem.at[0]).start()
        load(a_all.at[c], a_in, w_sem.at[1]).start()
        load(mid_all.at[c], mid_in, w_sem.at[2]).start()
        load(ab_all.at[c], ab_in, w_sem.at[3]).start()

    def send(slot_ref, sem, c, inner, next_device, next_all, next_sem, home_out, home_sem):
        home = c // own
        spot = lax.rem(c, own)

        @pl.when(inner)
        def _():
            pltpu.make_async_remote_copy(slot_ref, next_all.at[c], sem, next_sem.at[c], **on(next_device)).start()

        @pl.when(jnp.logical_not(inner) & (home != me))
        def _():
            pltpu.make_async_remote_copy(slot_ref, home_out.at[spot], sem, home_sem.at[spot], **on(home)).start()

        @pl.when(jnp.logical_not(inner) & (home == me))
        def _():
            load(slot_ref, home_out.at[spot], sem).start()

    def sent(slot_ref, sem):
        load(slot_ref, slot_ref, sem).wait()

    half = stages // 2
    first_half, edge = me < half, half // 2

    def feed_acts(t):
        by_way = (me >= edge) & first_half
        later = jnp.where(me < half + edge, own * me - own - own // 2, 3 * own + 3 + own * (me - half - edge))
        spot = t - jnp.where(first_half, 0, later)
        due = (me != 0) & (spot >= 0) & (spot < own)

        @pl.when(due & jnp.logical_not(by_way))
        def _():
            pltpu.make_async_remote_copy(acts.at[spot], h_all.at[own * me + spot], feed_h_sem.at[spot], got_h.at[own * me + spot], **on(0)).start()

        @pl.when(due & by_way)
        def _():
            pltpu.make_async_remote_copy(acts.at[spot], relay.at[spot], feed_h_sem.at[spot], got_relay.at[spot], **on(me + half)).start()

        spot = t - me - 4

        @pl.when((me >= half + edge) & (spot >= 0) & (spot < own))
        def _():
            arrival(relay, spot, got_relay).wait_recv()
            c = own * (me - half) + spot
            pltpu.make_async_remote_copy(relay.at[spot], h_all.at[c], relay_sem.at[spot], got_h.at[c], **on(0)).start()

    def feed_grads(t):
        by_way = (me == 0) | (jnp.logical_not(first_half) & (me < half + edge))
        later = jnp.where(me == 1, 2 * own + 2, own // 2 + own * me)
        spot = t - jnp.where(me == 0, 0, jnp.where(by_way, 2 * own - 2 + 10 * (me - half), later))
        due = (me != last) & (spot >= 0) & (spot < own)

        @pl.when(due & jnp.logical_not(by_way))
        def _():
            pltpu.make_async_remote_copy(gout.at[spot], g_all.at[own * me + spot], feed_g_sem.at[spot], got_g.at[own * me + spot], **on(last)).start()

        @pl.when(due & by_way)
        def _():
            pltpu.make_async_remote_copy(gout.at[spot], relay.at[spot], feed_g_sem.at[spot], got_relay.at[spot], **on(lax.rem(me + half, stages))).start()

        source = jnp.where(me == half, 0, me + half)
        early = jnp.maximum(t - ahead(half), -1)
        spot = jnp.where(me == half, jnp.where(early < own - 1, (early + 1) // 2, early - own // 2 + 1), t - span - own * me)
        due = (me < edge) | ((me == half) & (early >= 0) & ((early >= own - 1) | (lax.rem(early + 2, 2) == 0)))

        @pl.when(due & (spot >= 0) & (spot < own))
        def _():
            arrival(relay, spot, got_relay).wait_recv()
            c = own * source + spot
            pltpu.make_async_remote_copy(relay.at[spot], g_all.at[c], relay_sem.at[spot], got_g.at[c], **on(last)).start()

    def wide_saves(c):
        pairs = [(a_buf, a_all), (gp_buf, gp_all), (mid_buf, mid_all)]
        return [load(src, dst.at[c], st_sem.at[k]) for k, (src, dst) in enumerate(pairs)]

    def narrow_saves(c):
        pairs = [(ab_buf, ab_all), (gpb_buf, gpb_all)]
        return [load(src, dst.at[c], st_sem.at[k + 3]) for k, (src, dst) in enumerate(pairs)]

    def start(copies):
        for copy in copies:
            copy.start()

    def saved(c, copies):
        @pl.when(valid(c))
        def _():
            for copy in copies(c):
                copy.wait()

    @pl.when(me == 0)
    def _():
        load(acts.at[0], h_buf.at[h_slot(0)], h_sem.at[0]).start()
    for total in (dua, dwa, dub, dwb):
        total[...] = jnp.zeros_like(total)
    pl.semaphore_wait(barrier, stages)
    for copy in params:
        copy.wait()

    def step(t, _):
        cf, cb = fwd_chunk(t), bwd_chunk(t)
        has_f, has_b = valid(cf), valid(cb)
        feed_acts(t)
        feed_grads(t)

        f_alone = has_f & jnp.logical_not(has_b)
        late = f_alone & (cb + 1 < 0)
        before = cf - 1
        before_halved = valid(before) & (before < halved)
        loose = (cf < halved) & (cb + 1 < 0)

        @pl.when(valid(before) & (before >= halved))
        def _():
            saved(before, wide_saves)

            @pl.when(jnp.logical_not(late))
            def _():
                saved(before, narrow_saves)

        @pl.when(before_halved & jnp.logical_not(loose))
        def _():
            for r in range(2):
                for copy in half_saves(before, r):
                    copy.wait()

        @pl.when(valid(before) & (before < FIRST) & (me != 0))
        def _():
            keep_copy(before).wait()

        fetch_slopes(cb + 1)

        @pl.when(me == 0)
        def _():
            fetch_h(cf + 1)

        @pl.when(has_b)
        def _():
            fetch_weight_operands(cb)

        b_side = lax.rem(jnp.maximum(cb, 0), 2)
        f_side = lax.rem(jnp.maximum(cf, 0), 2)
        h_now = h_buf.at[h_slot(cf)]
        g_now, gp_now, gpb_now = g_buf.at[g_slot(cb)], gp_in.at[b_side], gpb_in.at[b_side]
        f_slot, b_slot = lax.rem(cf, SLOTS), lax.rem(cb, SLOTS)

        def f_begin():
            direct = (cf < FIRST) & (me != 0)

            @pl.when(direct)
            def _():
                for r in range(2):
                    half_arrival(cf, r).wait_recv()
                keep_copy(cf).start()

            @pl.when(jnp.logical_not(direct))
            def _():
                load(h_now, h_now, h_sem.at[f_side]).wait()

            @pl.when(cf >= SLOTS)
            def _():
                sent(f_send.at[f_slot], f_sem.at[f_slot])

        def f_tasks():
            def done(h):
                f_send[f_slot] = h
            return forward_tasks(h_now, weights, (a_buf, gp_buf, mid_buf, ab_buf, gpb_buf), done)

        def f_end():
            send(f_send.at[f_slot], f_sem.at[f_slot], cf, me != last, me + 1, h_all, got_h, acts_out, got_out)

        def b_begin():
            @pl.when(comes_direct(cb))
            def _():
                pltpu.make_async_remote_copy(g_now, g_now, got_g.at[chunks - 1], got_g.at[chunks - 1], **on(me)).wait_recv()

            @pl.when(jnp.logical_not(comes_direct(cb)))
            def _():
                load(g_now, g_now, g_sem).wait()
            load(gp_now, gp_now, gp_sem.at[b_side]).wait()
            load(gpb_now, gpb_now, gpb_sem.at[b_side]).wait()

            @pl.when(cb >= SLOTS)
            def _():
                sent(b_send.at[b_slot], b_sem.at[b_slot])

        def b_tasks():
            def done(g):
                b_send[b_slot] = g
            return backward_tasks(g_now, weights, (gp_now, gpb_now), (dzb_buf, gmid_buf, dz_buf), done)

        def b_end():
            @pl.when((cb == chunks - 1) & (me != 0))
            def _():
                pltpu.make_async_remote_copy(b_send.at[b_slot], g_buf.at[2], b_sem.at[b_slot], got_g.at[chunks - 1], **on(me - 1)).start()

            @pl.when((cb != chunks - 1) | (me == 0))
            def _():
                send_back()

        def send_back():
            send(b_send.at[b_slot], b_sem.at[b_slot], cb, me != 0, me - 1, g_all, got_g, grad_in, got_gin)

        @pl.when(has_f & has_b)
        def _():
            f_begin()
            b_begin()
            run_tasks(FB_ORDER, f_tasks() | b_tasks())
            b_end()
            f_end()
            start(wide_saves(cf) + narrow_saves(cf))

        @pl.when(has_f & (cf < halved))
        def _():
            @pl.when(me == 0)
            def _():
                load(h_now, h_now, h_sem.at[f_side]).wait()

            @pl.when(cf >= SLOTS)
            def _():
                sent(f_send.at[f_slot], f_sem.at[f_slot])

            def half_chunk(r, _):
                rows = half_rows(r)
                h_half, out_half = h_now.at[rows], f_send.at[f_slot, rows]

                @pl.when(me != 0)
                def _():
                    half_arrival(cf, r).wait_recv()

                    @pl.when(r == 1)
                    def _():
                        keep_copy(cf).start()

                @pl.when(before_halved & loose)
                def _():
                    for copy in half_saves(before, r):
                        copy.wait()

                def done(h):
                    out_half[...] = h
                run_tasks(HALF_ORDER, forward_tasks(h_half, weights, [buf.at[rows] for buf in (a_buf, gp_buf, mid_buf, ab_buf, gpb_buf)], done))

                @pl.when(me != last)
                def _():
                    pltpu.make_async_remote_copy(out_half, h_half, f_sem.at[f_slot], half_sem.at[cf, r], **on(me + 1)).start()

                @pl.when(me == last)
                def _():
                    pltpu.make_async_remote_copy(out_half, acts_out.at[cf, rows], f_sem.at[f_slot], got_out.at[cf], **on(0)).start()
                start(half_saves(cf, r))
                return 0

            lax.fori_loop(0, 2, half_chunk, 0)

        @pl.when(f_alone & (cf >= halved))
        def _():
            tasks = f_tasks()
            f_begin()
            run_tasks(F_ORDER[:-2], tasks)
            start(wide_saves(cf))

            @pl.when(late & (before >= halved))
            def _():
                saved(before, narrow_saves)
            run_tasks(F_ORDER[-2:], tasks)
            f_end()
            start(narrow_saves(cf))

        @pl.when(has_b & jnp.logical_not(has_f))
        def _():
            b_begin()
            run_tasks(B_ORDER, b_tasks())
            b_end()

        steady = cb + 1 < chunks - 2

        @pl.when(steady)
        def _():
            fetch_g(cb + 1)

            @pl.when(me != 0)
            def _():
                fetch_h(cf + 1)

        @pl.when(has_b)
        def _():
            for k, buf in enumerate((h_in, a_in, mid_in, ab_in)):
                load(buf, buf, w_sem.at[k]).wait()
            add_product(dwb, ab_in, g_now, 256)
            add_product(dub, mid_in, dzb_buf, 256)
            add_product(dwa, a_in, gmid_buf, 256)
            add_product(dua, h_in, dz_buf, 256)

        @pl.when(jnp.logical_not(steady))
        def _():
            fetch_g(cb + 1)
        return 0

    lax.fori_loop(0, chunks + span, step, 0)

    finals = [load(src, dst, param_sem.at[k]) for k, (src, dst) in enumerate(
        [(dua, dua_hbm), (dwa, dwa_hbm), (dub, dub_hbm), (dwb, dwb_hbm)])]
    for copy in finals:
        copy.start()
    for slot in range(SLOTS):
        sent(f_send.at[slot], f_sem.at[slot])
        sent(b_send.at[slot], b_sem.at[slot])

    def settle(k, _):
        @pl.when(me != 0)
        def _():
            load(acts.at[k], acts.at[k], feed_h_sem.at[k]).wait()
            arrival(grad_in, k, got_gin).wait_recv()

        @pl.when(me != last)
        def _():
            load(gout.at[k], gout.at[k], feed_g_sem.at[k]).wait()
            arrival(acts_out, k, got_out).wait_recv()

        @pl.when((me < edge) | (me == half) | (me >= half + edge))
        def _():
            load(relay.at[k], relay.at[k], relay_sem.at[k]).wait()
        return 0

    lax.fori_loop(0, own, settle, 0)
    for copy in finals:
        copy.wait()


def run_stages(axis, stages, acts, gout, ua, wa, ub, wb):
    tokens, width = acts.shape
    own = tokens // ROWS
    chunks = own * stages
    wide, narrow = ua.shape[1], ub.shape[1]
    bf, f32 = jnp.bfloat16, jnp.float32
    shape = jax.ShapeDtypeStruct
    outs = [
        shape((own, ROWS, width), bf), shape((own, ROWS, width), bf),
        shape(ua.shape, f32), shape(wa.shape, f32), shape(ub.shape, f32), shape(wb.shape, f32),
        shape((chunks, ROWS, width), bf), shape((chunks, ROWS, width), bf), shape((own, ROWS, width), bf), shape((chunks, ROWS, width), bf),
        shape((chunks, ROWS, wide), bf), shape((chunks, ROWS, wide), f32),
        shape((chunks, ROWS, narrow), bf), shape((chunks, ROWS, narrow), f32),
    ]
    vm, dma = pltpu.VMEM, pltpu.SemaphoreType.DMA
    tok, wid, nar = (ROWS, width), (ROWS, wide), (ROWS, narrow)
    scratch = [
        vm(ua.shape, bf), vm(wa.shape, bf), vm(ub.shape, bf), vm(wb.shape, bf),
        vm(ua.shape, f32), vm(wa.shape, f32), vm(ub.shape, f32), vm(wb.shape, f32),
        vm((2 + FIRST,) + tok, bf), vm(wid, bf), vm(wid, f32), vm(tok, bf), vm(nar, bf), vm(nar, f32), vm((SLOTS,) + tok, bf),
        vm((3,) + tok, bf), vm((2,) + wid, f32), vm((2,) + nar, f32), vm(nar, bf), vm(tok, bf), vm(wid, bf), vm((SLOTS,) + tok, bf),
        vm(wid, bf), vm(tok, bf), vm(tok, bf), vm(nar, bf),
        dma((chunks,)), dma((chunks,)), dma((own,)), dma((own,)), dma((SLOTS,)), dma((SLOTS,)), dma((own,)), dma((own,)), dma((own,)), dma((own,)), dma((FIRST, 2)), dma((FIRST,)), dma((2, 5)),
        dma((2,)), dma, dma((2,)), dma((2,)), dma((4,)), dma((5,)), dma((4,)),
    ]
    results = pl.pallas_call(
        functools.partial(kernel, axis),
        out_shape=outs,
        in_specs=[ANY] * 6,
        out_specs=[ANY] * len(outs),
        scratch_shapes=scratch,
        compiler_params=pltpu.CompilerParams(vmem_limit_bytes=VMEM_LIMIT, has_side_effects=True, collective_id=0),
    )(acts.reshape(own, ROWS, width), gout.reshape(own, ROWS, width), ua, wa, ub, wb)
    return results[:6]


def solution(mesh):
    tok_spec = P(('data', 'stage'))
    row_spec = P('stage')
    stages = mesh.shape['stage']

    def device_body(acts_in, grad_out, w_up_a, w_down_a, w_up_b, w_down_b):
        tokens, width = acts_in.shape[0] * acts_in.shape[1], acts_in.shape[2]
        out, gin, dua, dwa, dub, dwb = run_stages(
            'stage', stages, acts_in.reshape(tokens, width), grad_out.reshape(tokens, width),
            w_up_a[0], w_down_a[0], w_up_b[0], w_down_b[0])
        return (out.reshape(acts_in.shape), gin.reshape(acts_in.shape), dua[None], dwa[None], dub[None], dwb[None])

    return jax.shard_map(device_body, mesh=mesh, in_specs=(tok_spec, tok_spec, row_spec, row_spec, row_spec, row_spec), out_specs=(tok_spec,) * 6, check_vma=False)
```

```python
import functools

import jax
import jax.numpy as jnp
from jax import lax
from jax.experimental import pallas as pl
from jax.experimental.pallas import tpu as pltpu
from jax.sharding import PartitionSpec as P

MESH = pl.DeviceIdType.MESH
ANY = pl.BlockSpec(memory_space=pl.ANY)
VMEM_LIMIT = 67043328

GELU_C = 0.7978845608028654
GELU_K = 0.044715

ROWS = 256
LAG = 2
FIRST = 5
SLOTS = 4
WIDE_COLS = 512
F_ORDER = 'zzczczczczccyo'
HALF_ORDER = 'zzczczczczccyo'
B_ORDER = 'dmxxpxpxpxpxpp'

FB_ORDER = 'zdmzxzcxpzcpxzcxpzccpxcxpypo'

NT = (((1,), (1,)), ((), ()))
TN = (((0,), (0,)), ((), ()))


def mm(lhs, rhs, dims=(((1,), (0,)), ((), ()))):
    return lax.dot_general(lhs, rhs, dims, preferred_element_type=jnp.float32)


def gelu_and_slope(z):
    zz = z * z
    half = 0.5 + 0.5 * jnp.tanh(z * (GELU_C + (GELU_C * GELU_K) * zz))
    act = z * half
    return act, half + act * (1.0 - half) * (2.0 * GELU_C + (6.0 * GELU_C * GELU_K) * zz)


def blocks(size, width):
    return [slice(start, min(start + width, size)) for start in range(0, size, width)]


def forward_tasks(h, weights, saved, done):
    ua, wa, ub, wb = weights
    a_buf, gp_buf, mid_buf, ab_buf, gpb_buf = saved
    cols = blocks(ua.shape[1], WIDE_COLS)

    def wide_up():
        for part in cols:
            act, slope = gelu_and_slope(mm(h[...], ua[:, part]))
            a_buf[:, part] = act.astype(jnp.bfloat16)
            gp_buf[:, part] = slope
            yield

    def wide_down():
        total = 0.0
        for k, part in enumerate(cols):
            product = mm(a_buf[:, part], wa[part, :])
            total = product if k == 0 else total + product
            if k == len(cols) - 1:
                mid_buf[...] = (h[...].astype(jnp.float32) + total).astype(jnp.bfloat16)
            yield

    def narrow_up():
        act, slope = gelu_and_slope(mm(mid_buf[...], ub[...]))
        ab_buf[...] = act.astype(jnp.bfloat16)
        gpb_buf[...] = slope
        yield

    def narrow_down():
        done((mid_buf[...].astype(jnp.float32) + mm(ab_buf[...], wb[...])).astype(jnp.bfloat16))
        yield

    return dict(z=wide_up(), c=wide_down(), y=narrow_up(), o=narrow_down())


def backward_tasks(g, weights, slopes, kept, done):
    ua, wa, ub, wb = weights
    gp_buf, gpb_buf = slopes
    dzb_buf, gmid_buf, dz_buf = kept
    cols = blocks(wa.shape[0], WIDE_COLS)

    def narrow_down():
        dzb_buf[...] = (mm(g[...], wb[...], NT) * gpb_buf[...]).astype(jnp.bfloat16)
        yield

    def narrow_up():
        gmid_buf[...] = (g[...].astype(jnp.float32) + mm(dzb_buf[...], ub[...], NT)).astype(jnp.bfloat16)
        yield

    def wide_down():
        for part in cols:
            dz_buf[:, part] = (mm(gmid_buf[...], wa[part, :], NT) * gp_buf[:, part]).astype(jnp.bfloat16)
            yield

    def wide_up():
        total = 0.0
        for k, part in enumerate(cols):
            product = mm(dz_buf[:, part], ua[:, part], NT)
            total = product if k == 0 else total + product
            if k == len(cols) - 1:
                done((gmid_buf[...].astype(jnp.float32) + total).astype(jnp.bfloat16))
            yield

    return dict(d=narrow_down(), m=narrow_up(), x=wide_down(), p=wide_up())


def run_tasks(order, tasks):
    for name in order:
        next(tasks[name])


def add_product(total, lhs, rhs, width):
    for rows in blocks(total.shape[0], width):
        total[rows, :] += mm(lhs[:, rows].T, rhs[...])


def kernel(
    axis, acts, gout, ua_hbm, wa_hbm, ub_hbm, wb_hbm,
    acts_out, grad_in, dua_hbm, dwa_hbm, dub_hbm, dwb_hbm,
    h_all, g_all, relay, mid_all, a_all, gp_all, ab_all, gpb_all,
    ua, wa, ub, wb, dua, dwa, dub, dwb,
    h_buf, a_buf, gp_buf, mid_buf, ab_buf, gpb_buf, f_send,
    g_buf, gp_in, gpb_in, dzb_buf, gmid_buf, dz_buf, b_send,
    a_in, h_in, mid_in, ab_in,
    got_h, got_g, got_out, got_gin, f_sem, b_sem, feed_h_sem, feed_g_sem, got_relay, relay_sem, half_sem, keep_sem, half_st_sem,
    h_sem, g_sem, gp_sem, gpb_sem, w_sem, st_sem, param_sem,
):
    me = lax.axis_index(axis)
    stages = lax.axis_size(axis)
    last = stages - 1
    own = acts.shape[0]
    chunks = own * stages

    def ahead(stage):
        return stage + stage // 2

    def behind(stage):
        return 2 * stage + stage // 2

    span = ahead(last) + LAG + behind(last)

    weights = (ua, wa, ub, wb)

    def fwd_chunk(t):
        return t - ahead(me)

    def bwd_chunk(t):
        return t - span + behind(me)

    def valid(c):
        return (c >= 0) & (c < chunks)

    def on(device):
        return dict(device_id={axis: device}, device_id_type=MESH)

    def load(src, dst, sem):
        return pltpu.make_async_copy(src, dst, sem)

    params = [load(src, dst, param_sem.at[k]) for k, (src, dst) in enumerate(
        [(ua_hbm, ua), (wa_hbm, wa), (ub_hbm, ub), (wb_hbm, wb)])]
    for copy in params:
        copy.start()
    barrier = pltpu.get_barrier_semaphore()
    for device in range(stages):
        pl.semaphore_signal(barrier, inc=1, **on(device))

    def arrival(buf, c, sem):
        return pltpu.make_async_remote_copy(buf.at[c], buf.at[c], sem.at[c], sem.at[c], **on(me))

    halved = jnp.where(me == last, LAG, FIRST)

    def h_slot(c):
        return jnp.where(c < FIRST, 2 + jnp.maximum(c, 0), lax.rem(jnp.maximum(c, 0), 2))

    def half_rows(r):
        return pl.ds(pl.multiple_of(r * (ROWS // 2), ROWS // 2), ROWS // 2)

    def half_arrival(c, r):
        buf = h_buf.at[h_slot(c), half_rows(r)]
        return pltpu.make_async_remote_copy(buf, buf, half_sem.at[c, r], half_sem.at[c, r], **on(me))

    def keep_copy(c):
        return load(h_buf.at[h_slot(c)], h_all.at[c], keep_sem.at[c])

    def half_saves(c, r):
        pairs = [(a_buf, a_all), (gp_buf, gp_all), (mid_buf, mid_all), (ab_buf, ab_all), (gpb_buf, gpb_all)]
        return [load(src.at[half_rows(r)], dst.at[c, half_rows(r)], half_st_sem.at[r, k]) for k, (src, dst) in enumerate(pairs)]

    def fetch_h(c):
        @pl.when(valid(c) & ((c >= FIRST) | (me == 0)))
        def _():
            local = (me == 0) & (c < own)

            side = lax.rem(c, 2)
            buf = h_buf.at[h_slot(c)]

            @pl.when(local)
            def _():
                load(acts.at[lax.rem(c, own)], buf, h_sem.at[side]).start()

            @pl.when(jnp.logical_not(local))
            def _():
                arrival(h_all, c, got_h).wait_recv()
                load(h_all.at[c], buf, h_sem.at[side]).start()

    def fetch_slopes(c):
        @pl.when(valid(c))
        def _():
            side = lax.rem(c, 2)
            load(gp_all.at[c], gp_in.at[side], gp_sem.at[side]).start()
            load(gpb_all.at[c], gpb_in.at[side], gpb_sem.at[side]).start()

    def g_slot(c):
        return jnp.where(c == chunks - 1, 2, lax.rem(jnp.maximum(c, 0), 2))

    def comes_direct(c):
        return (c == chunks - 1) & (me != last)

    def fetch_g(c):
        @pl.when(valid(c) & jnp.logical_not(comes_direct(c)))
        def _():
            local = (me == last) & (c >= chunks - own)
            buf = g_buf.at[g_slot(c)]

            @pl.when(local)
            def _():
                load(gout.at[lax.rem(c, own)], buf, g_sem).start()

            @pl.when(jnp.logical_not(local))
            def _():
                arrival(g_all, c, got_g).wait_recv()
                load(g_all.at[c], buf, g_sem).start()

    def fetch_weight_operands(c):
        local_h = (me == 0) & (c < own)

        @pl.when(local_h)
        def _():
            load(acts.at[lax.rem(c, own)], h_in, w_sem.at[0]).start()

        @pl.when(jnp.logical_not(local_h))
        def _():
            load(h_all.at[c], h_in, w_sem.at[0]).start()
        load(a_all.at[c], a_in, w_sem.at[1]).start()
        load(mid_all.at[c], mid_in, w_sem.at[2]).start()
        load(ab_all.at[c], ab_in, w_sem.at[3]).start()

    def send(slot_ref, sem, c, inner, next_device, next_all, next_sem, home_out, home_sem):
        home = c // own
        spot = lax.rem(c, own)

        @pl.when(inner)
        def _():
            pltpu.make_async_remote_copy(slot_ref, next_all.at[c], sem, next_sem.at[c], **on(next_device)).start()

        @pl.when(jnp.logical_not(inner) & (home != me))
        def _():
            pltpu.make_async_remote_copy(slot_ref, home_out.at[spot], sem, home_sem.at[spot], **on(home)).start()

        @pl.when(jnp.logical_not(inner) & (home == me))
        def _():
            load(slot_ref, home_out.at[spot], sem).start()

    def sent(slot_ref, sem):
        load(slot_ref, slot_ref, sem).wait()

    half = stages // 2
    first_half, edge = me < half, half // 2

    def feed_acts(t):
        by_way = (me >= edge) & first_half
        later = jnp.where(me < half + edge, own * me - own - own // 2, 3 * own + 3 + own * (me - half - edge))
        spot = t - jnp.where(first_half, 0, later)
        due = (me != 0) & (spot >= 0) & (spot < own)

        @pl.when(due & jnp.logical_not(by_way))
        def _():
            pltpu.make_async_remote_copy(acts.at[spot], h_all.at[own * me + spot], feed_h_sem.at[spot], got_h.at[own * me + spot], **on(0)).start()

        @pl.when(due & by_way)
        def _():
            pltpu.make_async_remote_copy(acts.at[spot], relay.at[spot], feed_h_sem.at[spot], got_relay.at[spot], **on(me + half)).start()

        spot = t - me - 4

        @pl.when((me >= half + edge) & (spot >= 0) & (spot < own))
        def _():
            arrival(relay, spot, got_relay).wait_recv()
            c = own * (me - half) + spot
            pltpu.make_async_remote_copy(relay.at[spot], h_all.at[c], relay_sem.at[spot], got_h.at[c], **on(0)).start()

    def feed_grads(t):
        by_way = (me == 0) | (jnp.logical_not(first_half) & (me < half + edge))
        later = jnp.where(me == 1, 2 * own + 2, own // 2 + own * me)
        spot = t - jnp.where(me == 0, 0, jnp.where(by_way, 2 * own - 2 + 10 * (me - half), later))
        due = (me != last) & (spot >= 0) & (spot < own)

        @pl.when(due & jnp.logical_not(by_way))
        def _():
            pltpu.make_async_remote_copy(gout.at[spot], g_all.at[own * me + spot], feed_g_sem.at[spot], got_g.at[own * me + spot], **on(last)).start()

        @pl.when(due & by_way)
        def _():
            pltpu.make_async_remote_copy(gout.at[spot], relay.at[spot], feed_g_sem.at[spot], got_relay.at[spot], **on(lax.rem(me + half, stages))).start()

        source = jnp.where(me == half, 0, me + half)
        early = jnp.maximum(t - ahead(half), -1)
        spot = jnp.where(me == half, jnp.where(early < own - 1, (early + 1) // 2, early - own // 2 + 1), t - span - own * me)
        due = (me < edge) | ((me == half) & (early >= 0) & ((early >= own - 1) | (lax.rem(early + 2, 2) == 0)))

        @pl.when(due & (spot >= 0) & (spot < own))
        def _():
            arrival(relay, spot, got_relay).wait_recv()
            c = own * source + spot
            pltpu.make_async_remote_copy(relay.at[spot], g_all.at[c], relay_sem.at[spot], got_g.at[c], **on(last)).start()

    def wide_saves(c):
        pairs = [(a_buf, a_all), (gp_buf, gp_all), (mid_buf, mid_all)]
        return [load(src, dst.at[c], st_sem.at[k]) for k, (src, dst) in enumerate(pairs)]

    def narrow_saves(c):
        pairs = [(ab_buf, ab_all), (gpb_buf, gpb_all)]
        return [load(src, dst.at[c], st_sem.at[k + 3]) for k, (src, dst) in enumerate(pairs)]

    def start(copies):
        for copy in copies:
            copy.start()

    def saved(c, copies):
        @pl.when(valid(c))
        def _():
            for copy in copies(c):
                copy.wait()

    @pl.when(me == 0)
    def _():
        load(acts.at[0], h_buf.at[h_slot(0)], h_sem.at[0]).start()
    for total in (dua, dwa, dub, dwb):
        total[...] = jnp.zeros_like(total)
    pl.semaphore_wait(barrier, stages)
    for copy in params:
        copy.wait()

    def step(t, _):
        cf, cb = fwd_chunk(t), bwd_chunk(t)
        has_f, has_b = valid(cf), valid(cb)
        feed_acts(t)
        feed_grads(t)

        f_alone = has_f & jnp.logical_not(has_b)
        late = f_alone & (cb + 1 < 0)
        before = cf - 1
        before_halved = valid(before) & (before < halved)
        loose = (cf < halved) & (cb + 1 < 0)

        @pl.when(valid(before) & (before >= halved))
        def _():
            saved(before, wide_saves)

            @pl.when(jnp.logical_not(late))
            def _():
                saved(before, narrow_saves)

        @pl.when(before_halved & jnp.logical_not(loose))
        def _():
            for r in range(2):
                for copy in half_saves(before, r):
                    copy.wait()

        @pl.when(valid(before) & (before < FIRST) & (me != 0))
        def _():
            keep_copy(before).wait()

        fetch_slopes(cb + 1)

        @pl.when(me == 0)
        def _():
            fetch_h(cf + 1)

        @pl.when(has_b)
        def _():
            fetch_weight_operands(cb)

        b_side = lax.rem(jnp.maximum(cb, 0), 2)
        f_side = lax.rem(jnp.maximum(cf, 0), 2)
        h_now = h_buf.at[h_slot(cf)]
        g_now, gp_now, gpb_now = g_buf.at[g_slot(cb)], gp_in.at[b_side], gpb_in.at[b_side]
        f_slot, b_slot = lax.rem(cf, SLOTS), lax.rem(cb, SLOTS)

        def f_begin():
            direct = (cf < FIRST) & (me != 0)

            @pl.when(direct)
            def _():
                for r in range(2):
                    half_arrival(cf, r).wait_recv()
                keep_copy(cf).start()

            @pl.when(jnp.logical_not(direct))
            def _():
                load(h_now, h_now, h_sem.at[f_side]).wait()

            @pl.when(cf >= SLOTS)
            def _():
                sent(f_send.at[f_slot], f_sem.at[f_slot])

        def f_tasks():
            def done(h):
                f_send[f_slot] = h
            return forward_tasks(h_now, weights, (a_buf, gp_buf, mid_buf, ab_buf, gpb_buf), done)

        def f_end():
            send(f_send.at[f_slot], f_sem.at[f_slot], cf, me != last, me + 1, h_all, got_h, acts_out, got_out)

        def b_begin():
            @pl.when(comes_direct(cb))
            def _():
                pltpu.make_async_remote_copy(g_now, g_now, got_g.at[chunks - 1], got_g.at[chunks - 1], **on(me)).wait_recv()

            @pl.when(jnp.logical_not(comes_direct(cb)))
            def _():
                load(g_now, g_now, g_sem).wait()
            load(gp_now, gp_now, gp_sem.at[b_side]).wait()
            load(gpb_now, gpb_now, gpb_sem.at[b_side]).wait()

            @pl.when(cb >= SLOTS)
            def _():
                sent(b_send.at[b_slot], b_sem.at[b_slot])

        def b_tasks():
            def done(g):
                b_send[b_slot] = g
            return backward_tasks(g_now, weights, (gp_now, gpb_now), (dzb_buf, gmid_buf, dz_buf), done)

        def b_end():
            @pl.when((cb == chunks - 1) & (me != 0))
            def _():
                pltpu.make_async_remote_copy(b_send.at[b_slot], g_buf.at[2], b_sem.at[b_slot], got_g.at[chunks - 1], **on(me - 1)).start()

            @pl.when((cb != chunks - 1) | (me == 0))
            def _():
                send_back()

        def send_back():
            send(b_send.at[b_slot], b_sem.at[b_slot], cb, me != 0, me - 1, g_all, got_g, grad_in, got_gin)

        @pl.when(has_f & has_b)
        def _():
            f_begin()
            b_begin()
            run_tasks(FB_ORDER, f_tasks() | b_tasks())
            b_end()
            f_end()
            start(wide_saves(cf) + narrow_saves(cf))

        @pl.when(has_f & (cf < halved))
        def _():
            @pl.when(me == 0)
            def _():
                load(h_now, h_now, h_sem.at[f_side]).wait()

            @pl.when(cf >= SLOTS)
            def _():
                sent(f_send.at[f_slot], f_sem.at[f_slot])

            def half_chunk(r, _):
                rows = half_rows(r)
                h_half, out_half = h_now.at[rows], f_send.at[f_slot, rows]

                @pl.when(me != 0)
                def _():
                    half_arrival(cf, r).wait_recv()

                    @pl.when(r == 1)
                    def _():
                        keep_copy(cf).start()

                @pl.when(before_halved & loose)
                def _():
                    for copy in half_saves(before, r):
                        copy.wait()

                def done(h):
                    out_half[...] = h
                run_tasks(HALF_ORDER, forward_tasks(h_half, weights, [buf.at[rows] for buf in (a_buf, gp_buf, mid_buf, ab_buf, gpb_buf)], done))

                @pl.when(me != last)
                def _():
                    pltpu.make_async_remote_copy(out_half, h_half, f_sem.at[f_slot], half_sem.at[cf, r], **on(me + 1)).start()

                @pl.when(me == last)
                def _():
                    pltpu.make_async_remote_copy(out_half, acts_out.at[cf, rows], f_sem.at[f_slot], got_out.at[cf], **on(0)).start()
                start(half_saves(cf, r))
                return 0

            lax.fori_loop(0, 2, half_chunk, 0)

        @pl.when(f_alone & (cf >= halved))
        def _():
            tasks = f_tasks()
            f_begin()
            run_tasks(F_ORDER[:-2], tasks)
            start(wide_saves(cf))

            @pl.when(late & (before >= halved))
            def _():
                saved(before, narrow_saves)
            run_tasks(F_ORDER[-2:], tasks)
            f_end()
            start(narrow_saves(cf))

        @pl.when(has_b & jnp.logical_not(has_f))
        def _():
            b_begin()
            run_tasks(B_ORDER, b_tasks())
            b_end()

        steady = cb + 1 < chunks - 2

        @pl.when(steady)
        def _():
            fetch_g(cb + 1)

            @pl.when(me != 0)
            def _():
                fetch_h(cf + 1)

        @pl.when(has_b)
        def _():
            for k, buf in enumerate((h_in, a_in, mid_in, ab_in)):
                load(buf, buf, w_sem.at[k]).wait()
            add_product(dwb, ab_in, g_now, 256)
            add_product(dub, mid_in, dzb_buf, 256)
            add_product(dwa, a_in, gmid_buf, 256)
            add_product(dua, h_in, dz_buf, 256)

        @pl.when(jnp.logical_not(steady))
        def _():
            fetch_g(cb + 1)
        return 0

    lax.fori_loop(0, chunks + span, step, 0)

    finals = [load(src, dst, param_sem.at[k]) for k, (src, dst) in enumerate(
        [(dua, dua_hbm), (dwa, dwa_hbm), (dub, dub_hbm), (dwb, dwb_hbm)])]
    for copy in finals:
        copy.start()
    for slot in range(SLOTS):
        sent(f_send.at[slot], f_sem.at[slot])
        sent(b_send.at[slot], b_sem.at[slot])

    def settle(k, _):
        @pl.when(me != 0)
        def _():
            load(acts.at[k], acts.at[k], feed_h_sem.at[k]).wait()
            arrival(grad_in, k, got_gin).wait_recv()

        @pl.when(me != last)
        def _():
            load(gout.at[k], gout.at[k], feed_g_sem.at[k]).wait()
            arrival(acts_out, k, got_out).wait_recv()

        @pl.when((me < edge) | (me == half) | (me >= half + edge))
        def _():
            load(relay.at[k], relay.at[k], relay_sem.at[k]).wait()
        return 0

    lax.fori_loop(0, own, settle, 0)
    for copy in finals:
        copy.wait()


def run_stages(axis, stages, acts, gout, ua, wa, ub, wb):
    tokens, width = acts.shape
    own = tokens // ROWS
    chunks = own * stages
    wide, narrow = ua.shape[1], ub.shape[1]
    bf, f32 = jnp.bfloat16, jnp.float32
    shape = jax.ShapeDtypeStruct
    outs = [
        shape((own, ROWS, width), bf), shape((own, ROWS, width), bf),
        shape(ua.shape, f32), shape(wa.shape, f32), shape(ub.shape, f32), shape(wb.shape, f32),
        shape((chunks, ROWS, width), bf), shape((chunks, ROWS, width), bf), shape((own, ROWS, width), bf), shape((chunks, ROWS, width), bf),
        shape((chunks, ROWS, wide), bf), shape((chunks, ROWS, wide), f32),
        shape((chunks, ROWS, narrow), bf), shape((chunks, ROWS, narrow), f32),
    ]
    vm, dma = pltpu.VMEM, pltpu.SemaphoreType.DMA
    tok, wid, nar = (ROWS, width), (ROWS, wide), (ROWS, narrow)
    scratch = [
        vm(ua.shape, bf), vm(wa.shape, bf), vm(ub.shape, bf), vm(wb.shape, bf),
        vm(ua.shape, f32), vm(wa.shape, f32), vm(ub.shape, f32), vm(wb.shape, f32),
        vm((2 + FIRST,) + tok, bf), vm(wid, bf), vm(wid, f32), vm(tok, bf), vm(nar, bf), vm(nar, f32), vm((SLOTS,) + tok, bf),
        vm((3,) + tok, bf), vm((2,) + wid, f32), vm((2,) + nar, f32), vm(nar, bf), vm(tok, bf), vm(wid, bf), vm((SLOTS,) + tok, bf),
        vm(wid, bf), vm(tok, bf), vm(tok, bf), vm(nar, bf),
        dma((chunks,)), dma((chunks,)), dma((own,)), dma((own,)), dma((SLOTS,)), dma((SLOTS,)), dma((own,)), dma((own,)), dma((own,)), dma((own,)), dma((FIRST, 2)), dma((FIRST,)), dma((2, 5)),
        dma((2,)), dma, dma((2,)), dma((2,)), dma((4,)), dma((5,)), dma((4,)),
    ]
    results = pl.pallas_call(
        functools.partial(kernel, axis),
        out_shape=outs,
        in_specs=[ANY] * 6,
        out_specs=[ANY] * len(outs),
        scratch_shapes=scratch,
        compiler_params=pltpu.CompilerParams(vmem_limit_bytes=VMEM_LIMIT, has_side_effects=True, collective_id=0),
    )(acts.reshape(own, ROWS, width), gout.reshape(own, ROWS, width), ua, wa, ub, wb)
    return results[:6]


def solution(mesh):
    tok_spec = P(('data', 'stage'))
    row_spec = P('stage')
    stages = mesh.shape['stage']

    def device_body(acts_in, grad_out, w_up_a, w_down_a, w_up_b, w_down_b):
        tokens, width = acts_in.shape[0] * acts_in.shape[1], acts_in.shape[2]
        out, gin, dua, dwa, dub, dwb = run_stages(
            'stage', stages, acts_in.reshape(tokens, width), grad_out.reshape(tokens, width),
            w_up_a[0], w_down_a[0], w_up_b[0], w_down_b[0])
        return (out.reshape(acts_in.shape), gin.reshape(acts_in.shape), dua[None], dwa[None], dub[None], dwb[None])

    return jax.shard_map(device_body, mesh=mesh, in_specs=(tok_spec, tok_spec, row_spec, row_spec, row_spec, row_spec), out_specs=(tok_spec,) * 6, check_vma=False)
```
